128 devices in a mesh: band: 32 (over z, y, x_hi), grid: 4 (over x_lo, core).
Axes of the slice: x: 4 (x_hi: 2, x_lo: 2; x = x_hi * 2 + x_lo), y: 4, z: 4, core: 2. Of those that a mesh axis runs over, the one named last changes fastest.
Arguments:
- orbitals: float32 [128, 110592], P('band', 'grid'), may hold values from -6 to 6
Outputs:
- exchange_vectors: float32 [128, 110592], P('band', 'grid')
- margin: float32 [128, 128], P('grid', 'band')
The draws below stay inside these ranges and needn't reach their ends.
All inputs are finite; a program needn't handle non-finite values.
Results may differ from the reference program's by a relative error of at most 0.00012.
Values sent between devices are 32-bit elements; how exact they have to be, the bound alone decides.
No kernel may reach another device: no remote copies, remote signals or barrier semaphores. Data moves between devices by JAX's collectives and lax.ppermute only.
A program may use at most 128 MiB of HBM per device.

```python
import jax
import jax.numpy as jnp
from jax import lax

NG = 48
BAND_DEV = 4
NBANDS = 128
NCELL = 110592
N_BAND = 32


def steps_of(rng, dims, split, least, top_value):
    gain, own = 1.0, jax.random.fold_in(rng, 6)
    for position, shards_of in split:
        heights = jnp.exp(jax.random.uniform(jax.random.fold_in(own, position), (shards_of,), jnp.float32, least / len(split), top_value / len(split)))
        gain = gain * jnp.repeat(heights, dims[position] // shards_of).reshape([-1 if axis == position else 1 for axis in range(len(dims))])
    return gain


def normal_values(stream_key, shape, deviation, reach, split=(), kind=jnp.bfloat16):
    result = jax.random.normal(stream_key, shape, jnp.float32) * deviation
    if len(split) > 0:
        result = steps_of(stream_key, shape, split, -0.22, 0.18) * result
    return jnp.clip(result, min=-reach, max=reach).astype(kind)


def setup_inputs(seed: int = 0) -> dict:
    streams_of = jax.random.split(jax.random.key(seed), 2)
    orbitals = normal_values(streams_of[0], (NBANDS, NCELL), 1.0, 6.0, ((0, 32), (1, 4)), jnp.float32)
    return dict(orbitals=orbitals)


def folded_freq(count):
    indices = jnp.arange(count)
    return ((indices + count // 2) % count - count // 2).astype(jnp.float32)


def kernel_table():
    freqs = folded_freq(NG)
    squares = freqs[:, None, None] ** 2 + freqs[None, :, None] ** 2 + freqs[None, None, :] ** 2
    safe_sq = jnp.where(squares > 0, squares, jnp.float32(1.0))
    return jnp.where(squares > 0, 40.0 * (1.0 - jnp.exp(-squares / 16.0)) / safe_sq, jnp.float32(0.0))


def reference(orbitals):
    kernel = kernel_table()
    blocks = orbitals.reshape(N_BAND, BAND_DEV, NCELL)
    window = jnp.concatenate([blocks, jnp.roll(blocks, 1, axis=0), jnp.roll(blocks, -1, axis=0)], axis=1)

    def per_band(single, partners):
        density = (single[None, :] * partners).reshape(-1, NG, NG, NG)
        spectrum = jnp.fft.fftn(density, axes=(1, 2, 3))
        potential = jnp.real(jnp.fft.ifftn(spectrum * kernel, axes=(1, 2, 3))).reshape(-1, NCELL)
        return -jnp.sum(partners * potential, axis=0)

    def per_block(args):
        own_block, partners = args
        return lax.map(lambda single: per_band(single, partners), own_block)

    vectors = lax.map(per_block, (blocks, window)).reshape(NBANDS, NCELL).astype(jnp.float32)
    margin = jnp.dot(orbitals, vectors.T, precision=lax.Precision.HIGHEST, preferred_element_type=jnp.float32) / NCELL
    return vectors, margin
```

```python
import math

import jax
import jax.numpy as jnp
import numpy as np
from jax import lax
from jax.experimental import pallas as pl
from jax.experimental.pallas import tpu as pltpu
from jax.sharding import PartitionSpec as P

NG = 48
NCELL = 110592
PLANE = NG * NG
SLAB = 768
QX = 12
QCELL = QX * PLANE
F32 = jnp.float32
BF16 = jnp.bfloat16
R2 = math.sqrt(0.5)
C1 = math.cos(math.pi / 8)
C3 = math.cos(3 * math.pi / 8)
S3 = math.sqrt(3.0) / 2

ORDER = [("C", b) for b in range(9)] + [("S", b) for b in range(1, 8)]
SWAPPED = [("C", 0)] + [("S", b) for b in range(1, 8)] + [("C", 8)] + [("C", b) for b in range(1, 8)]


def sixteen(order):
    u = np.arange(16)
    cols = []
    for kind, b in order:
        col = np.cos(2 * np.pi * b * u / 16) if kind == "C" else np.sin(2 * np.pi * b * u / 16)
        cols.append(col / np.linalg.norm(col))
    return np.stack(cols, 1)


def forty_eight():
    z = np.arange(NG)
    cols, freqs = [], []
    for g in range(25):
        for kind in ("C", "S") if 0 < g < 24 else ("C",):
            col = np.cos(2 * np.pi * g * z / NG) if kind == "C" else np.sin(2 * np.pi * g * z / NG)
            cols.append(col / np.linalg.norm(col))
            freqs.append(g)
    return np.stack(cols, 1), np.array(freqs)


def folded(g):
    return (g + 24) % 48 - 24


def x_basis():
    keys, freqs, norms = [], [], []
    for b in range(9):
        keys.append(("A", "C", b)); freqs.append(3 * b); norms.append(48 if b in (0, 8) else 24)
    for b in range(1, 8):
        keys.append(("A", "S", b)); freqs.append(3 * b); norms.append(24)
    for b in (0, 8):
        for t in "cs":
            keys.append((t, "C", b)); freqs.append(16 + 3 * b); norms.append(24)
    for b in range(1, 8):
        for sign in (1, -1):
            for kind in ("cos", "sin"):
                keys.append((kind, sign, b)); freqs.append(16 + 3 * sign * b); norms.append(24)
    return keys, np.array(freqs), np.array(norms)


def kernel_values():
    _, gx, nx = x_basis()
    _, gz = forty_eight()
    gy = []
    for slab in "Auv":
        for kind, b in ORDER:
            if slab == "A":
                gy.append(3 * b)
            elif b in (0, 8):
                gy.append(16 + 3 * b)
            else:
                plus = (slab == "u") == (kind == "C")
                gy.append(16 + 3 * b if plus else 16 - 3 * b)
    gy = np.array(gy)
    q = (folded(gx)[:, None, None] ** 2 + folded(gy)[None, :, None] ** 2 + folded(gz)[None, None, :] ** 2).astype(np.float64)
    kern = np.where(q > 0, 40.0 * (1.0 - np.exp(-q / 16.0)) / np.where(q > 0, q, 1.0), 0.0)
    return (kern / (3.0 * nx[:, None, None])).reshape(NG, PLANE).astype(np.float32)


def thirds():
    u = np.arange(SLAB) // NG
    rows = [np.cos(2 * np.pi * (m + u) / 3) for m in range(3)] + [np.sin(2 * np.pi * (m + u) / 3) for m in range(3)]
    return np.concatenate([np.stack(rows), np.zeros((2, SLAB))]).astype(np.float32)


def factor_tables():
    za, _ = forty_eight()
    ta, ts = sixteen(ORDER), sixteen(SWAPPED)
    tens = np.stack([np.repeat(t, NG, 0) for t in (ta, ts, ta.T, ts.T)])
    zs = np.stack([np.tile(z, (16, 1)) for z in (za, za.T)])
    hot16 = np.repeat(np.eye(16), NG, 1)
    hot48 = np.tile(np.eye(NG), (1, 16))
    return [a.astype(np.float32) for a in (tens, zs, hot16, hot48)]


def tables_kernel(tens, zs, hot16, hot48, hi, lo):
    for way in range(2):
        z = jnp.dot(zs[way], hot48[...], precision=lax.Precision.HIGHEST, preferred_element_type=F32)
        for which in range(2):
            k = way * 2 + which
            t = jnp.dot(tens[k], hot16[...], precision=lax.Precision.HIGHEST, preferred_element_type=F32)
            w = t * z
            top = w.astype(BF16)
            hi[k] = top
            lo[k] = (w - top.astype(F32)).astype(BF16)


def plane_tables():
    out = jax.ShapeDtypeStruct((4, SLAB, SLAB), BF16)
    return pl.pallas_call(
        tables_kernel, out_shape=(out, out), name="plane_tables",
        compiler_params=pltpu.CompilerParams(vmem_limit_bytes=40 << 20),
    )(*[jnp.asarray(a) for a in factor_tables()])


def t16(f):
    o = [f[u] - f[u + 8] for u in range(8)]
    e = [f[u] + f[u + 8] for u in range(8)]
    ee = [e[u] + e[u + 4] for u in range(4)]
    eo = [e[u] - e[u + 4] for u in range(4)]
    c, s = {}, {}
    p0, p1 = ee[0] + ee[2], ee[1] + ee[3]
    c[0], c[8], c[4], s[4] = p0 + p1, p0 - p1, ee[0] - ee[2], ee[1] - ee[3]
    d, a = R2 * (eo[1] - eo[3]), R2 * (eo[1] + eo[3])
    c[2], c[6], s[2], s[6] = eo[0] + d, eo[0] - d, a + eo[2], a - eo[2]
    d1, d2, d3 = (o[u] - o[8 - u] for u in (1, 2, 3))
    s1, s2, s3 = (o[u] + o[8 - u] for u in (1, 2, 3))
    d2, s2 = R2 * d2, R2 * s2
    e1, e3 = o[0] + d2, o[0] - d2
    o1, o3 = C1 * d1 + C3 * d3, C3 * d1 - C1 * d3
    c[1], c[7], c[3], c[5] = e1 + o1, e1 - o1, e3 + o3, e3 - o3
    x1, x3 = o[4] + s2, o[4] - s2
    y1, y3 = C3 * s1 + C1 * s3, C1 * s1 - C3 * s3
    s[1], s[7], s[3], s[5] = y1 + x1, y1 - x1, y3 - x3, y3 + x3
    return c, s


def t16_back(c, s):
    e1, o1, e3, o3 = c[1] + c[7], c[1] - c[7], c[3] + c[5], c[3] - c[5]
    o0, d2 = e1 + e3, R2 * (e1 - e3)
    d1, d3 = C1 * o1 + C3 * o3, C3 * o1 - C1 * o3
    y1, x1, y3, x3 = s[1] + s[7], s[1] - s[7], s[3] + s[5], s[5] - s[3]
    o4, s2 = x1 + x3, R2 * (x1 - x3)
    s1, s3 = C3 * y1 + C1 * y3, C1 * y1 - C3 * y3
    o = [o0, d1 + s1, d2 + s2, d3 + s3, o4, s3 - d3, s2 - d2, s1 - d1]
    d, a = R2 * (c[2] - c[6]), R2 * (s[2] + s[6])
    eo = [c[2] + c[6], d + a, s[2] - s[6], a - d]
    p0, p1 = c[0] + c[8], c[0] - c[8]
    ee = [p0 + c[4], p1 + s[4], p0 - c[4], p1 - s[4]]
    e = [ee[u] + eo[u] for u in range(4)] + [ee[u] - eo[u] for u in range(4)]
    return [e[u] + o[u] for u in range(8)] + [e[u] - o[u] for u in range(8)]


def convolve_x(f, table):
    keys, _, _ = x_basis()
    row = {key: k for k, key in enumerate(keys)}
    place = {(x % 3, x % 16): x for x in range(NG)}
    part = {"A": [], "c": [], "s": []}
    for u in range(16):
        f0, f1, f2 = (f[place[t, u]] for t in range(3))
        a = f1 + f2
        part["A"].append(f0 + a)
        part["c"].append(f0 - 0.5 * a)
        part["s"].append(S3 * (f1 - f2))
    c, s = t16(part["A"])
    c = {b: v * table(row["A", "C", b]) for b, v in c.items()}
    s = {b: v * table(row["A", "S", b]) for b, v in s.items()}
    back_a = t16_back(c, s)
    cc, cs = t16(part["c"])
    sc, ss = t16(part["s"])
    for b in (0, 8):
        cc[b] = cc[b] * table(row["c", "C", b])
        sc[b] = sc[b] * table(row["s", "C", b])
    for b in range(1, 8):
        p = (cc[b] - ss[b]) * table(row["cos", 1, b])
        m = (cc[b] + ss[b]) * table(row["cos", -1, b])
        cc[b], ss[b] = p + m, m - p
        p = (sc[b] + cs[b]) * table(row["sin", 1, b])
        m = (sc[b] - cs[b]) * table(row["sin", -1, b])
        sc[b], cs[b] = p + m, p - m
    back_c, back_s = t16_back(cc, cs), t16_back(sc, ss)
    out = [None] * NG
    for u in range(16):
        a, c_, s_ = back_a[u], back_c[u], S3 * back_s[u]
        h = a - 0.5 * c_
        out[place[0, u]] = a + c_
        out[place[1, u]] = h + s_
        out[place[2, u]] = h - s_
    return out


def solve_kernel(q_ref, o0, o1, o2, o3, l0, l1, l2, l3, kern, third, whi_hbm, wlo_hbm, own_out, low_out,
                 right, left, hi, lo, field, whi, wlo, sems):
    q = q_ref[0]
    copies = []
    for way in range(2):
        part = pl.ds(2 * way, 2)
        copies.append([pltpu.make_async_copy(whi_hbm.at[part], whi.at[part], sems.at[2 * way]),
                       pltpu.make_async_copy(wlo_hbm.at[part], wlo.at[part], sems.at[2 * way + 1])])
        for copy in copies[-1]:
            copy.start()
    for delta, (own, low) in enumerate(((o0, l0), (o1, l1), (o2, l2), (o3, l3))):
        base = (q ^ delta) * QX

        for x in range(QX):
            span = pl.ds(x * PLANE, PLANE)
            bands = own[:, span]
            right[base + x, 0:4, :] = bands
            right[base + x, 4:8, :] = bands
            left[base + x, 0:4, :] = jnp.broadcast_to(own[pl.ds(q, 1), span], (4, PLANE))
            left[base + x, 4:8, :] = jnp.broadcast_to(low[:, span], (4, PLANE))

    def split(rows, m, value):
        top = value.astype(BF16)
        span = slice(m * SLAB, (m + 1) * SLAB)
        hi[rows, span] = top
        lo[rows, span] = (value - top.astype(F32)).astype(BF16)

    def densities(i, carry):
        x = pl.ds(2 * i, 2)
        rows = pl.ds(pl.multiple_of(16 * i, 16), 16)
        f = []
        for m in range(3):
            span = slice(m * SLAB, (m + 1) * SLAB)
            f.append((right[x, :, span] * left[x, :, span]).reshape(16, SLAB))
        split(rows, 0, f[0] + f[1] + f[2])
        split(rows, 1, f[0] * third[0:1, :] + f[1] * third[1:2, :] + f[2] * third[2:3, :])
        split(rows, 2, f[0] * third[3:4, :] + f[1] * third[4:5, :] + f[2] * third[5:6, :])
        return carry

    lax.fori_loop(0, NG // 2, densities, 0)

    def product(m, k, cols):
        span = slice(m * SLAB, (m + 1) * SLAB)
        a, b = hi[:, span], lo[:, span]
        lhs = jnp.concatenate([a, b, a], axis=1)
        w = jnp.concatenate([whi[k, :, cols], whi[k, :, cols], wlo[k, :, cols]], axis=0)
        return jnp.dot(lhs, w, preferred_element_type=F32)

    for copy in copies[0]:
        copy.wait()
    for j in range(3):
        cols = slice(j * 256, (j + 1) * 256)
        field[:, cols] = product(0, 0, cols)
        c = product(1, 0, cols)
        s = product(2, 1, cols)
        field[:, SLAB + j * 256 : SLAB + (j + 1) * 256] = c - s
        field[:, 2 * SLAB + j * 256 : 2 * SLAB + (j + 1) * 256] = c + s

    def along_x(i, carry):
        span = pl.ds(pl.multiple_of(128 * i, 128), 128)
        f = [field[8 * x : 8 * x + 8, span] for x in range(NG)]
        out = convolve_x(f, lambda k: kern[k : k + 1, span])
        for x in range(NG):
            field[8 * x : 8 * x + 8, span] = out[x]
        return carry

    lax.fori_loop(0, PLANE // 128, along_x, 0)

    def unmix(i, carry):
        rows = pl.ds(pl.multiple_of(16 * i, 16), 16)
        u = field[rows, SLAB : 2 * SLAB]
        v = field[rows, 2 * SLAB : 3 * SLAB]
        split(rows, 0, field[rows, 0:SLAB])
        split(rows, 1, u + v)
        split(rows, 2, v - u)
        return carry

    lax.fori_loop(0, NG // 2, unmix, 0)
    for copy in copies[1]:
        copy.wait()
    for j in range(3):
        cols = slice(j * 256, (j + 1) * 256)
        for m, k in ((0, 2), (1, 2), (2, 3)):
            field[:, m * SLAB + j * 256 : m * SLAB + (j + 1) * 256] = product(m, k, cols)

    mine = (lax.broadcasted_iota(jnp.int32, (8, SLAB), 0) == q).astype(F32)

    for delta in range(4):
        base = (q ^ delta) * QX

        def finish(i, carry):
            x = base + i
            rows = pl.ds(pl.multiple_of(x * 8, 8), 8)
            a = field[rows, 0:SLAB]
            c = field[rows, SLAB : 2 * SLAB]
            s = field[rows, 2 * SLAB : 3 * SLAB]
            for m in range(3):
                span = slice(m * SLAB, (m + 1) * SLAB)
                v = a + c * third[m : m + 1, :] + s * third[3 + m : 4 + m, :]
                pr = v * right[x, :, span]
                pr = pr + pltpu.roll(pr, 6, 0)
                pr = pr + pltpu.roll(pr, 7, 0)
                po = pltpu.roll(v * left[x, :, span], 4, 0) + mine * pr[0:1, :]
                at = pl.ds(pl.multiple_of(i * PLANE + m * SLAB, SLAB), SLAB)
                own_out[delta, :, at] = -po[0:4, :]
                low_out[delta, :, at] = -pr[4:5, :]
            return carry

        lax.fori_loop(0, QX, finish, 0)


def solve_pairs(q, owns, lows, tables):
    vmem = pl.BlockSpec(memory_space=pltpu.VMEM)
    hbm = pl.BlockSpec(memory_space=pl.ANY)
    return pl.pallas_call(
        solve_kernel,
        out_shape=(jax.ShapeDtypeStruct((4, 4, QCELL), F32), jax.ShapeDtypeStruct((4, 1, QCELL), F32)),
        in_specs=[pl.BlockSpec(memory_space=pltpu.SMEM)] + [vmem] * 10 + [hbm] * 2,
        out_specs=(vmem, vmem),
        scratch_shapes=[
            pltpu.VMEM((NG, 8, PLANE), F32),
            pltpu.VMEM((NG, 8, PLANE), F32),
            pltpu.VMEM((NG * 8, PLANE), BF16),
            pltpu.VMEM((NG * 8, PLANE), BF16),
            pltpu.VMEM((NG * 8, PLANE), F32),
            pltpu.VMEM((4, SLAB, SLAB), BF16),
            pltpu.VMEM((4, SLAB, SLAB), BF16),
            pltpu.SemaphoreType.DMA((4,)),
        ],
        name="solve_pairs",
        compiler_params=pltpu.CompilerParams(vmem_limit_bytes=56 << 20),
    )(q.reshape(1), *owns, *lows, jnp.asarray(kernel_values()), jnp.asarray(thirds()), *tables)


BOTH = ("band", "grid")


def move(value, blocks, flip):
    nb, nq = lax.axis_size("band"), lax.axis_size("grid")
    pairs = [(b * nq + q, (b + blocks) % nb * nq + (q ^ flip)) for b in range(nb) for q in range(nq)]
    return lax.ppermute(value, BOTH, pairs)


def spread(fields):
    nb = lax.axis_size("band")
    pieces = fields.reshape(4, nb, QCELL // nb).transpose(1, 0, 2)
    every = lax.all_to_all(pieces, "band", 0, 0, tiled=True)
    return every.reshape(4 * nb, QCELL // nb)


def on_device(orbitals):
    q = lax.axis_index("grid").astype(jnp.int32)
    two = move(orbitals, 0, 2)
    one = move(orbitals, 0, 1)
    lows = [move(lax.dynamic_slice_in_dim(orbitals, q ^ d, 1, 0), 1, d) for d in range(4)]
    tables = plane_tables()
    three = move(two, 0, 1)
    every_orbital = spread(orbitals)
    own, low = solve_pairs(q, (orbitals, one, two, three), lows, tables)
    owed = [move(low[d], -1, d) for d in range(4)]
    across = move(jnp.stack([own[1], own[3]]), 0, 1)
    far = move(own[2] + across[1], 0, 2)
    owed_rows = jnp.concatenate(
        [sum(jnp.where(q == (g ^ d), owed[d], 0.0) for d in range(4)) for g in range(4)], axis=0
    )
    vectors = own[0] + across[0] + far + owed_rows
    every_vector = spread(vectors)
    partial = lax.dot_general(
        every_orbital, every_vector, (((1,), (1,)), ((), ())),
        precision=lax.Precision.HIGHEST, preferred_element_type=F32,
    ) / NCELL
    nb, nq = lax.axis_size("band"), lax.axis_size("grid")
    pieces = partial.reshape(nq, 32, nb, 4).transpose(2, 0, 1, 3).reshape(nb * nq, 128)
    margin = jnp.sum(lax.all_to_all(pieces, BOTH, 0, 0, tiled=True), axis=0).reshape(32, 4)
    return vectors, margin


def solution(mesh):
    return jax.shard_map(
        on_device,
        mesh=mesh,
        in_specs=(P("band", "grid"),),
        out_specs=(P("band", "grid"), P("grid", "band")),
        check_vma=False,
    )
```

```python
import math

import jax
import jax.numpy as jnp
import numpy as np
from jax import lax
from jax.experimental import pallas as pl
from jax.experimental.pallas import tpu as pltpu
from jax.sharding import PartitionSpec as P

NG = 48
NCELL = 110592
PLANE = NG * NG
SLAB = 768
QX = 12
QCELL = QX * PLANE
F32 = jnp.float32
BF16 = jnp.bfloat16
R2 = math.sqrt(0.5)
C1 = math.cos(math.pi / 8)
C3 = math.cos(3 * math.pi / 8)
S3 = math.sqrt(3.0) / 2

ORDER = [("C", b) for b in range(9)] + [("S", b) for b in range(1, 8)]
SWAPPED = [("C", 0)] + [("S", b) for b in range(1, 8)] + [("C", 8)] + [("C", b) for b in range(1, 8)]


def sixteen(order):
    u = np.arange(16)
    cols = []
    for kind, b in order:
        col = np.cos(2 * np.pi * b * u / 16) if kind == "C" else np.sin(2 * np.pi * b * u / 16)
        cols.append(col / np.linalg.norm(col))
    return np.stack(cols, 1)


def forty_eight():
    z = np.arange(NG)
    cols, freqs = [], []
    for g in range(25):
        for kind in ("C", "S") if 0 < g < 24 else ("C",):
            col = np.cos(2 * np.pi * g * z / NG) if kind == "C" else np.sin(2 * np.pi * g * z / NG)
            cols.append(col / np.linalg.norm(col))
            freqs.append(g)
    return np.stack(cols, 1), np.array(freqs)


def folded(g):
    return (g + 24) % 48 - 24


def x_basis():
    keys, freqs, norms = [], [], []
    for b in range(9):
        keys.append(("A", "C", b)); freqs.append(3 * b); norms.append(48 if b in (0, 8) else 24)
    for b in range(1, 8):
        keys.append(("A", "S", b)); freqs.append(3 * b); norms.append(24)
    for b in (0, 8):
        for t in "cs":
            keys.append((t, "C", b)); freqs.append(16 + 3 * b); norms.append(24)
    for b in range(1, 8):
        for sign in (1, -1):
            for kind in ("cos", "sin"):
                keys.append((kind, sign, b)); freqs.append(16 + 3 * sign * b); norms.append(24)
    return keys, np.array(freqs), np.array(norms)


def kernel_values():
    _, gx, nx = x_basis()
    _, gz = forty_eight()
    gy = []
    for slab in "Auv":
        for kind, b in ORDER:
            if slab == "A":
                gy.append(3 * b)
            elif b in (0, 8):
                gy.append(16 + 3 * b)
            else:
                plus = (slab == "u") == (kind == "C")
                gy.append(16 + 3 * b if plus else 16 - 3 * b)
    gy = np.array(gy)
    q = (folded(gx)[:, None, None] ** 2 + folded(gy)[None, :, None] ** 2 + folded(gz)[None, None, :] ** 2).astype(np.float64)
    kern = np.where(q > 0, 40.0 * (1.0 - np.exp(-q / 16.0)) / np.where(q > 0, q, 1.0), 0.0)
    return (kern / (3.0 * nx[:, None, None])).reshape(NG, PLANE).astype(np.float32)


def thirds():
    u = np.arange(SLAB) // NG
    rows = [np.cos(2 * np.pi * (m + u) / 3) for m in range(3)] + [np.sin(2 * np.pi * (m + u) / 3) for m in range(3)]
    return np.concatenate([np.stack(rows), np.zeros((2, SLAB))]).astype(np.float32)


def factor_tables():
    za, _ = forty_eight()
    ta, ts = sixteen(ORDER), sixteen(SWAPPED)
    tens = np.stack([np.repeat(t, NG, 1) for t in (ta, ts, ta.T, ts.T)])
    zs = np.stack([np.tile(z, (1, 16)) for z in (za, za.T)])
    return [a.astype(np.float32) for a in (tens, zs)]


def tables_kernel(tens, zs, hi, lo):
    for way in range(2):
        for which in range(2):
            k = way * 2 + which

            def block(u, carry):
                w = zs[way] * tens[k, pl.ds(u, 1), :]
                top = w.astype(BF16)
                rows = pl.ds(pl.multiple_of(u * NG, 16), NG)
                hi[k, rows, :] = top
                lo[k, rows, :] = (w - top.astype(F32)).astype(BF16)
                return carry

            lax.fori_loop(0, 16, block, 0)


def plane_tables():
    out = jax.ShapeDtypeStruct((4, SLAB, SLAB), BF16)
    return pl.pallas_call(
        tables_kernel, out_shape=(out, out), name="plane_tables",
        compiler_params=pltpu.CompilerParams(vmem_limit_bytes=16 << 20),
    )(*[jnp.asarray(a) for a in factor_tables()])


def t16(f):
    o = [f[u] - f[u + 8] for u in range(8)]
    e = [f[u] + f[u + 8] for u in range(8)]
    ee = [e[u] + e[u + 4] for u in range(4)]
    eo = [e[u] - e[u + 4] for u in range(4)]
    c, s = {}, {}
    p0, p1 = ee[0] + ee[2], ee[1] + ee[3]
    c[0], c[8], c[4], s[4] = p0 + p1, p0 - p1, ee[0] - ee[2], ee[1] - ee[3]
    d, a = R2 * (eo[1] - eo[3]), R2 * (eo[1] + eo[3])
    c[2], c[6], s[2], s[6] = eo[0] + d, eo[0] - d, a + eo[2], a - eo[2]
    d1, d2, d3 = (o[u] - o[8 - u] for u in (1, 2, 3))
    s1, s2, s3 = (o[u] + o[8 - u] for u in (1, 2, 3))
    d2, s2 = R2 * d2, R2 * s2
    e1, e3 = o[0] + d2, o[0] - d2
    o1, o3 = C1 * d1 + C3 * d3, C3 * d1 - C1 * d3
    c[1], c[7], c[3], c[5] = e1 + o1, e1 - o1, e3 + o3, e3 - o3
    x1, x3 = o[4] + s2, o[4] - s2
    y1, y3 = C3 * s1 + C1 * s3, C1 * s1 - C3 * s3
    s[1], s[7], s[3], s[5] = y1 + x1, y1 - x1, y3 - x3, y3 + x3
    return c, s


def t16_back(c, s):
    e1, o1, e3, o3 = c[1] + c[7], c[1] - c[7], c[3] + c[5], c[3] - c[5]
    o0, d2 = e1 + e3, R2 * (e1 - e3)
    d1, d3 = C1 * o1 + C3 * o3, C3 * o1 - C1 * o3
    y1, x1, y3, x3 = s[1] + s[7], s[1] - s[7], s[3] + s[5], s[5] - s[3]
    o4, s2 = x1 + x3, R2 * (x1 - x3)
    s1, s3 = C3 * y1 + C1 * y3, C1 * y1 - C3 * y3
    o = [o0, d1 + s1, d2 + s2, d3 + s3, o4, s3 - d3, s2 - d2, s1 - d1]
    d, a = R2 * (c[2] - c[6]), R2 * (s[2] + s[6])
    eo = [c[2] + c[6], d + a, s[2] - s[6], a - d]
    p0, p1 = c[0] + c[8], c[0] - c[8]
    ee = [p0 + c[4], p1 + s[4], p0 - c[4], p1 - s[4]]
    e = [ee[u] + eo[u] for u in range(4)] + [ee[u] - eo[u] for u in range(4)]
    return [e[u] + o[u] for u in range(8)] + [e[u] - o[u] for u in range(8)]


def convolve_x(f, table):
    keys, _, _ = x_basis()
    row = {key: k for k, key in enumerate(keys)}
    place = {(x % 3, x % 16): x for x in range(NG)}
    part = {"A": [], "c": [], "s": []}
    for u in range(16):
        f0, f1, f2 = (f[place[t, u]] for t in range(3))
        a = f1 + f2
        part["A"].append(f0 + a)
        part["c"].append(f0 - 0.5 * a)
        part["s"].append(S3 * (f1 - f2))
    c, s = t16(part["A"])
    c = {b: v * table(row["A", "C", b]) for b, v in c.items()}
    s = {b: v * table(row["A", "S", b]) for b, v in s.items()}
    back_a = t16_back(c, s)
    cc, cs = t16(part["c"])
    sc, ss = t16(part["s"])
    for b in (0, 8):
        cc[b] = cc[b] * table(row["c", "C", b])
        sc[b] = sc[b] * table(row["s", "C", b])
    for b in range(1, 8):
        p = (cc[b] - ss[b]) * table(row["cos", 1, b])
        m = (cc[b] + ss[b]) * table(row["cos", -1, b])
        cc[b], ss[b] = p + m, m - p
        p = (sc[b] + cs[b]) * table(row["sin", 1, b])
        m = (sc[b] - cs[b]) * table(row["sin", -1, b])
        sc[b], cs[b] = p + m, p - m
    back_c, back_s = t16_back(cc, cs), t16_back(sc, ss)
    out = [None] * NG
    for u in range(16):
        a, c_, s_ = back_a[u], back_c[u], S3 * back_s[u]
        h = a - 0.5 * c_
        out[place[0, u]] = a + c_
        out[place[1, u]] = h + s_
        out[place[2, u]] = h - s_
    return out


def solve_kernel(q_ref, o0, o1, o2, o3, l0, l1, l2, l3, kern, third, whi, wlo, near0, near2, cross, low0, low1, low2, low3,
                 right, left, hi, lo, field):
    q = q_ref[0]
    for delta, (own, low) in enumerate(((o0, l0), (o1, l1), (o2, l2), (o3, l3))):
        base = (q ^ delta) * QX

        def place(x, carry):
            span = pl.ds(pl.multiple_of(x * PLANE, 128), PLANE)
            bands = own[:, span]
            right[base + x, 0:4, :] = bands
            right[base + x, 4:8, :] = bands
            left[base + x, 0:4, :] = jnp.broadcast_to(own[pl.ds(q, 1), span], (4, PLANE))
            left[base + x, 4:8, :] = jnp.broadcast_to(low[:, span], (4, PLANE))
            return carry

        lax.fori_loop(0, QX, place, 0)

    def split(rows, m, value):
        top = value.astype(BF16)
        span = slice(m * SLAB, (m + 1) * SLAB)
        hi[rows, span] = top
        lo[rows, span] = (value - top.astype(F32)).astype(BF16)

    def densities(i, carry):
        x = pl.ds(2 * i, 2)
        rows = pl.ds(pl.multiple_of(16 * i, 16), 16)
        f = []
        for m in range(3):
            span = slice(m * SLAB, (m + 1) * SLAB)
            f.append((right[x, :, span] * left[x, :, span]).reshape(16, SLAB))
        split(rows, 0, f[0] + f[1] + f[2])
        split(rows, 1, f[0] * third[0:1, :] + f[1] * third[1:2, :] + f[2] * third[2:3, :])
        split(rows, 2, f[0] * third[3:4, :] + f[1] * third[4:5, :] + f[2] * third[5:6, :])
        return carry

    lax.fori_loop(0, NG // 2, densities, 0)

    def product(m, k, cols):
        span = slice(m * SLAB, (m + 1) * SLAB)
        a, b = hi[:, span], lo[:, span]
        lhs = jnp.concatenate([a, b, a], axis=1)
        w = jnp.concatenate([whi[k, :, cols], whi[k, :, cols], wlo[k, :, cols]], axis=0)
        return jnp.dot(lhs, w, preferred_element_type=F32)

    for j in range(3):
        cols = slice(j * 256, (j + 1) * 256)
        field[:, cols] = product(0, 0, cols)
        c = product(1, 0, cols)
        s = product(2, 1, cols)
        field[:, SLAB + j * 256 : SLAB + (j + 1) * 256] = c - s
        field[:, 2 * SLAB + j * 256 : 2 * SLAB + (j + 1) * 256] = c + s

    def along_x(i, carry):
        span = pl.ds(pl.multiple_of(128 * i, 128), 128)
        f = [field[8 * x : 8 * x + 8, span] for x in range(NG)]
        out = convolve_x(f, lambda k: kern[k : k + 1, span])
        for x in range(NG):
            field[8 * x : 8 * x + 8, span] = out[x]
        return carry

    lax.fori_loop(0, PLANE // 128, along_x, 0)

    def unmix(i, carry):
        rows = pl.ds(pl.multiple_of(16 * i, 16), 16)
        u = field[rows, SLAB : 2 * SLAB]
        v = field[rows, 2 * SLAB : 3 * SLAB]
        split(rows, 0, field[rows, 0:SLAB])
        split(rows, 1, u + v)
        split(rows, 2, v - u)
        return carry

    lax.fori_loop(0, NG // 2, unmix, 0)
    for j in range(3):
        cols = slice(j * 256, (j + 1) * 256)
        for m, k in ((0, 2), (1, 2), (2, 3)):
            field[:, m * SLAB + j * 256 : m * SLAB + (j + 1) * 256] = product(m, k, cols)

    mine = (lax.broadcasted_iota(jnp.int32, (8, SLAB), 0) == q).astype(F32)

    for delta in range(4):
        base = (q ^ delta) * QX

        def finish(i, carry):
            x = base + i
            rows = pl.ds(pl.multiple_of(x * 8, 8), 8)
            a = field[rows, 0:SLAB]
            c = field[rows, SLAB : 2 * SLAB]
            s = field[rows, 2 * SLAB : 3 * SLAB]
            for m in range(3):
                span = slice(m * SLAB, (m + 1) * SLAB)
                v = a + c * third[m : m + 1, :] + s * third[3 + m : 4 + m, :]
                pr = v * right[x, :, span]
                pr = pr + pltpu.roll(pr, 6, 0)
                pr = pr + pltpu.roll(pr, 7, 0)
                po = pltpu.roll(v * left[x, :, span], 4, 0) + mine * pr[0:1, :]
                at = pl.ds(pl.multiple_of(i * PLANE + m * SLAB, SLAB), SLAB)
                bands = -po[0:4, :]
                if delta % 2:
                    cross[delta // 2, :, at] = bands
                else:
                    (near0, near2)[delta // 2][:, at] = bands
                (low0, low1, low2, low3)[delta][:, at] = -pr[4:5, :]
            return carry

        lax.fori_loop(0, QX, finish, 0)


def solve_pairs(q, owns, lows, tables):
    vmem = pl.BlockSpec(memory_space=pltpu.VMEM)
    return pl.pallas_call(
        solve_kernel,
        out_shape=[jax.ShapeDtypeStruct(shape, F32) for shape in [(4, QCELL)] * 2 + [(2, 4, QCELL)] + [(1, QCELL)] * 4],
        in_specs=[pl.BlockSpec(memory_space=pltpu.SMEM)] + [vmem] * 12,
        out_specs=[vmem] * 7,
        scratch_shapes=[
            pltpu.VMEM((NG, 8, PLANE), F32),
            pltpu.VMEM((NG, 8, PLANE), F32),
            pltpu.VMEM((NG * 8, PLANE), BF16),
            pltpu.VMEM((NG * 8, PLANE), BF16),
            pltpu.VMEM((NG * 8, PLANE), F32),
        ],
        name="solve_pairs",
        compiler_params=pltpu.CompilerParams(vmem_limit_bytes=34 << 20),
    )(q.reshape(1), *owns, *lows, jnp.asarray(kernel_values()), jnp.asarray(thirds()), *tables)


BOTH = ("band", "grid")
CHUNK = QCELL // 4


def small_call(body, outs, scratch=()):
    vmem = pl.BlockSpec(memory_space=pltpu.VMEM)

    def call(where, *arrays):
        return pl.pallas_call(
            body,
            out_shape=[jax.ShapeDtypeStruct(shape, F32) for shape in outs],
            in_specs=[pl.BlockSpec(memory_space=pltpu.SMEM)] + [vmem] * len(arrays),
            out_specs=[vmem] * len(outs),
            scratch_shapes=list(scratch),
            compiler_params=pltpu.CompilerParams(vmem_limit_bytes=24 << 20),
        )(where, *arrays)

    return call


def chunk_of(where, k):
    return pl.ds(pl.multiple_of(((where[1] + k) % 4) * CHUNK, 128), CHUNK)


def prepare_kernel(where, orbitals, *outs):
    q = where[0]
    for d in range(4):
        outs[d][...] = orbitals[pl.ds(q ^ d, 1), :]
        outs[4 + d][...] = orbitals[:, chunk_of(where, d)]


def finalize_kernel(where, near, across, far, o0, o1, o2, o3, vectors, *chunks):
    q = where[0]
    row = lax.broadcasted_iota(jnp.int32, (4, CHUNK), 0)
    for c in range(4):
        span = pl.ds(c * CHUNK, CHUNK)
        total = near[:, span] + across[0, :, span] + far[:, span]
        for d, owed in enumerate((o0, o1, o2, o3)):
            total = total + jnp.where(row == (q ^ d), jnp.broadcast_to(owed[:, span], (4, CHUNK)), 0.0)
        vectors[:, span] = total
    for k in range(4):
        chunks[k][...] = vectors[:, chunk_of(where, k)]


def add_kernel(where, near, across, out):
    out[...] = near[...] + across[1]


def pair_kernel(where, f0, f1, f2, f3, other, out):
    mine_first = where[3] == 0
    for k, f in enumerate((f0, f1, f2, f3)):
        a, b = f[...], other[k]
        out[k, 0:4, :] = jnp.where(mine_first, a, b)
        out[k, 4:8, :] = jnp.where(mine_first, b, a)


def margin_kernel(where, p0, p1, p2, p3, v0, v1, v2, v3, m0, m1, m2, m3, block):
    z, y = where[1], where[2]

    def halves(a):
        top = a.astype(BF16)
        return top, (a - top.astype(F32)).astype(BF16)

    bands = jnp.concatenate([v0[...], v1[...], v2[...], v3[...]], axis=0)
    vt, vl = halves(bands)
    dims = (((1,), (1,)), ((), ()))
    for dy, part in enumerate((p0, p1, p2, p3)):
        ft, fl = halves(part[...].reshape(32, CHUNK))
        got = (
            lax.dot_general(ft, vt, dims, preferred_element_type=F32)
            + lax.dot_general(fl, vt, dims, preferred_element_type=F32)
            + lax.dot_general(ft, vl, dims, preferred_element_type=F32)
        )
        for dz in range(4):
            at = ((z + 4 - dz) % 4) * 4 + (y + 4 - dy) % 4
            block[at, :, :] = got[8 * dz : 8 * dz + 8, :]
    out = block[...].reshape(128, 16).T * (1.0 / NCELL)
    for k, m in enumerate((m0, m1, m2, m3)):
        m[...] = out[4 * k : 4 * k + 4, :]


def move(value, target):
    nb, nq = lax.axis_size("band"), lax.axis_size("grid")
    pairs = []
    for b in range(nb):
        for q in range(nq):
            z, y, h, q_to = target(b // 8, b // 2 % 4, b % 2, q)
            pairs.append((b * nq + q, ((z % 4) * 8 + (y % 4) * 2 + h) * nq + q_to))
    return lax.ppermute(value, BOTH, pairs)


def along_z(value, k):
    return move(value, lambda z, y, h, q: (z + k, y, h, q))


def along_y(value, k):
    return move(value, lambda z, y, h, q: (z, y + k, h, q))


def within(value, flip):
    return move(value, lambda z, y, h, q: (z, y, h, q ^ flip))


def around(value, blocks, flip):
    def target(z, y, h, q):
        b = (z * 8 + y * 2 + h + blocks) % 32
        return b // 8, b // 2 % 4, b % 2, q ^ flip

    return move(value, target)


def step(orbitals):
    b = lax.axis_index("band").astype(jnp.int32)
    q = lax.axis_index("grid").astype(jnp.int32)
    where = jnp.stack([q, b // 8, b // 2 % 4, b % 2])
    two = within(orbitals, 2)
    one = within(orbitals, 1)
    prepare = small_call(prepare_kernel, [(1, QCELL)] * 4 + [(4, CHUNK)] * 4)
    ready = prepare(where, orbitals)
    lows = [around(ready[d], 1, d) for d in range(4)]
    pieces = [ready[4]] + [along_z(ready[4 + k], k) for k in (1, 2, 3)]
    tables = plane_tables()
    stacked = jnp.stack(pieces)
    two, tables, stacked = lax.optimization_barrier((two, tables, stacked))
    three = within(two, 1)
    other = move(stacked, lambda z, y, h, q: (z, y, 1 - h, q))
    near0, near2, cross, *low = solve_pairs(q, (orbitals, one, two, three), lows, tables)
    across = within(cross, 1)
    owed = [around(low[d], -1, d) for d in range(4)]
    both = small_call(add_kernel, [(4, QCELL)])(where, near2, across)[0]
    far = within(both, 2)
    other, _ = lax.optimization_barrier((other, near0))
    (paired,) = small_call(pair_kernel, [(4, 8, CHUNK)])(where, *pieces, other)
    parts = [paired] + [along_y(paired, k) for k in (1, 2, 3)]
    finalize = small_call(finalize_kernel, [(4, QCELL)] + [(4, CHUNK)] * 4)
    vectors, *chunks = finalize(where, near0, across, far, *owed)
    given = [chunks[0]] + [along_z(chunks[k], k) for k in (1, 2, 3)]
    margin_part = small_call(margin_kernel, [(4, 128)] * 4, [pltpu.VMEM((16, 8, 16), F32)])
    sums = margin_part(where, *parts, *given)
    mine = sums[0] + sum(along_z(sums[k], -k) for k in (1, 2, 3))
    total = mine + sum(within(mine, d) for d in (1, 2, 3))
    margin = lax.dynamic_slice_in_dim(total, q * 32, 32, 1).T
    return vectors, margin


def solution(mesh):
    return jax.shard_map(
        step,
        mesh=mesh,
        in_specs=(P("band", "grid"),),
        out_specs=(P("band", "grid"), P("grid", "band")),
        check_vma=False,
    )
```

```python
import math

import jax
import jax.numpy as jnp
import numpy as np
from jax import lax
from jax.experimental import pallas as pl
from jax.experimental.pallas import tpu as pltpu
from jax.sharding import PartitionSpec as P

NG = 48
NCELL = 110592
PLANE = NG * NG
SLAB = 768
QX = 12
QCELL = QX * PLANE
F32 = jnp.float32
BF16 = jnp.bfloat16
R2 = math.sqrt(0.5)
C1 = math.cos(math.pi / 8)
C3 = math.cos(3 * math.pi / 8)
S3 = math.sqrt(3.0) / 2

ORDER = [("C", b) for b in range(9)] + [("S", b) for b in range(1, 8)]
SWAPPED = [("C", 0)] + [("S", b) for b in range(1, 8)] + [("C", 8)] + [("C", b) for b in range(1, 8)]


def sixteen(order):
    u = np.arange(16)
    cols = []
    for kind, b in order:
        col = np.cos(2 * np.pi * b * u / 16) if kind == "C" else np.sin(2 * np.pi * b * u / 16)
        cols.append(col / np.linalg.norm(col))
    return np.stack(cols, 1)


def forty_eight():
    z = np.arange(NG)
    cols, freqs = [], []
    for g in range(25):
        for kind in ("C", "S") if 0 < g < 24 else ("C",):
            col = np.cos(2 * np.pi * g * z / NG) if kind == "C" else np.sin(2 * np.pi * g * z / NG)
            cols.append(col / np.linalg.norm(col))
            freqs.append(g)
    return np.stack(cols, 1), np.array(freqs)


def folded(g):
    return (g + 24) % 48 - 24


def x_basis():
    keys, freqs, norms = [], [], []
    for b in range(9):
        keys.append(("A", "C", b)); freqs.append(3 * b); norms.append(48 if b in (0, 8) else 24)
    for b in range(1, 8):
        keys.append(("A", "S", b)); freqs.append(3 * b); norms.append(24)
    for b in (0, 8):
        for t in "cs":
            keys.append((t, "C", b)); freqs.append(16 + 3 * b); norms.append(24)
    for b in range(1, 8):
        for sign in (1, -1):
            for kind in ("cos", "sin"):
                keys.append((kind, sign, b)); freqs.append(16 + 3 * sign * b); norms.append(24)
    return keys, np.array(freqs), np.array(norms)


def kernel_values():
    _, gx, nx = x_basis()
    _, gz = forty_eight()
    gy = []
    for slab in "Auv":
        for kind, b in ORDER:
            if slab == "A":
                gy.append(3 * b)
            elif b in (0, 8):
                gy.append(16 + 3 * b)
            else:
                plus = (slab == "u") == (kind == "C")
                gy.append(16 + 3 * b if plus else 16 - 3 * b)
    gy = np.array(gy)
    q = (folded(gx)[:, None, None] ** 2 + folded(gy)[None, :, None] ** 2 + folded(gz)[None, None, :] ** 2).astype(np.float64)
    kern = np.where(q > 0, 40.0 * (1.0 - np.exp(-q / 16.0)) / np.where(q > 0, q, 1.0), 0.0)
    return (kern / (3.0 * nx[:, None, None])).reshape(NG, PLANE).astype(np.float32)


def thirds():
    u = np.arange(SLAB) // NG
    rows = [np.cos(2 * np.pi * (m + u) / 3) for m in range(3)] + [np.sin(2 * np.pi * (m + u) / 3) for m in range(3)]
    return np.concatenate([np.stack(rows), np.zeros((2, SLAB))]).astype(np.float32)


def factor_tables():
    za, _ = forty_eight()
    ta, ts = sixteen(ORDER), sixteen(SWAPPED)
    tens = np.stack([np.repeat(t, NG, 1) for t in (ta, ts, ta.T, ts.T)])
    zs = np.stack([np.tile(z, (1, 16)) for z in (za, za.T)])
    return [a.astype(np.float32) for a in (tens, zs)]


def tables_kernel(tens, zs, hi, lo):
    for way in range(2):
        for which in range(2):
            k = way * 2 + which

            def block(u, carry):
                w = zs[way] * tens[k, pl.ds(u, 1), :]
                top = w.astype(BF16)
                rows = pl.ds(pl.multiple_of(u * NG, 16), NG)
                hi[k, rows, :] = top
                lo[k, rows, :] = (w - top.astype(F32)).astype(BF16)
                return carry

            lax.fori_loop(0, 16, block, 0)


def plane_tables():
    out = jax.ShapeDtypeStruct((4, SLAB, SLAB), BF16)
    return pl.pallas_call(
        tables_kernel, out_shape=(out, out), name="plane_tables",
        compiler_params=pltpu.CompilerParams(vmem_limit_bytes=16 << 20),
    )(*[jnp.asarray(a) for a in factor_tables()])


def t16(f):
    o = [f[u] - f[u + 8] for u in range(8)]
    e = [f[u] + f[u + 8] for u in range(8)]
    ee = [e[u] + e[u + 4] for u in range(4)]
    eo = [e[u] - e[u + 4] for u in range(4)]
    c, s = {}, {}
    p0, p1 = ee[0] + ee[2], ee[1] + ee[3]
    c[0], c[8], c[4], s[4] = p0 + p1, p0 - p1, ee[0] - ee[2], ee[1] - ee[3]
    d, a = R2 * (eo[1] - eo[3]), R2 * (eo[1] + eo[3])
    c[2], c[6], s[2], s[6] = eo[0] + d, eo[0] - d, a + eo[2], a - eo[2]
    d1, d2, d3 = (o[u] - o[8 - u] for u in (1, 2, 3))
    s1, s2, s3 = (o[u] + o[8 - u] for u in (1, 2, 3))
    d2, s2 = R2 * d2, R2 * s2
    e1, e3 = o[0] + d2, o[0] - d2
    o1, o3 = C1 * d1 + C3 * d3, C3 * d1 - C1 * d3
    c[1], c[7], c[3], c[5] = e1 + o1, e1 - o1, e3 + o3, e3 - o3
    x1, x3 = o[4] + s2, o[4] - s2
    y1, y3 = C3 * s1 + C1 * s3, C1 * s1 - C3 * s3
    s[1], s[7], s[3], s[5] = y1 + x1, y1 - x1, y3 - x3, y3 + x3
    return c, s


def t16_back(c, s):
    e1, o1, e3, o3 = c[1] + c[7], c[1] - c[7], c[3] + c[5], c[3] - c[5]
    o0, d2 = e1 + e3, R2 * (e1 - e3)
    d1, d3 = C1 * o1 + C3 * o3, C3 * o1 - C1 * o3
    y1, x1, y3, x3 = s[1] + s[7], s[1] - s[7], s[3] + s[5], s[5] - s[3]
    o4, s2 = x1 + x3, R2 * (x1 - x3)
    s1, s3 = C3 * y1 + C1 * y3, C1 * y1 - C3 * y3
    o = [o0, d1 + s1, d2 + s2, d3 + s3, o4, s3 - d3, s2 - d2, s1 - d1]
    d, a = R2 * (c[2] - c[6]), R2 * (s[2] + s[6])
    eo = [c[2] + c[6], d + a, s[2] - s[6], a - d]
    p0, p1 = c[0] + c[8], c[0] - c[8]
    ee = [p0 + c[4], p1 + s[4], p0 - c[4], p1 - s[4]]
    e = [ee[u] + eo[u] for u in range(4)] + [ee[u] - eo[u] for u in range(4)]
    return [e[u] + o[u] for u in range(8)] + [e[u] - o[u] for u in range(8)]


def convolve_x(f, table):
    keys, _, _ = x_basis()
    row = {key: k for k, key in enumerate(keys)}
    place = {(x % 3, x % 16): x for x in range(NG)}
    part = {"A": [], "c": [], "s": []}
    for u in range(16):
        f0, f1, f2 = (f[place[t, u]] for t in range(3))
        a = f1 + f2
        part["A"].append(f0 + a)
        part["c"].append(f0 - 0.5 * a)
        part["s"].append(S3 * (f1 - f2))
    c, s = t16(part["A"])
    c = {b: v * table(row["A", "C", b]) for b, v in c.items()}
    s = {b: v * table(row["A", "S", b]) for b, v in s.items()}
    back_a = t16_back(c, s)
    cc, cs = t16(part["c"])
    sc, ss = t16(part["s"])
    for b in (0, 8):
        cc[b] = cc[b] * table(row["c", "C", b])
        sc[b] = sc[b] * table(row["s", "C", b])
    for b in range(1, 8):
        p = (cc[b] - ss[b]) * table(row["cos", 1, b])
        m = (cc[b] + ss[b]) * table(row["cos", -1, b])
        cc[b], ss[b] = p + m, m - p
        p = (sc[b] + cs[b]) * table(row["sin", 1, b])
        m = (sc[b] - cs[b]) * table(row["sin", -1, b])
        sc[b], cs[b] = p + m, p - m
    back_c, back_s = t16_back(cc, cs), t16_back(sc, ss)
    out = [None] * NG
    for u in range(16):
        a, c_, s_ = back_a[u], back_c[u], S3 * back_s[u]
        h = a - 0.5 * c_
        out[place[0, u]] = a + c_
        out[place[1, u]] = h + s_
        out[place[2, u]] = h - s_
    return out


def solve_kernel(q_ref, own, two, one, low_a, low_b, core, kern, third, whi_hbm, wlo_hbm, near0, near2, cross, low0, low2,
                 right, left, hi, lo, field, whi, wlo, sems):
    q = q_ref[0]
    copies = []
    for way in range(2):
        part = pl.ds(2 * way, 2)
        copies.append([pltpu.make_async_copy(whi_hbm.at[part], whi.at[part], sems.at[2 * way]),
                       pltpu.make_async_copy(wlo_hbm.at[part], wlo.at[part], sems.at[2 * way + 1])])
        for copy in copies[-1]:
            copy.start()
    sources = (
        (own, 0, low_a, 0),
        (one, 0, core, 4),
        (two, 0, low_b, 0),
        (core, 0, core, 6),
    )
    for delta, (bands_ref, first, low_ref, low_first) in enumerate(sources):
        base = (q ^ delta) * QX

        def place(x, carry):
            span = pl.ds(pl.multiple_of(x * PLANE, 128), PLANE)
            bands = bands_ref[first : first + 4, span]
            right[base + x, 0:4, :] = bands
            right[base + x, 4:8, :] = bands
            left[base + x, 0:4, :] = jnp.broadcast_to(bands_ref[pl.ds(first + q, 1), span], (4, PLANE))
            left[base + x, 4:8, :] = jnp.broadcast_to(low_ref[pl.ds(low_first + q % 2, 1), span], (4, PLANE))
            return carry

        lax.fori_loop(0, QX, place, 0)

    def split(rows, m, value):
        top = value.astype(BF16)
        span = slice(m * SLAB, (m + 1) * SLAB)
        hi[rows, span] = top
        lo[rows, span] = (value - top.astype(F32)).astype(BF16)

    def densities(i, carry):
        x = pl.ds(2 * i, 2)
        rows = pl.ds(pl.multiple_of(16 * i, 16), 16)
        f = []
        for m in range(3):
            span = slice(m * SLAB, (m + 1) * SLAB)
            f.append((right[x, :, span] * left[x, :, span]).reshape(16, SLAB))
        split(rows, 0, f[0] + f[1] + f[2])
        split(rows, 1, f[0] * third[0:1, :] + f[1] * third[1:2, :] + f[2] * third[2:3, :])
        split(rows, 2, f[0] * third[3:4, :] + f[1] * third[4:5, :] + f[2] * third[5:6, :])
        return carry

    lax.fori_loop(0, NG // 2, densities, 0)

    def product(m, k, cols):
        span = slice(m * SLAB, (m + 1) * SLAB)
        a, b = hi[:, span], lo[:, span]
        lhs = jnp.concatenate([a, b, a], axis=1)
        w = jnp.concatenate([whi[k, :, cols], whi[k, :, cols], wlo[k, :, cols]], axis=0)
        return jnp.dot(lhs, w, preferred_element_type=F32)

    for copy in copies[0]:
        copy.wait()
    for j in range(3):
        cols = slice(j * 256, (j + 1) * 256)
        field[:, cols] = product(0, 0, cols)
        c = product(1, 0, cols)
        s = product(2, 1, cols)
        field[:, SLAB + j * 256 : SLAB + (j + 1) * 256] = c - s
        field[:, 2 * SLAB + j * 256 : 2 * SLAB + (j + 1) * 256] = c + s

    def along_x(i, carry):
        span = pl.ds(pl.multiple_of(128 * i, 128), 128)
        f = [field[8 * x : 8 * x + 8, span] for x in range(NG)]
        out = convolve_x(f, lambda k: kern[k : k + 1, span])
        for x in range(NG):
            field[8 * x : 8 * x + 8, span] = out[x]
        return carry

    lax.fori_loop(0, PLANE // 128, along_x, 0)

    def unmix(i, carry):
        rows = pl.ds(pl.multiple_of(16 * i, 16), 16)
        u = field[rows, SLAB : 2 * SLAB]
        v = field[rows, 2 * SLAB : 3 * SLAB]
        split(rows, 0, field[rows, 0:SLAB])
        split(rows, 1, u + v)
        split(rows, 2, v - u)
        return carry

    lax.fori_loop(0, NG // 2, unmix, 0)
    for copy in copies[1]:
        copy.wait()
    for j in range(3):
        cols = slice(j * 256, (j + 1) * 256)
        for m, k in ((0, 2), (1, 2), (2, 3)):
            field[:, m * SLAB + j * 256 : m * SLAB + (j + 1) * 256] = product(m, k, cols)

    mine = (lax.broadcasted_iota(jnp.int32, (8, SLAB), 0) == q).astype(F32)

    for delta in range(4):
        base = (q ^ delta) * QX

        def finish(i, carry):
            x = base + i
            rows = pl.ds(pl.multiple_of(x * 8, 8), 8)
            a = field[rows, 0:SLAB]
            c = field[rows, SLAB : 2 * SLAB]
            s = field[rows, 2 * SLAB : 3 * SLAB]
            for m in range(3):
                span = slice(m * SLAB, (m + 1) * SLAB)
                v = a + c * third[m : m + 1, :] + s * third[3 + m : 4 + m, :]
                pr = v * right[x, :, span]
                pr = pr + pltpu.roll(pr, 6, 0)
                pr = pr + pltpu.roll(pr, 7, 0)
                po = pltpu.roll(v * left[x, :, span], 4, 0) + mine * pr[0:1, :]
                at = pl.ds(pl.multiple_of(i * PLANE + m * SLAB, SLAB), SLAB)
                bands, low = -po[0:4, :], -pr[4:5, :]
                if delta % 2:
                    cross[delta // 2 * 4 : delta // 2 * 4 + 4, at] = bands
                    cross[8 + delta // 2 : 9 + delta // 2, at] = low
                else:
                    (near0, near2)[delta // 2][:, at] = bands
                    (low0, low2)[delta // 2][:, at] = low
            return carry

        lax.fori_loop(0, QX, finish, 0)


def solve_pairs(q, bands, tables):
    vmem = pl.BlockSpec(memory_space=pltpu.VMEM)
    return pl.pallas_call(
        solve_kernel,
        out_shape=[jax.ShapeDtypeStruct(shape, F32) for shape in [(4, QCELL)] * 2 + [(10, QCELL)] + [(1, QCELL)] * 2],
        in_specs=[pl.BlockSpec(memory_space=pltpu.SMEM)] + [vmem] * 8 + [pl.BlockSpec(memory_space=pltpu.HBM)] * 2,
        out_specs=[vmem] * 5,
        scratch_shapes=[
            pltpu.VMEM((NG, 8, PLANE), F32),
            pltpu.VMEM((NG, 8, PLANE), F32),
            pltpu.VMEM((NG * 8, PLANE), BF16),
            pltpu.VMEM((NG * 8, PLANE), BF16),
            pltpu.VMEM((NG * 8, PLANE), F32),
            pltpu.VMEM((4, SLAB, SLAB), BF16),
            pltpu.VMEM((4, SLAB, SLAB), BF16),
            pltpu.SemaphoreType.DMA((4,)),
        ],
        name="solve_pairs",
        compiler_params=pltpu.CompilerParams(vmem_limit_bytes=40 << 20),
    )(q.reshape(1), *bands, jnp.asarray(kernel_values()), jnp.asarray(thirds()), *tables)


BOTH = ("band", "grid")
CHUNK = QCELL // 4


def small_call(body, outs, scratch=(), limit=8):
    vmem = pl.BlockSpec(memory_space=pltpu.VMEM)

    def call(where, *arrays):
        return pl.pallas_call(
            body,
            out_shape=[jax.ShapeDtypeStruct(shape, F32) for shape in outs],
            in_specs=[pl.BlockSpec(memory_space=pltpu.SMEM)] + [vmem] * len(arrays),
            out_specs=[vmem] * len(outs),
            scratch_shapes=list(scratch),
            compiler_params=pltpu.CompilerParams(vmem_limit_bytes=limit << 20),
        )(where, *arrays)

    return call


def chunk_of(where, k):
    return pl.ds(pl.multiple_of((where[1] ^ k) * CHUNK, 128), CHUNK)


def prepare_kernel(where, orbitals, sel_a, sel_b, *chunks):
    lower = where[0] < 2
    a, b = orbitals[0:2, :], orbitals[2:4, :]
    sel_a[...] = jnp.where(lower, a, b)
    sel_b[...] = jnp.where(lower, b, a)
    for k in range(4):
        chunks[k][...] = orbitals[:, chunk_of(where, k)]


def stack_kernel(where, two, low_a, low_b, out):
    out[0:4, :] = two[...]
    out[4:6, :] = low_a[...]
    out[6:8, :] = low_b[...]


def merge_kernel(where, near0, near2, low0, low2, across, near, far, owed_a, owed_b):
    first = where[0] % 2 == 0
    near[...] = near0[...] + across[0:4, :]
    far[...] = near2[...] + across[4:8, :]
    for out, low, row in ((owed_a, low0, 8), (owed_b, low2, 9)):
        a, b = low[...], across[row : row + 1, :]
        out[0:1, :] = jnp.where(first, a, b)
        out[1:2, :] = jnp.where(first, b, a)


def finalize_kernel(where, near, far, owed_a, owed_b, vectors, *chunks):
    lower = where[0] < 2
    a, b = owed_a[...], owed_b[...]
    total = near[...] + far[...]
    vectors[0:2, :] = total[0:2, :] + jnp.where(lower, a, b)
    vectors[2:4, :] = total[2:4, :] + jnp.where(lower, b, a)
    for k in range(4):
        chunks[k][...] = vectors[:, chunk_of(where, k)]


def margin_kernel(where, gathered, v0, v1, v2, v3, m01, m23, block):
    z = where[1]

    def halves(a):
        top = a.astype(BF16)
        return top, (a - top.astype(F32)).astype(BF16)

    vt, vl = halves(jnp.concatenate([v0[...], v1[...], v2[...], v3[...]], axis=0))
    ft, fl = halves(gathered[...])
    dims = (((1,), (1,)), ((), ()))
    got = (
        lax.dot_general(ft, vt, dims, preferred_element_type=F32)
        + lax.dot_general(fl, vt, dims, preferred_element_type=F32)
        + lax.dot_general(ft, vl, dims, preferred_element_type=F32)
    )
    for m in range(8):
        for dz in range(4):
            row = 16 * m + 4 * dz
            block[(z ^ dz) * 8 + m, :, :] = got[row : row + 4, :]
    out = jnp.concatenate([block[i] for i in range(32)], axis=0).T * (1.0 / NCELL)
    m01[...] = out[0:8, :]
    m23[...] = out[8:16, :]


def move(value, target):
    nb, nq = lax.axis_size("band"), lax.axis_size("grid")
    pairs = []
    for b in range(nb):
        for q in range(nq):
            z, y, h, q_to = target(b // 8, b // 2 % 4, b % 2, q)
            pairs.append((b * nq + q, ((z % 4) * 8 + (y % 4) * 2 + h) * nq + q_to))
    return lax.ppermute(value, BOTH, pairs)


def along_z(value, flip):
    return move(value, lambda z, y, h, q: (z ^ flip, y, h, q))


def within(value, flip):
    return move(value, lambda z, y, h, q: (z, y, h, q ^ flip))


def around(value, blocks, flip):
    def target(z, y, h, q):
        b = (z * 8 + y * 2 + h + blocks) % 32
        return b // 8, b // 2 % 4, b % 2, q ^ flip

    return move(value, target)


def step(orbitals):
    b = lax.axis_index("band").astype(jnp.int32)
    q = lax.axis_index("grid").astype(jnp.int32)
    where = jnp.stack([q, b // 8])
    two = within(orbitals, 2)
    prepare = small_call(prepare_kernel, [(2, QCELL)] * 2 + [(4, CHUNK)] * 4)
    sel_a, sel_b, *zc = prepare(where, orbitals)
    low_a = around(sel_a, 1, 0)
    low_b = around(sel_b, 1, 2)
    one = within(orbitals, 1)
    pieces = [zc[0]] + [along_z(zc[k], k) for k in (1, 2, 3)]
    tables = plane_tables()
    together = jnp.concatenate(pieces, axis=0)
    groups = [[z * 8 + i for i in range(8)] for z in range(4)]
    gathered = lax.all_gather(together, "band", axis_index_groups=groups, axis=0, tiled=True)
    two, together = lax.optimization_barrier((two, together))
    (stacked,) = small_call(stack_kernel, [(8, QCELL)])(where, two, low_a, low_b)
    core = within(stacked, 1)
    near0, near2, cross, low0, low2 = solve_pairs(q, (orbitals, two, one, low_a, low_b, core), tables)
    across = within(cross, 1)
    merge = small_call(merge_kernel, [(4, QCELL)] * 2 + [(2, QCELL)] * 2)
    near, both, owe_a, owe_b = merge(where, near0, near2, low0, low2, across)
    far = within(both, 2)
    owed_a = around(owe_a, -1, 0)
    owed_b = around(owe_b, -1, 2)
    finalize = small_call(finalize_kernel, [(4, QCELL)] + [(4, CHUNK)] * 4)
    vectors, *vc = finalize(where, near, far, owed_a, owed_b)
    given = [vc[0]] + [along_z(vc[k], k) for k in (1, 2, 3)]
    gathered, _ = lax.optimization_barrier((gathered, vc[0]))
    margin_part = small_call(margin_kernel, [(8, 128)] * 2, [pltpu.VMEM((32, 4, 16), F32)], 20)
    m01, m23 = margin_part(where, gathered, *given)
    m01 = m01 + along_z(m23, 2)
    mine = m01[0:4] + along_z(m01[4:8], 1)
    mine = mine + within(mine, 1)
    mine = mine + within(mine, 2)
    margin = lax.dynamic_slice_in_dim(mine, q * 32, 32, 1).T
    return vectors, margin


def solution(mesh):
    return jax.shard_map(
        step,
        mesh=mesh,
        in_specs=(P("band", "grid"),),
        out_specs=(P("band", "grid"), P("grid", "band")),
        check_vma=False,
    )
```

```python
import math

import jax
import jax.numpy as jnp
import numpy as np
from jax import lax
from jax.experimental import pallas as pl
from jax.experimental.pallas import tpu as pltpu
from jax.sharding import PartitionSpec as P

NG = 48
NCELL = 110592
PLANE = NG * NG
SLAB = 768
QX = 12
QCELL = QX * PLANE
F32 = jnp.float32
BF16 = jnp.bfloat16
R2 = math.sqrt(0.5)
C1 = math.cos(math.pi / 8)
C3 = math.cos(3 * math.pi / 8)
S3 = math.sqrt(3.0) / 2

ORDER = [("C", b) for b in range(9)] + [("S", b) for b in range(1, 8)]
SWAPPED = [("C", 0)] + [("S", b) for b in range(1, 8)] + [("C", 8)] + [("C", b) for b in range(1, 8)]


def sixteen(order):
    u = np.arange(16)
    cols = []
    for kind, b in order:
        col = np.cos(2 * np.pi * b * u / 16) if kind == "C" else np.sin(2 * np.pi * b * u / 16)
        cols.append(col / np.linalg.norm(col))
    return np.stack(cols, 1)


def forty_eight():
    z = np.arange(NG)
    cols, freqs = [], []
    for g in range(25):
        for kind in ("C", "S") if 0 < g < 24 else ("C",):
            col = np.cos(2 * np.pi * g * z / NG) if kind == "C" else np.sin(2 * np.pi * g * z / NG)
            cols.append(col / np.linalg.norm(col))
            freqs.append(g)
    return np.stack(cols, 1), np.array(freqs)


def folded(g):
    return (g + 24) % 48 - 24


def x_basis():
    keys, freqs, norms = [], [], []
    for b in range(9):
        keys.append(("A", "C", b)); freqs.append(3 * b); norms.append(48 if b in (0, 8) else 24)
    for b in range(1, 8):
        keys.append(("A", "S", b)); freqs.append(3 * b); norms.append(24)
    for b in (0, 8):
        for t in "cs":
            keys.append((t, "C", b)); freqs.append(16 + 3 * b); norms.append(24)
    for b in range(1, 8):
        for sign in (1, -1):
            for kind in ("cos", "sin"):
                keys.append((kind, sign, b)); freqs.append(16 + 3 * sign * b); norms.append(24)
    return keys, np.array(freqs), np.array(norms)


def kernel_values():
    _, gx, nx = x_basis()
    _, gz = forty_eight()
    gy = []
    for slab in "Auv":
        for kind, b in ORDER:
            if slab == "A":
                gy.append(3 * b)
            elif b in (0, 8):
                gy.append(16 + 3 * b)
            else:
                plus = (slab == "u") == (kind == "C")
                gy.append(16 + 3 * b if plus else 16 - 3 * b)
    gy = np.array(gy)
    q = (folded(gx)[:, None, None] ** 2 + folded(gy)[None, :, None] ** 2 + folded(gz)[None, None, :] ** 2).astype(np.float64)
    kern = np.where(q > 0, 40.0 * (1.0 - np.exp(-q / 16.0)) / np.where(q > 0, q, 1.0), 0.0)
    return (kern / (3.0 * nx[:, None, None])).reshape(NG, PLANE).astype(np.float32)


def thirds():
    u = np.arange(SLAB) // NG
    rows = [np.cos(2 * np.pi * (m + u) / 3) for m in range(3)] + [np.sin(2 * np.pi * (m + u) / 3) for m in range(3)]
    return np.concatenate([np.stack(rows), np.zeros((2, SLAB))]).astype(np.float32)


def factor_tables():
    za, _ = forty_eight()
    ta, ts = sixteen(ORDER), sixteen(SWAPPED)
    tens = np.stack([np.repeat(t, NG, 1) for t in (ta, ts, ta.T, ts.T)])
    zs = np.stack([np.tile(z, (1, 16)) for z in (za, za.T)])
    return [a.astype(np.float32) for a in (tens, zs)]


def tables_kernel(tens, zs, hi_there, lo_there, hi_back, lo_back):
    for way, (hi, lo) in enumerate(((hi_there, lo_there), (hi_back, lo_back))):
        for which in range(2):

            def block(u, carry):
                w = zs[way] * tens[2 * way + which, pl.ds(u, 1), :]
                top = w.astype(BF16)
                rows = pl.ds(pl.multiple_of(u * NG, 16), NG)
                hi[which, rows, :] = top
                lo[which, rows, :] = (w - top.astype(F32)).astype(BF16)
                return carry

            lax.fori_loop(0, 16, block, 0)


def plane_tables():
    out = [jax.ShapeDtypeStruct((2, SLAB, SLAB), BF16)] * 4
    return pl.pallas_call(
        tables_kernel, out_shape=out, name="plane_tables",
        compiler_params=pltpu.CompilerParams(vmem_limit_bytes=16 << 20),
    )(*[jnp.asarray(a) for a in factor_tables()])


def t16(f):
    o = [f[u] - f[u + 8] for u in range(8)]
    e = [f[u] + f[u + 8] for u in range(8)]
    ee = [e[u] + e[u + 4] for u in range(4)]
    eo = [e[u] - e[u + 4] for u in range(4)]
    c, s = {}, {}
    p0, p1 = ee[0] + ee[2], ee[1] + ee[3]
    c[0], c[8], c[4], s[4] = p0 + p1, p0 - p1, ee[0] - ee[2], ee[1] - ee[3]
    d, a = R2 * (eo[1] - eo[3]), R2 * (eo[1] + eo[3])
    c[2], c[6], s[2], s[6] = eo[0] + d, eo[0] - d, a + eo[2], a - eo[2]
    d1, d2, d3 = (o[u] - o[8 - u] for u in (1, 2, 3))
    s1, s2, s3 = (o[u] + o[8 - u] for u in (1, 2, 3))
    d2, s2 = R2 * d2, R2 * s2
    e1, e3 = o[0] + d2, o[0] - d2
    o1, o3 = C1 * d1 + C3 * d3, C3 * d1 - C1 * d3
    c[1], c[7], c[3], c[5] = e1 + o1, e1 - o1, e3 + o3, e3 - o3
    x1, x3 = o[4] + s2, o[4] - s2
    y1, y3 = C3 * s1 + C1 * s3, C1 * s1 - C3 * s3
    s[1], s[7], s[3], s[5] = y1 + x1, y1 - x1, y3 - x3, y3 + x3
    return c, s


def t16_back(c, s):
    e1, o1, e3, o3 = c[1] + c[7], c[1] - c[7], c[3] + c[5], c[3] - c[5]
    o0, d2 = e1 + e3, R2 * (e1 - e3)
    d1, d3 = C1 * o1 + C3 * o3, C3 * o1 - C1 * o3
    y1, x1, y3, x3 = s[1] + s[7], s[1] - s[7], s[3] + s[5], s[5] - s[3]
    o4, s2 = x1 + x3, R2 * (x1 - x3)
    s1, s3 = C3 * y1 + C1 * y3, C1 * y1 - C3 * y3
    o = [o0, d1 + s1, d2 + s2, d3 + s3, o4, s3 - d3, s2 - d2, s1 - d1]
    d, a = R2 * (c[2] - c[6]), R2 * (s[2] + s[6])
    eo = [c[2] + c[6], d + a, s[2] - s[6], a - d]
    p0, p1 = c[0] + c[8], c[0] - c[8]
    ee = [p0 + c[4], p1 + s[4], p0 - c[4], p1 - s[4]]
    e = [ee[u] + eo[u] for u in range(4)] + [ee[u] - eo[u] for u in range(4)]
    return [e[u] + o[u] for u in range(8)] + [e[u] - o[u] for u in range(8)]


def convolve_x(f, table):
    keys, _, _ = x_basis()
    row = {key: k for k, key in enumerate(keys)}
    place = {(x % 3, x % 16): x for x in range(NG)}
    part = {"A": [], "c": [], "s": []}
    for u in range(16):
        f0, f1, f2 = (f[place[t, u]] for t in range(3))
        a = f1 + f2
        part["A"].append(f0 + a)
        part["c"].append(f0 - 0.5 * a)
        part["s"].append(S3 * (f1 - f2))
    c, s = t16(part["A"])
    c = {b: v * table(row["A", "C", b]) for b, v in c.items()}
    s = {b: v * table(row["A", "S", b]) for b, v in s.items()}
    back_a = t16_back(c, s)
    cc, cs = t16(part["c"])
    sc, ss = t16(part["s"])
    for b in (0, 8):
        cc[b] = cc[b] * table(row["c", "C", b])
        sc[b] = sc[b] * table(row["s", "C", b])
    for b in range(1, 8):
        p = (cc[b] - ss[b]) * table(row["cos", 1, b])
        m = (cc[b] + ss[b]) * table(row["cos", -1, b])
        cc[b], ss[b] = p + m, m - p
        p = (sc[b] + cs[b]) * table(row["sin", 1, b])
        m = (sc[b] - cs[b]) * table(row["sin", -1, b])
        sc[b], cs[b] = p + m, p - m
    back_c, back_s = t16_back(cc, cs), t16_back(sc, ss)
    out = [None] * NG
    for u in range(16):
        a, c_, s_ = back_a[u], back_c[u], S3 * back_s[u]
        h = a - 0.5 * c_
        out[place[0, u]] = a + c_
        out[place[1, u]] = h + s_
        out[place[2, u]] = h - s_
    return out


def split(hi, lo, rows, m, value):
    top = value.astype(BF16)
    span = slice(m * SLAB, (m + 1) * SLAB)
    hi[rows, span] = top
    lo[rows, span] = (value - top.astype(F32)).astype(BF16)


def product(hi, lo, whi, wlo, m, k, cols):
    span = slice(m * SLAB, (m + 1) * SLAB)
    a, b = hi[:, span], lo[:, span]
    lhs = jnp.concatenate([a, b, a], axis=1)
    w = jnp.concatenate([whi[k, :, cols], whi[k, :, cols], wlo[k, :, cols]], axis=0)
    return jnp.dot(lhs, w, preferred_element_type=F32)


def spectrum_kernel(q_ref, own, two, one, low_a, low_b, core, kern, third, whi, wlo, right, left, field, hi, lo):
    q = q_ref[0]
    sources = (
        (own, 0, low_a, 0),
        (one, 0, core, 4),
        (two, 0, low_b, 0),
        (core, 0, core, 6),
    )
    for delta, (bands_ref, first, low_ref, low_first) in enumerate(sources):
        base = (q ^ delta) * QX

        def place(x, carry):
            span = pl.ds(pl.multiple_of(x * PLANE, 128), PLANE)
            bands = bands_ref[first : first + 4, span]
            right[base + x, 0:4, :] = bands
            right[base + x, 4:8, :] = bands
            left[base + x, 0:4, :] = jnp.broadcast_to(bands_ref[pl.ds(first + q, 1), span], (4, PLANE))
            left[base + x, 4:8, :] = jnp.broadcast_to(low_ref[pl.ds(low_first + q % 2, 1), span], (4, PLANE))
            return carry

        lax.fori_loop(0, QX, place, 0)

    def densities(i, carry):
        x = pl.ds(2 * i, 2)
        rows = pl.ds(pl.multiple_of(16 * i, 16), 16)
        f = []
        for m in range(3):
            span = slice(m * SLAB, (m + 1) * SLAB)
            f.append((right[x, :, span] * left[x, :, span]).reshape(16, SLAB))
        split(hi, lo, rows, 0, f[0] + f[1] + f[2])
        split(hi, lo, rows, 1, f[0] * third[0:1, :] + f[1] * third[1:2, :] + f[2] * third[2:3, :])
        split(hi, lo, rows, 2, f[0] * third[3:4, :] + f[1] * third[4:5, :] + f[2] * third[5:6, :])
        return carry

    lax.fori_loop(0, NG // 2, densities, 0)

    for j in range(3):
        cols = slice(j * 256, (j + 1) * 256)
        field[:, cols] = product(hi, lo, whi, wlo, 0, 0, cols)
        c = product(hi, lo, whi, wlo, 1, 0, cols)
        s = product(hi, lo, whi, wlo, 2, 1, cols)
        field[:, SLAB + j * 256 : SLAB + (j + 1) * 256] = c - s
        field[:, 2 * SLAB + j * 256 : 2 * SLAB + (j + 1) * 256] = c + s

    def along_x(i, carry):
        span = pl.ds(pl.multiple_of(128 * i, 128), 128)
        f = [field[8 * x : 8 * x + 8, span] for x in range(NG)]
        out = convolve_x(f, lambda k: kern[k : k + 1, span])
        for x in range(NG):
            field[8 * x : 8 * x + 8, span] = out[x]
        return carry

    lax.fori_loop(0, PLANE // 128, along_x, 0)


def terms_kernel(q_ref, right, left, field, third, whi, wlo, near0, near2, cross, low0, low2, hi, lo, back):
    q = q_ref[0]

    def unmix(i, carry):
        rows = pl.ds(pl.multiple_of(16 * i, 16), 16)
        u = field[rows, SLAB : 2 * SLAB]
        v = field[rows, 2 * SLAB : 3 * SLAB]
        split(hi, lo, rows, 0, field[rows, 0:SLAB])
        split(hi, lo, rows, 1, u + v)
        split(hi, lo, rows, 2, v - u)
        return carry

    lax.fori_loop(0, NG // 2, unmix, 0)
    for j in range(3):
        cols = slice(j * 256, (j + 1) * 256)
        for m, k in ((0, 0), (1, 0), (2, 1)):
            back[:, m * SLAB + j * 256 : m * SLAB + (j + 1) * 256] = product(hi, lo, whi, wlo, m, k, cols)

    mine = (lax.broadcasted_iota(jnp.int32, (8, SLAB), 0) == q).astype(F32)

    for delta in range(4):
        base = (q ^ delta) * QX

        def finish(i, carry):
            x = base + i
            rows = pl.ds(pl.multiple_of(x * 8, 8), 8)
            a = back[rows, 0:SLAB]
            c = back[rows, SLAB : 2 * SLAB]
            s = back[rows, 2 * SLAB : 3 * SLAB]
            for m in range(3):
                span = slice(m * SLAB, (m + 1) * SLAB)
                v = a + c * third[m : m + 1, :] + s * third[3 + m : 4 + m, :]
                pr = v * right[x, :, span]
                pr = pr + pltpu.roll(pr, 6, 0)
                pr = pr + pltpu.roll(pr, 7, 0)
                po = pltpu.roll(v * left[x, :, span], 4, 0) + mine * pr[0:1, :]
                at = pl.ds(pl.multiple_of(i * PLANE + m * SLAB, SLAB), SLAB)
                bands, low = -po[0:4, :], -pr[4:5, :]
                if delta % 2:
                    cross[delta // 2 * 4 : delta // 2 * 4 + 4, at] = bands
                    cross[8 + delta // 2 : 9 + delta // 2, at] = low
                else:
                    (near0, near2)[delta // 2][:, at] = bands
                    (low0, low2)[delta // 2][:, at] = low
            return carry

        lax.fori_loop(0, QX, finish, 0)


VMEM_SPEC = pl.BlockSpec(memory_space=pltpu.VMEM)
SMEM_SPEC = pl.BlockSpec(memory_space=pltpu.SMEM)
SPLIT = [pltpu.VMEM((NG * 8, PLANE), BF16)] * 2


def spectrum(q, bands, tables):
    return pl.pallas_call(
        spectrum_kernel,
        out_shape=[jax.ShapeDtypeStruct((NG, 8, PLANE), F32)] * 2 + [jax.ShapeDtypeStruct((NG * 8, PLANE), F32)],
        in_specs=[SMEM_SPEC] + [VMEM_SPEC] * 10,
        out_specs=[VMEM_SPEC] * 3,
        scratch_shapes=SPLIT,
        name="spectrum",
        compiler_params=pltpu.CompilerParams(vmem_limit_bytes=24 << 20),
    )(q.reshape(1), *bands, jnp.asarray(kernel_values()), jnp.asarray(thirds()), *tables)


def terms(q, right, left, field, tables):
    return pl.pallas_call(
        terms_kernel,
        out_shape=[jax.ShapeDtypeStruct(shape, F32) for shape in [(4, QCELL)] * 2 + [(10, QCELL)] + [(1, QCELL)] * 2],
        in_specs=[SMEM_SPEC] + [VMEM_SPEC] * 6,
        out_specs=[VMEM_SPEC] * 5,
        scratch_shapes=SPLIT + [pltpu.VMEM((NG * 8, PLANE), F32)],
        name="terms",
        compiler_params=pltpu.CompilerParams(vmem_limit_bytes=28 << 20),
    )(q.reshape(1), right, left, field, jnp.asarray(thirds()), *tables)


BOTH = ("band", "grid")
CHUNK = QCELL // 4


def small_call(body, outs, scratch=(), limit=8):
    vmem = pl.BlockSpec(memory_space=pltpu.VMEM)

    def call(where, *arrays):
        return pl.pallas_call(
            body,
            out_shape=[jax.ShapeDtypeStruct(shape, F32) for shape in outs],
            in_specs=[pl.BlockSpec(memory_space=pltpu.SMEM)] + [vmem] * len(arrays),
            out_specs=[vmem] * len(outs),
            scratch_shapes=list(scratch),
            compiler_params=pltpu.CompilerParams(vmem_limit_bytes=limit << 20),
        )(where, *arrays)

    return call


def chunk_of(where, k):
    return pl.ds(pl.multiple_of((where[1] ^ k) * CHUNK, 128), CHUNK)


def prepare_kernel(where, orbitals, sel_a, sel_b, *chunks):
    lower = where[0] < 2
    a, b = orbitals[0:2, :], orbitals[2:4, :]
    sel_a[...] = jnp.where(lower, a, b)
    sel_b[...] = jnp.where(lower, b, a)
    for k in range(4):
        chunks[k][...] = orbitals[:, chunk_of(where, k)]


def stack_kernel(where, two, low_a, low_b, out):
    out[0:4, :] = two[...]
    out[4:6, :] = low_a[...]
    out[6:8, :] = low_b[...]


def merge_kernel(where, near0, near2, low0, low2, across, near, far, owed_a, owed_b):
    first = where[0] % 2 == 0
    near[...] = near0[...] + across[0:4, :]
    far[...] = near2[...] + across[4:8, :]
    for out, low, row in ((owed_a, low0, 8), (owed_b, low2, 9)):
        a, b = low[...], across[row : row + 1, :]
        out[0:1, :] = jnp.where(first, a, b)
        out[1:2, :] = jnp.where(first, b, a)


def finalize_kernel(where, near, far, owed_a, owed_b, vectors, *chunks):
    lower = where[0] < 2
    a, b = owed_a[...], owed_b[...]
    total = near[...] + far[...]
    vectors[0:2, :] = total[0:2, :] + jnp.where(lower, a, b)
    vectors[2:4, :] = total[2:4, :] + jnp.where(lower, b, a)
    for k in range(4):
        chunks[k][...] = vectors[:, chunk_of(where, k)]


def pair_kernel(where, f0, f1, f2, f3, other, out):
    first = where[3] == 0
    for k, f in enumerate((f0, f1, f2, f3)):
        a, b = f[...], other[4 * k : 4 * k + 4, :]
        out[8 * k : 8 * k + 4, :] = jnp.where(first, a, b)
        out[8 * k + 4 : 8 * k + 8, :] = jnp.where(first, b, a)


def margin_kernel(where, p0, p1, p3, p2a, p2b, v0, v1, v2, v3, m01, m23, block):
    z, y = where[1], where[2]

    def halves(a):
        top = a.astype(BF16)
        return top, (a - top.astype(F32)).astype(BF16)

    vt, vl = halves(jnp.concatenate([v0[...], v1[...], v2[...], v3[...]], axis=0))
    dims = (((1,), (1,)), ((), ()))
    parts = jnp.concatenate([p0[...], p1[...], p2a[...], p2b[...], p3[...]], axis=0)
    ft, fl = halves(parts)
    got = (
        lax.dot_general(ft, vt, dims, preferred_element_type=F32)
        + lax.dot_general(fl, vt, dims, preferred_element_type=F32)
        + lax.dot_general(ft, vl, dims, preferred_element_type=F32)
    )
    for dy in range(4):
        for dz in range(4):
            row = 32 * dy + 8 * dz
            block[(z ^ dz) * 4 + (y + 4 - dy) % 4, :, :] = got[row : row + 8, :]
    out = block[...].reshape(128, 16).T * (1.0 / NCELL)
    m01[...] = out[0:8, :]
    m23[...] = out[8:16, :]


def move(value, target):
    nb, nq = lax.axis_size("band"), lax.axis_size("grid")
    pairs = []
    for b in range(nb):
        for q in range(nq):
            z, y, h, q_to = target(b // 8, b // 2 % 4, b % 2, q)
            pairs.append((b * nq + q, ((z % 4) * 8 + (y % 4) * 2 + h) * nq + q_to))
    return lax.ppermute(value, BOTH, pairs)


def along_z(value, flip):
    return move(value, lambda z, y, h, q: (z ^ flip, y, h, q))


def along_y(value, k):
    return move(value, lambda z, y, h, q: (z, y + k, h, q))


def within(value, flip):
    return move(value, lambda z, y, h, q: (z, y, h, q ^ flip))


def around(value, blocks, flip):
    def target(z, y, h, q):
        b = (z * 8 + y * 2 + h + blocks) % 32
        return b // 8, b // 2 % 4, b % 2, q ^ flip

    return move(value, target)


def step(orbitals):
    b = lax.axis_index("band").astype(jnp.int32)
    q = lax.axis_index("grid").astype(jnp.int32)
    where = jnp.stack([q, b // 8, b // 2 % 4, b % 2])
    two = within(orbitals, 2)
    prepare = small_call(prepare_kernel, [(2, QCELL)] * 2 + [(4, CHUNK)] * 4)
    sel_a, sel_b, *zc = prepare(where, orbitals)
    low_a = around(sel_a, 1, 0)
    low_b = around(sel_b, 1, 2)
    one = within(orbitals, 1)
    pieces = [zc[0]] + [along_z(zc[k], k) for k in (1, 2, 3)]
    tables = plane_tables()
    together = jnp.concatenate(pieces, axis=0)
    two, together = lax.optimization_barrier((two, together))
    (stacked,) = small_call(stack_kernel, [(8, QCELL)])(where, two, low_a, low_b)
    core = within(stacked, 1)
    other = move(together, lambda z, y, h, q: (z, y, 1 - h, q))
    right, left, field = spectrum(q, (orbitals, two, one, low_a, low_b, core), tables[:2])
    (p0,) = small_call(pair_kernel, [(32, CHUNK)])(where, *pieces, other)
    p1 = along_y(p0, 1)
    p3 = along_y(p0, 3)
    near0, near2, cross, low0, low2 = terms(q, right, left, field, tables[2:])
    across = within(cross, 1)
    merge = small_call(merge_kernel, [(4, QCELL)] * 2 + [(2, QCELL)] * 2)
    near, both, owe_a, owe_b = merge(where, near0, near2, low0, low2, across)
    far = within(both, 2)
    owed_a = around(owe_a, -1, 0)
    owed_b = around(owe_b, -1, 2)
    p2a = along_y(p1[:16], 1)
    p2b = along_y(p3[16:], 3)
    finalize = small_call(finalize_kernel, [(4, QCELL)] + [(4, CHUNK)] * 4)
    vectors, *vc = finalize(where, near, far, owed_a, owed_b)
    given = [vc[0]] + [along_z(vc[k], k) for k in (1, 2, 3)]
    margin_part = small_call(margin_kernel, [(8, 128)] * 2, [pltpu.VMEM((16, 8, 16), F32)], 20)
    m01, m23 = margin_part(where, p0, p1, p3, p2a, p2b, *given)
    m01 = m01 + along_z(m23, 2)
    mine = m01[0:4] + along_z(m01[4:8], 1)
    mine = mine + within(mine, 1)
    mine = mine + within(mine, 2)
    margin = lax.dynamic_slice_in_dim(mine, q * 32, 32, 1).T
    return vectors, margin


def solution(mesh):
    return jax.shard_map(
        step,
        mesh=mesh,
        in_specs=(P("band", "grid"),),
        out_specs=(P("band", "grid"), P("grid", "band")),
        check_vma=False,
    )
```

```python
import math

import jax
import jax.numpy as jnp
import numpy as np
from jax import lax
from jax.experimental import pallas as pl
from jax.experimental.pallas import tpu as pltpu
from jax.sharding import PartitionSpec as P

NG = 48
NCELL = 110592
PLANE = NG * NG
SLAB = 768
QX = 12
QCELL = QX * PLANE
F32 = jnp.float32
BF16 = jnp.bfloat16
R2 = math.sqrt(0.5)
C1 = math.cos(math.pi / 8)
C3 = math.cos(3 * math.pi / 8)
S3 = math.sqrt(3.0) / 2

ORDER = [("C", b) for b in range(9)] + [("S", b) for b in range(1, 8)]
SWAPPED = [("C", 0)] + [("S", b) for b in range(1, 8)] + [("C", 8)] + [("C", b) for b in range(1, 8)]


def sixteen(order):
    u = np.arange(16)
    cols = []
    for kind, b in order:
        col = np.cos(2 * np.pi * b * u / 16) if kind == "C" else np.sin(2 * np.pi * b * u / 16)
        cols.append(col / np.linalg.norm(col))
    return np.stack(cols, 1)


def forty_eight():
    z = np.arange(NG)
    cols, freqs = [], []
    for g in range(25):
        for kind in ("C", "S") if 0 < g < 24 else ("C",):
            col = np.cos(2 * np.pi * g * z / NG) if kind == "C" else np.sin(2 * np.pi * g * z / NG)
            cols.append(col / np.linalg.norm(col))
            freqs.append(g)
    return np.stack(cols, 1), np.array(freqs)


def folded(g):
    return (g + 24) % 48 - 24


def x_basis():
    keys, freqs, norms = [], [], []
    for b in range(9):
        keys.append(("A", "C", b)); freqs.append(3 * b); norms.append(48 if b in (0, 8) else 24)
    for b in range(1, 8):
        keys.append(("A", "S", b)); freqs.append(3 * b); norms.append(24)
    for b in (0, 8):
        for t in "cs":
            keys.append((t, "C", b)); freqs.append(16 + 3 * b); norms.append(24)
    for b in range(1, 8):
        for sign in (1, -1):
            for kind in ("cos", "sin"):
                keys.append((kind, sign, b)); freqs.append(16 + 3 * sign * b); norms.append(24)
    return keys, np.array(freqs), np.array(norms)


def kernel_values():
    _, gx, nx = x_basis()
    _, gz = forty_eight()
    gy = []
    for slab in "Auv":
        for kind, b in ORDER:
            if slab == "A":
                gy.append(3 * b)
            elif b in (0, 8):
                gy.append(16 + 3 * b)
            else:
                plus = (slab == "u") == (kind == "C")
                gy.append(16 + 3 * b if plus else 16 - 3 * b)
    gy = np.array(gy)
    q = (folded(gx)[:, None, None] ** 2 + folded(gy)[None, :, None] ** 2 + folded(gz)[None, None, :] ** 2).astype(np.float64)
    kern = np.where(q > 0, 40.0 * (1.0 - np.exp(-q / 16.0)) / np.where(q > 0, q, 1.0), 0.0)
    return (kern / (3.0 * nx[:, None, None])).reshape(NG, PLANE).astype(np.float32)


def thirds():
    u = np.arange(SLAB) // NG
    rows = [np.cos(2 * np.pi * (m + u) / 3) for m in range(3)] + [np.sin(2 * np.pi * (m + u) / 3) for m in range(3)]
    return np.concatenate([np.stack(rows), np.zeros((2, SLAB))]).astype(np.float32)


def factor_tables():
    za, _ = forty_eight()
    ta, ts = sixteen(ORDER), sixteen(SWAPPED)
    tens = np.stack([np.repeat(t, NG, 1) for t in (ta, ts, ta.T, ts.T)])
    zs = np.stack([np.tile(z, (1, 16)) for z in (za, za.T)])
    return [a.astype(np.float32) for a in (tens, zs)]


def tables_kernel(tens, zs, hi_there, lo_there, hi_back, lo_back):
    for way, (hi, lo) in enumerate(((hi_there, lo_there), (hi_back, lo_back))):
        for which in range(2):

            def block(u, carry):
                w = zs[way] * tens[2 * way + which, pl.ds(u, 1), :]
                top = w.astype(BF16)
                rows = pl.ds(pl.multiple_of(u * NG, 16), NG)
                hi[which, rows, :] = top
                lo[which, rows, :] = (w - top.astype(F32)).astype(BF16)
                return carry

            lax.fori_loop(0, 16, block, 0)


def plane_tables():
    out = [jax.ShapeDtypeStruct((2, SLAB, SLAB), BF16)] * 4
    return pl.pallas_call(
        tables_kernel, out_shape=out, name="plane_tables",
        compiler_params=pltpu.CompilerParams(vmem_limit_bytes=16 << 20),
    )(*[jnp.asarray(a) for a in factor_tables()])


def t16(f):
    o = [f[u] - f[u + 8] for u in range(8)]
    e = [f[u] + f[u + 8] for u in range(8)]
    ee = [e[u] + e[u + 4] for u in range(4)]
    eo = [e[u] - e[u + 4] for u in range(4)]
    c, s = {}, {}
    p0, p1 = ee[0] + ee[2], ee[1] + ee[3]
    c[0], c[8], c[4], s[4] = p0 + p1, p0 - p1, ee[0] - ee[2], ee[1] - ee[3]
    d, a = R2 * (eo[1] - eo[3]), R2 * (eo[1] + eo[3])
    c[2], c[6], s[2], s[6] = eo[0] + d, eo[0] - d, a + eo[2], a - eo[2]
    d1, d2, d3 = (o[u] - o[8 - u] for u in (1, 2, 3))
    s1, s2, s3 = (o[u] + o[8 - u] for u in (1, 2, 3))
    d2, s2 = R2 * d2, R2 * s2
    e1, e3 = o[0] + d2, o[0] - d2
    o1, o3 = C1 * d1 + C3 * d3, C3 * d1 - C1 * d3
    c[1], c[7], c[3], c[5] = e1 + o1, e1 - o1, e3 + o3, e3 - o3
    x1, x3 = o[4] + s2, o[4] - s2
    y1, y3 = C3 * s1 + C1 * s3, C1 * s1 - C3 * s3
    s[1], s[7], s[3], s[5] = y1 + x1, y1 - x1, y3 - x3, y3 + x3
    return c, s


def t16_back(c, s):
    e1, o1, e3, o3 = c[1] + c[7], c[1] - c[7], c[3] + c[5], c[3] - c[5]
    o0, d2 = e1 + e3, R2 * (e1 - e3)
    d1, d3 = C1 * o1 + C3 * o3, C3 * o1 - C1 * o3
    y1, x1, y3, x3 = s[1] + s[7], s[1] - s[7], s[3] + s[5], s[5] - s[3]
    o4, s2 = x1 + x3, R2 * (x1 - x3)
    s1, s3 = C3 * y1 + C1 * y3, C1 * y1 - C3 * y3
    o = [o0, d1 + s1, d2 + s2, d3 + s3, o4, s3 - d3, s2 - d2, s1 - d1]
    d, a = R2 * (c[2] - c[6]), R2 * (s[2] + s[6])
    eo = [c[2] + c[6], d + a, s[2] - s[6], a - d]
    p0, p1 = c[0] + c[8], c[0] - c[8]
    ee = [p0 + c[4], p1 + s[4], p0 - c[4], p1 - s[4]]
    e = [ee[u] + eo[u] for u in range(4)] + [ee[u] - eo[u] for u in range(4)]
    return [e[u] + o[u] for u in range(8)] + [e[u] - o[u] for u in range(8)]


def convolve_x(f, table):
    keys, _, _ = x_basis()
    row = {key: k for k, key in enumerate(keys)}
    place = {(x % 3, x % 16): x for x in range(NG)}
    part = {"A": [], "c": [], "s": []}
    for u in range(16):
        f0, f1, f2 = (f[place[t, u]] for t in range(3))
        a = f1 + f2
        part["A"].append(f0 + a)
        part["c"].append(f0 - 0.5 * a)
        part["s"].append(S3 * (f1 - f2))
    c, s = t16(part["A"])
    c = {b: v * table(row["A", "C", b]) for b, v in c.items()}
    s = {b: v * table(row["A", "S", b]) for b, v in s.items()}
    back_a = t16_back(c, s)
    cc, cs = t16(part["c"])
    sc, ss = t16(part["s"])
    for b in (0, 8):
        cc[b] = cc[b] * table(row["c", "C", b])
        sc[b] = sc[b] * table(row["s", "C", b])
    for b in range(1, 8):
        p = (cc[b] - ss[b]) * table(row["cos", 1, b])
        m = (cc[b] + ss[b]) * table(row["cos", -1, b])
        cc[b], ss[b] = p + m, m - p
        p = (sc[b] + cs[b]) * table(row["sin", 1, b])
        m = (sc[b] - cs[b]) * table(row["sin", -1, b])
        sc[b], cs[b] = p + m, p - m
    back_c, back_s = t16_back(cc, cs), t16_back(sc, ss)
    out = [None] * NG
    for u in range(16):
        a, c_, s_ = back_a[u], back_c[u], S3 * back_s[u]
        h = a - 0.5 * c_
        out[place[0, u]] = a + c_
        out[place[1, u]] = h + s_
        out[place[2, u]] = h - s_
    return out


def split(hi, lo, rows, m, value):
    top = value.astype(BF16)
    span = slice(m * SLAB, (m + 1) * SLAB)
    hi[rows, span] = top
    lo[rows, span] = (value - top.astype(F32)).astype(BF16)


def product(hi, lo, whi, wlo, m, k, cols):
    span = slice(m * SLAB, (m + 1) * SLAB)
    a, b = hi[:, span], lo[:, span]
    lhs = jnp.concatenate([a, b, a], axis=1)
    w = jnp.concatenate([whi[k, :, cols], whi[k, :, cols], wlo[k, :, cols]], axis=0)
    return jnp.dot(lhs, w, preferred_element_type=F32)


def spectrum_kernel(q_ref, own, two, one, low_a, low_b, core, kern, third, whi, wlo, right, left, field, hi, lo):
    q = q_ref[0]
    sources = (
        (own, 0, low_a, 0),
        (one, 0, core, 4),
        (two, 0, low_b, 0),
        (core, 0, core, 6),
    )
    for delta, (bands_ref, first, low_ref, low_first) in enumerate(sources):
        base = (q ^ delta) * QX

        def place(x, carry):
            span = pl.ds(pl.multiple_of(x * PLANE, 128), PLANE)
            bands = bands_ref[first : first + 4, span]
            right[base + x, 0:4, :] = bands
            right[base + x, 4:8, :] = bands
            left[base + x, 0:4, :] = jnp.broadcast_to(bands_ref[pl.ds(first + q, 1), span], (4, PLANE))
            left[base + x, 4:8, :] = jnp.broadcast_to(low_ref[pl.ds(low_first + q % 2, 1), span], (4, PLANE))
            return carry

        lax.fori_loop(0, QX, place, 0)

    def densities(i, carry):
        x = pl.ds(2 * i, 2)
        rows = pl.ds(pl.multiple_of(16 * i, 16), 16)
        f = []
        for m in range(3):
            span = slice(m * SLAB, (m + 1) * SLAB)
            f.append((right[x, :, span] * left[x, :, span]).reshape(16, SLAB))
        split(hi, lo, rows, 0, f[0] + f[1] + f[2])
        split(hi, lo, rows, 1, f[0] * third[0:1, :] + f[1] * third[1:2, :] + f[2] * third[2:3, :])
        split(hi, lo, rows, 2, f[0] * third[3:4, :] + f[1] * third[4:5, :] + f[2] * third[5:6, :])
        return carry

    lax.fori_loop(0, NG // 2, densities, 0)

    for j in range(3):
        cols = slice(j * 256, (j + 1) * 256)
        field[:, cols] = product(hi, lo, whi, wlo, 0, 0, cols)
        c = product(hi, lo, whi, wlo, 1, 0, cols)
        s = product(hi, lo, whi, wlo, 2, 1, cols)
        field[:, SLAB + j * 256 : SLAB + (j + 1) * 256] = c - s
        field[:, 2 * SLAB + j * 256 : 2 * SLAB + (j + 1) * 256] = c + s

    def along_x(i, carry):
        span = pl.ds(pl.multiple_of(128 * i, 128), 128)
        f = [field[8 * x : 8 * x + 8, span] for x in range(NG)]
        out = convolve_x(f, lambda k: kern[k : k + 1, span])
        for x in range(NG):
            field[8 * x : 8 * x + 8, span] = out[x]
        return carry

    lax.fori_loop(0, PLANE // 128, along_x, 0)


def terms_kernel(q_ref, right, left, field, third, whi, wlo, near0, near2, cross, low0, low2, hi, lo, back):
    q = q_ref[0]

    def unmix(i, carry):
        rows = pl.ds(pl.multiple_of(16 * i, 16), 16)
        u = field[rows, SLAB : 2 * SLAB]
        v = field[rows, 2 * SLAB : 3 * SLAB]
        split(hi, lo, rows, 0, field[rows, 0:SLAB])
        split(hi, lo, rows, 1, u + v)
        split(hi, lo, rows, 2, v - u)
        return carry

    lax.fori_loop(0, NG // 2, unmix, 0)
    for j in range(3):
        cols = slice(j * 256, (j + 1) * 256)
        for m, k in ((0, 0), (1, 0), (2, 1)):
            back[:, m * SLAB + j * 256 : m * SLAB + (j + 1) * 256] = product(hi, lo, whi, wlo, m, k, cols)

    mine = (lax.broadcasted_iota(jnp.int32, (8, SLAB), 0) == q).astype(F32)

    for delta in range(4):
        base = (q ^ delta) * QX

        def finish(i, carry):
            x = base + i
            rows = pl.ds(pl.multiple_of(x * 8, 8), 8)
            a = back[rows, 0:SLAB]
            c = back[rows, SLAB : 2 * SLAB]
            s = back[rows, 2 * SLAB : 3 * SLAB]
            for m in range(3):
                span = slice(m * SLAB, (m + 1) * SLAB)
                v = a + c * third[m : m + 1, :] + s * third[3 + m : 4 + m, :]
                pr = v * right[x, :, span]
                pr = pr + pltpu.roll(pr, 6, 0)
                pr = pr + pltpu.roll(pr, 7, 0)
                po = pltpu.roll(v * left[x, :, span], 4, 0) + mine * pr[0:1, :]
                at = pl.ds(pl.multiple_of(i * PLANE + m * SLAB, SLAB), SLAB)
                bands, low = -po[0:4, :], -pr[4:5, :]
                if delta % 2:
                    cross[delta // 2 * 4 : delta // 2 * 4 + 4, at] = bands
                    cross[8 + delta // 2 : 9 + delta // 2, at] = low
                else:
                    (near0, near2)[delta // 2][:, at] = bands
                    (low0, low2)[delta // 2][:, at] = low
            return carry

        lax.fori_loop(0, QX, finish, 0)


VMEM_SPEC = pl.BlockSpec(memory_space=pltpu.VMEM)
SMEM_SPEC = pl.BlockSpec(memory_space=pltpu.SMEM)
SPLIT = [pltpu.VMEM((NG * 8, PLANE), BF16)] * 2


def spectrum(q, bands, tables):
    return pl.pallas_call(
        spectrum_kernel,
        out_shape=[jax.ShapeDtypeStruct((NG, 8, PLANE), F32)] * 2 + [jax.ShapeDtypeStruct((NG * 8, PLANE), F32)],
        in_specs=[SMEM_SPEC] + [VMEM_SPEC] * 10,
        out_specs=[VMEM_SPEC] * 3,
        scratch_shapes=SPLIT,
        name="spectrum",
        compiler_params=pltpu.CompilerParams(vmem_limit_bytes=24 << 20),
    )(q.reshape(1), *bands, jnp.asarray(kernel_values()), jnp.asarray(thirds()), *tables)


def terms(q, right, left, field, tables):
    return pl.pallas_call(
        terms_kernel,
        out_shape=[jax.ShapeDtypeStruct(shape, F32) for shape in [(4, QCELL)] * 2 + [(10, QCELL)] + [(1, QCELL)] * 2],
        in_specs=[SMEM_SPEC] + [VMEM_SPEC] * 6,
        out_specs=[VMEM_SPEC] * 5,
        scratch_shapes=SPLIT + [pltpu.VMEM((NG * 8, PLANE), F32)],
        name="terms",
        compiler_params=pltpu.CompilerParams(vmem_limit_bytes=28 << 20),
    )(q.reshape(1), right, left, field, jnp.asarray(thirds()), *tables)


BOTH = ("band", "grid")
CHUNK = QCELL // 4


def small_call(body, outs, scratch=(), limit=8):
    vmem = pl.BlockSpec(memory_space=pltpu.VMEM)

    def call(where, *arrays):
        return pl.pallas_call(
            body,
            out_shape=[jax.ShapeDtypeStruct(shape, F32) for shape in outs],
            in_specs=[pl.BlockSpec(memory_space=pltpu.SMEM)] + [vmem] * len(arrays),
            out_specs=[vmem] * len(outs),
            scratch_shapes=list(scratch),
            compiler_params=pltpu.CompilerParams(vmem_limit_bytes=limit << 20),
        )(where, *arrays)

    return call


def chunk_of(where, k):
    return pl.ds(pl.multiple_of((where[1] ^ k) * CHUNK, 128), CHUNK)


def prepare_kernel(where, orbitals, sel_a, sel_b, *chunks):
    lower = where[0] < 2
    a, b = orbitals[0:2, :], orbitals[2:4, :]
    sel_a[...] = jnp.where(lower, a, b)
    sel_b[...] = jnp.where(lower, b, a)
    for k in range(4):
        chunks[k][...] = orbitals[:, chunk_of(where, k)]


def stack_kernel(where, two, low_a, low_b, out):
    out[0:4, :] = two[...]
    out[4:6, :] = low_a[...]
    out[6:8, :] = low_b[...]


def merge_kernel(where, near0, near2, low0, low2, across, near, far, owed_a, owed_b):
    first = where[0] % 2 == 0
    near[...] = near0[...] + across[0:4, :]
    far[...] = near2[...] + across[4:8, :]
    for out, low, row in ((owed_a, low0, 8), (owed_b, low2, 9)):
        a, b = low[...], across[row : row + 1, :]
        out[0:1, :] = jnp.where(first, a, b)
        out[1:2, :] = jnp.where(first, b, a)


def finalize_kernel(where, near, far, owed_a, owed_b, vectors, *chunks):
    lower = where[0] < 2
    a, b = owed_a[...], owed_b[...]
    total = near[...] + far[...]
    vectors[0:2, :] = total[0:2, :] + jnp.where(lower, a, b)
    vectors[2:4, :] = total[2:4, :] + jnp.where(lower, b, a)
    for k in range(4):
        chunks[k][...] = vectors[:, chunk_of(where, k)]


def pair_kernel(where, f0, f1, f2, f3, other, out):
    first = where[3] == 0
    for k, f in enumerate((f0, f1, f2, f3)):
        a, b = f[...], other[4 * k : 4 * k + 4, :]
        out[8 * k : 8 * k + 4, :] = jnp.where(first, a, b)
        out[8 * k + 4 : 8 * k + 8, :] = jnp.where(first, b, a)


def margin_kernel(where, p0, p1, p3, p2a, p2b, v0, v1, v2, v3, pieces, block):
    z, y = where[1], where[2]

    def halves(a):
        top = a.astype(BF16)
        return top, (a - top.astype(F32)).astype(BF16)

    vt, vl = halves(jnp.concatenate([v0[...], v1[...], v2[...], v3[...]], axis=0))
    dims = (((1,), (1,)), ((), ()))
    parts = jnp.concatenate([p0[...], p1[...], p2a[...], p2b[...], p3[...]], axis=0)
    ft, fl = halves(parts)
    got = (
        lax.dot_general(ft, vt, dims, preferred_element_type=F32)
        + lax.dot_general(fl, vt, dims, preferred_element_type=F32)
        + lax.dot_general(ft, vl, dims, preferred_element_type=F32)
    )
    for dy in range(4):
        for dz in range(4):
            row = 32 * dy + 8 * dz
            block[(z ^ dz) * 4 + (y + 4 - dy) % 4, :, :] = got[row : row + 8, :]
    out = block[...].reshape(128, 16).T * (1.0 / NCELL)
    turned = [out] + [pltpu.roll(out, 32 * r, 1) for r in (1, 2, 3)]
    third_of = lax.broadcasted_iota(jnp.int32, (16, 128), 1) // 32
    keep = third_of == lax.broadcasted_iota(jnp.int32, (16, 128), 0) % 4
    for q_to in range(4):
        picked = turned[(3 - q_to) % 4]
        for j in range(3):
            picked = jnp.where(third_of == j, turned[(j - q_to) % 4], picked)
        picked = jnp.where(keep, picked, 0.0)
        for dz in range(4):
            row = jnp.sum(picked[4 * dz : 4 * dz + 4, :], axis=0, keepdims=True)
            pieces[pl.ds((z ^ dz) * 4 + q_to, 1), :] = row


def move(value, target):
    nb, nq = lax.axis_size("band"), lax.axis_size("grid")
    pairs = []
    for b in range(nb):
        for q in range(nq):
            z, y, h, q_to = target(b // 8, b // 2 % 4, b % 2, q)
            pairs.append((b * nq + q, ((z % 4) * 8 + (y % 4) * 2 + h) * nq + q_to))
    return lax.ppermute(value, BOTH, pairs)


def along_z(value, flip):
    return move(value, lambda z, y, h, q: (z ^ flip, y, h, q))


def along_y(value, k):
    return move(value, lambda z, y, h, q: (z, y + k, h, q))


def within(value, flip):
    return move(value, lambda z, y, h, q: (z, y, h, q ^ flip))


def around(value, blocks, flip):
    def target(z, y, h, q):
        b = (z * 8 + y * 2 + h + blocks) % 32
        return b // 8, b // 2 % 4, b % 2, q ^ flip

    return move(value, target)


def step(orbitals):
    b = lax.axis_index("band").astype(jnp.int32)
    q = lax.axis_index("grid").astype(jnp.int32)
    where = jnp.stack([q, b // 8, b // 2 % 4, b % 2])
    two = within(orbitals, 2)
    prepare = small_call(prepare_kernel, [(2, QCELL)] * 2 + [(4, CHUNK)] * 4)
    sel_a, sel_b, *zc = prepare(where, orbitals)
    low_a = around(sel_a, 1, 0)
    low_b = around(sel_b, 1, 2)
    one = within(orbitals, 1)
    pieces = [zc[0]] + [along_z(zc[k], k) for k in (1, 2, 3)]
    tables = plane_tables()
    together = jnp.concatenate(pieces, axis=0)
    two, together = lax.optimization_barrier((two, together))
    (stacked,) = small_call(stack_kernel, [(8, QCELL)])(where, two, low_a, low_b)
    core = within(stacked, 1)
    other = move(together, lambda z, y, h, q: (z, y, 1 - h, q))
    right, left, field = spectrum(q, (orbitals, two, one, low_a, low_b, core), tables[:2])
    (p0,) = small_call(pair_kernel, [(32, CHUNK)])(where, *pieces, other)
    p1 = along_y(p0, 1)
    p3 = along_y(p0, 3)
    near0, near2, cross, low0, low2 = terms(q, right, left, field, tables[2:])
    across = within(cross, 1)
    merge = small_call(merge_kernel, [(4, QCELL)] * 2 + [(2, QCELL)] * 2)
    near, both, owe_a, owe_b = merge(where, near0, near2, low0, low2, across)
    far = within(both, 2)
    owed_a = around(owe_a, -1, 0)
    owed_b = around(owe_b, -1, 2)
    p2a = along_y(p1[:16], 1)
    p2b = along_y(p3[16:], 3)
    finalize = small_call(finalize_kernel, [(4, QCELL)] + [(4, CHUNK)] * 4)
    vectors, *vc = finalize(where, near, far, owed_a, owed_b)
    given = [vc[0]] + [along_z(vc[k], k) for k in (1, 2, 3)]
    margin_part = small_call(margin_kernel, [(16, 128)], [pltpu.VMEM((16, 8, 16), F32)], 20)
    (sums,) = margin_part(where, p0, p1, p3, p2a, p2b, *given)
    groups = [[(z * 8 + r) * 4 + p for z in range(4) for p in range(4)] for r in range(8)]
    sums = lax.all_to_all(sums, BOTH, 0, 0, tiled=True, axis_index_groups=groups)
    margin = jnp.sum(sums, axis=0).reshape(4, 32).T
    return vectors, margin


def solution(mesh):
    return jax.shard_map(
        step,
        mesh=mesh,
        in_specs=(P("band", "grid"),),
        out_specs=(P("band", "grid"), P("grid", "band")),
        check_vma=False,
    )
```

```python
import math

import jax
import jax.numpy as jnp
import numpy as np
from jax import lax
from jax.experimental import pallas as pl
from jax.experimental.pallas import tpu as pltpu
from jax.sharding import PartitionSpec as P

NG = 48
NCELL = 110592
PLANE = NG * NG
SLAB = 768
QX = 12
QCELL = QX * PLANE
F32 = jnp.float32
BF16 = jnp.bfloat16
R2 = math.sqrt(0.5)
C1 = math.cos(math.pi / 8)
C3 = math.cos(3 * math.pi / 8)
S3 = math.sqrt(3.0) / 2

ORDER = [("C", b) for b in range(9)] + [("S", b) for b in range(1, 8)]
SWAPPED = [("C", 0)] + [("S", b) for b in range(1, 8)] + [("C", 8)] + [("C", b) for b in range(1, 8)]


def sixteen(order):
    u = np.arange(16)
    cols = []
    for kind, b in order:
        col = np.cos(2 * np.pi * b * u / 16) if kind == "C" else np.sin(2 * np.pi * b * u / 16)
        cols.append(col / np.linalg.norm(col))
    return np.stack(cols, 1)


def forty_eight():
    z = np.arange(NG)
    cols, freqs = [], []
    for g in range(25):
        for kind in ("C", "S") if 0 < g < 24 else ("C",):
            col = np.cos(2 * np.pi * g * z / NG) if kind == "C" else np.sin(2 * np.pi * g * z / NG)
            cols.append(col / np.linalg.norm(col))
            freqs.append(g)
    return np.stack(cols, 1), np.array(freqs)


def folded(g):
    return (g + 24) % 48 - 24


def x_basis():
    keys, freqs, norms = [], [], []
    for b in range(9):
        keys.append(("A", "C", b)); freqs.append(3 * b); norms.append(48 if b in (0, 8) else 24)
    for b in range(1, 8):
        keys.append(("A", "S", b)); freqs.append(3 * b); norms.append(24)
    for b in (0, 8):
        for t in "cs":
            keys.append((t, "C", b)); freqs.append(16 + 3 * b); norms.append(24)
    for b in range(1, 8):
        for sign in (1, -1):
            for kind in ("cos", "sin"):
                keys.append((kind, sign, b)); freqs.append(16 + 3 * sign * b); norms.append(24)
    return keys, np.array(freqs), np.array(norms)


def kernel_values():
    _, gx, nx = x_basis()
    _, gz = forty_eight()
    gy = []
    for slab in "Auv":
        for kind, b in ORDER:
            if slab == "A":
                gy.append(3 * b)
            elif b in (0, 8):
                gy.append(16 + 3 * b)
            else:
                plus = (slab == "u") == (kind == "C")
                gy.append(16 + 3 * b if plus else 16 - 3 * b)
    gy = np.array(gy)
    q = (folded(gx)[:, None, None] ** 2 + folded(gy)[None, :, None] ** 2 + folded(gz)[None, None, :] ** 2).astype(np.float64)
    kern = np.where(q > 0, 40.0 * (1.0 - np.exp(-q / 16.0)) / np.where(q > 0, q, 1.0), 0.0)
    return (kern / (3.0 * nx[:, None, None])).reshape(NG, PLANE).astype(np.float32)


def thirds():
    u = np.arange(SLAB) // NG
    rows = [np.cos(2 * np.pi * (m + u) / 3) for m in range(3)] + [np.sin(2 * np.pi * (m + u) / 3) for m in range(3)]
    return np.concatenate([np.stack(rows), np.zeros((2, SLAB))]).astype(np.float32)


def factor_tables():
    za, _ = forty_eight()
    ta, ts = sixteen(ORDER), sixteen(SWAPPED)
    tens = np.stack([np.repeat(t, NG, 1) for t in (ta, ts, ta.T, ts.T)])
    zs = np.stack([np.tile(z, (1, 16)) for z in (za, za.T)])
    return [a.astype(np.float32) for a in (tens, zs)]


def tables_kernel(tens, zs, hi_there, lo_there, hi_back, lo_back):
    for way, (hi, lo) in enumerate(((hi_there, lo_there), (hi_back, lo_back))):
        for which in range(2):

            def block(u, carry):
                w = zs[way] * tens[2 * way + which, pl.ds(u, 1), :]
                top = w.astype(BF16)
                rows = pl.ds(pl.multiple_of(u * NG, 16), NG)
                hi[which, rows, :] = top
                lo[which, rows, :] = (w - top.astype(F32)).astype(BF16)
                return carry

            lax.fori_loop(0, 16, block, 0)


def plane_tables():
    out = [jax.ShapeDtypeStruct((2, SLAB, SLAB), BF16)] * 4
    return pl.pallas_call(
        tables_kernel, out_shape=out, name="plane_tables",
        compiler_params=pltpu.CompilerParams(vmem_limit_bytes=16 << 20),
    )(*[jnp.asarray(a) for a in factor_tables()])


def t16(f):
    o = [f[u] - f[u + 8] for u in range(8)]
    e = [f[u] + f[u + 8] for u in range(8)]
    ee = [e[u] + e[u + 4] for u in range(4)]
    eo = [e[u] - e[u + 4] for u in range(4)]
    c, s = {}, {}
    p0, p1 = ee[0] + ee[2], ee[1] + ee[3]
    c[0], c[8], c[4], s[4] = p0 + p1, p0 - p1, ee[0] - ee[2], ee[1] - ee[3]
    d, a = R2 * (eo[1] - eo[3]), R2 * (eo[1] + eo[3])
    c[2], c[6], s[2], s[6] = eo[0] + d, eo[0] - d, a + eo[2], a - eo[2]
    d1, d2, d3 = (o[u] - o[8 - u] for u in (1, 2, 3))
    s1, s2, s3 = (o[u] + o[8 - u] for u in (1, 2, 3))
    d2, s2 = R2 * d2, R2 * s2
    e1, e3 = o[0] + d2, o[0] - d2
    o1, o3 = C1 * d1 + C3 * d3, C3 * d1 - C1 * d3
    c[1], c[7], c[3], c[5] = e1 + o1, e1 - o1, e3 + o3, e3 - o3
    x1, x3 = o[4] + s2, o[4] - s2
    y1, y3 = C3 * s1 + C1 * s3, C1 * s1 - C3 * s3
    s[1], s[7], s[3], s[5] = y1 + x1, y1 - x1, y3 - x3, y3 + x3
    return c, s


def t16_back(c, s):
    e1, o1, e3, o3 = c[1] + c[7], c[1] - c[7], c[3] + c[5], c[3] - c[5]
    o0, d2 = e1 + e3, R2 * (e1 - e3)
    d1, d3 = C1 * o1 + C3 * o3, C3 * o1 - C1 * o3
    y1, x1, y3, x3 = s[1] + s[7], s[1] - s[7], s[3] + s[5], s[5] - s[3]
    o4, s2 = x1 + x3, R2 * (x1 - x3)
    s1, s3 = C3 * y1 + C1 * y3, C1 * y1 - C3 * y3
    o = [o0, d1 + s1, d2 + s2, d3 + s3, o4, s3 - d3, s2 - d2, s1 - d1]
    d, a = R2 * (c[2] - c[6]), R2 * (s[2] + s[6])
    eo = [c[2] + c[6], d + a, s[2] - s[6], a - d]
    p0, p1 = c[0] + c[8], c[0] - c[8]
    ee = [p0 + c[4], p1 + s[4], p0 - c[4], p1 - s[4]]
    e = [ee[u] + eo[u] for u in range(4)] + [ee[u] - eo[u] for u in range(4)]
    return [e[u] + o[u] for u in range(8)] + [e[u] - o[u] for u in range(8)]


def convolve_x(f, table):
    keys, _, _ = x_basis()
    row = {key: k for k, key in enumerate(keys)}
    place = {(x % 3, x % 16): x for x in range(NG)}
    part = {"A": [], "c": [], "s": []}
    for u in range(16):
        f0, f1, f2 = (f[place[t, u]] for t in range(3))
        a = f1 + f2
        part["A"].append(f0 + a)
        part["c"].append(f0 - 0.5 * a)
        part["s"].append(S3 * (f1 - f2))
    c, s = t16(part["A"])
    c = {b: v * table(row["A", "C", b]) for b, v in c.items()}
    s = {b: v * table(row["A", "S", b]) for b, v in s.items()}
    back_a = t16_back(c, s)
    cc, cs = t16(part["c"])
    sc, ss = t16(part["s"])
    for b in (0, 8):
        cc[b] = cc[b] * table(row["c", "C", b])
        sc[b] = sc[b] * table(row["s", "C", b])
    for b in range(1, 8):
        p = (cc[b] - ss[b]) * table(row["cos", 1, b])
        m = (cc[b] + ss[b]) * table(row["cos", -1, b])
        cc[b], ss[b] = p + m, m - p
        p = (sc[b] + cs[b]) * table(row["sin", 1, b])
        m = (sc[b] - cs[b]) * table(row["sin", -1, b])
        sc[b], cs[b] = p + m, p - m
    back_c, back_s = t16_back(cc, cs), t16_back(sc, ss)
    out = [None] * NG
    for u in range(16):
        a, c_, s_ = back_a[u], back_c[u], S3 * back_s[u]
        h = a - 0.5 * c_
        out[place[0, u]] = a + c_
        out[place[1, u]] = h + s_
        out[place[2, u]] = h - s_
    return out


def split(hi, lo, rows, m, value):
    top = value.astype(BF16)
    span = slice(m * SLAB, (m + 1) * SLAB)
    hi[rows, span] = top
    lo[rows, span] = (value - top.astype(F32)).astype(BF16)


def product(hi, lo, whi, wlo, m, k, cols):
    span = slice(m * SLAB, (m + 1) * SLAB)
    a, b = hi[:, span], lo[:, span]
    lhs = jnp.concatenate([a, b, a], axis=1)
    w = jnp.concatenate([whi[k, :, cols], whi[k, :, cols], wlo[k, :, cols]], axis=0)
    return jnp.dot(lhs, w, preferred_element_type=F32)


def spectrum_kernel(q_ref, own, two, one, low_a, low_b, core, kern, third, whi, wlo, right, left, field, hi, lo):
    q = q_ref[0]
    sources = (
        (own, 0, low_a, 0),
        (one, 0, core, 4),
        (two, 0, low_b, 0),
        (core, 0, core, 6),
    )
    for delta, (bands_ref, first, low_ref, low_first) in enumerate(sources):
        base = (q ^ delta) * QX

        def place(x, carry):
            span = pl.ds(pl.multiple_of(x * PLANE, 128), PLANE)
            bands = bands_ref[first : first + 4, span]
            right[base + x, 0:4, :] = bands
            right[base + x, 4:8, :] = bands
            left[base + x, 0:4, :] = jnp.broadcast_to(bands_ref[pl.ds(first + q, 1), span], (4, PLANE))
            left[base + x, 4:8, :] = jnp.broadcast_to(low_ref[pl.ds(low_first + q % 2, 1), span], (4, PLANE))
            return carry

        lax.fori_loop(0, QX, place, 0)

    def densities(i, carry):
        x = pl.ds(2 * i, 2)
        rows = pl.ds(pl.multiple_of(16 * i, 16), 16)
        f = []
        for m in range(3):
            span = slice(m * SLAB, (m + 1) * SLAB)
            f.append((right[x, :, span] * left[x, :, span]).reshape(16, SLAB))
        split(hi, lo, rows, 0, f[0] + f[1] + f[2])
        split(hi, lo, rows, 1, f[0] * third[0:1, :] + f[1] * third[1:2, :] + f[2] * third[2:3, :])
        split(hi, lo, rows, 2, f[0] * third[3:4, :] + f[1] * third[4:5, :] + f[2] * third[5:6, :])
        return carry

    lax.fori_loop(0, NG // 2, densities, 0)

    for j in range(3):
        cols = slice(j * 256, (j + 1) * 256)
        field[:, cols] = product(hi, lo, whi, wlo, 0, 0, cols)
        c = product(hi, lo, whi, wlo, 1, 0, cols)
        s = product(hi, lo, whi, wlo, 2, 1, cols)
        field[:, SLAB + j * 256 : SLAB + (j + 1) * 256] = c - s
        field[:, 2 * SLAB + j * 256 : 2 * SLAB + (j + 1) * 256] = c + s

    def along_x(i, carry):
        span = pl.ds(pl.multiple_of(128 * i, 128), 128)
        f = [field[8 * x : 8 * x + 8, span] for x in range(NG)]
        out = convolve_x(f, lambda k: kern[k : k + 1, span])
        for x in range(NG):
            field[8 * x : 8 * x + 8, span] = out[x]
        return carry

    lax.fori_loop(0, PLANE // 128, along_x, 0)


def terms_kernel(q_ref, right, left, field, third, whi, wlo, near0, near2, cross, low0, low2, hi, lo, back):
    q = q_ref[0]

    def unmix(i, carry):
        rows = pl.ds(pl.multiple_of(16 * i, 16), 16)
        u = field[rows, SLAB : 2 * SLAB]
        v = field[rows, 2 * SLAB : 3 * SLAB]
        split(hi, lo, rows, 0, field[rows, 0:SLAB])
        split(hi, lo, rows, 1, u + v)
        split(hi, lo, rows, 2, v - u)
        return carry

    lax.fori_loop(0, NG // 2, unmix, 0)
    for j in range(3):
        cols = slice(j * 256, (j + 1) * 256)
        for m, k in ((0, 0), (1, 0), (2, 1)):
            back[:, m * SLAB + j * 256 : m * SLAB + (j + 1) * 256] = product(hi, lo, whi, wlo, m, k, cols)

    mine = (lax.broadcasted_iota(jnp.int32, (8, SLAB), 0) == q).astype(F32)

    for delta in range(4):
        base = (q ^ delta) * QX

        def finish(i, carry):
            x = base + i
            rows = pl.ds(pl.multiple_of(x * 8, 8), 8)
            a = back[rows, 0:SLAB]
            c = back[rows, SLAB : 2 * SLAB]
            s = back[rows, 2 * SLAB : 3 * SLAB]
            for m in range(3):
                span = slice(m * SLAB, (m + 1) * SLAB)
                v = a + c * third[m : m + 1, :] + s * third[3 + m : 4 + m, :]
                pr = v * right[x, :, span]
                pr = pr + pltpu.roll(pr, 6, 0)
                pr = pr + pltpu.roll(pr, 7, 0)
                po = pltpu.roll(v * left[x, :, span], 4, 0) + mine * pr[0:1, :]
                at = pl.ds(pl.multiple_of(i * PLANE + m * SLAB, SLAB), SLAB)
                bands, low = -po[0:4, :], -pr[4:5, :]
                if delta % 2:
                    cross[delta // 2 * 4 : delta // 2 * 4 + 4, at] = bands
                    cross[8 + delta // 2 : 9 + delta // 2, at] = low
                else:
                    (near0, near2)[delta // 2][:, at] = bands
                    (low0, low2)[delta // 2][:, at] = low
            return carry

        lax.fori_loop(0, QX, finish, 0)


VMEM_SPEC = pl.BlockSpec(memory_space=pltpu.VMEM)
SMEM_SPEC = pl.BlockSpec(memory_space=pltpu.SMEM)
SPLIT = [pltpu.VMEM((NG * 8, PLANE), BF16)] * 2


def spectrum(q, bands, tables):
    return pl.pallas_call(
        spectrum_kernel,
        out_shape=[jax.ShapeDtypeStruct((NG, 8, PLANE), F32)] * 2 + [jax.ShapeDtypeStruct((NG * 8, PLANE), F32)],
        in_specs=[SMEM_SPEC] + [VMEM_SPEC] * 10,
        out_specs=[VMEM_SPEC] * 3,
        scratch_shapes=SPLIT,
        name="spectrum",
        compiler_params=pltpu.CompilerParams(vmem_limit_bytes=24 << 20),
    )(q.reshape(1), *bands, jnp.asarray(kernel_values()), jnp.asarray(thirds()), *tables)


def terms(q, right, left, field, tables):
    return pl.pallas_call(
        terms_kernel,
        out_shape=[jax.ShapeDtypeStruct(shape, F32) for shape in [(4, QCELL)] * 2 + [(10, QCELL)] + [(1, QCELL)] * 2],
        in_specs=[SMEM_SPEC] + [VMEM_SPEC] * 6,
        out_specs=[VMEM_SPEC] * 5,
        scratch_shapes=SPLIT + [pltpu.VMEM((NG * 8, PLANE), F32)],
        name="terms",
        compiler_params=pltpu.CompilerParams(vmem_limit_bytes=28 << 20),
    )(q.reshape(1), right, left, field, jnp.asarray(thirds()), *tables)


BOTH = ("band", "grid")
CHUNK = QCELL // 4


def small_call(body, outs, scratch=(), limit=8):
    vmem = pl.BlockSpec(memory_space=pltpu.VMEM)

    def call(where, *arrays):
        return pl.pallas_call(
            body,
            out_shape=[jax.ShapeDtypeStruct(shape, F32) for shape in outs],
            in_specs=[pl.BlockSpec(memory_space=pltpu.SMEM)] + [vmem] * len(arrays),
            out_specs=[vmem] * len(outs),
            scratch_shapes=list(scratch),
            compiler_params=pltpu.CompilerParams(vmem_limit_bytes=limit << 20),
        )(where, *arrays)

    return call


def chunk_of(where, k):
    return pl.ds(pl.multiple_of((where[1] ^ k) * CHUNK, 128), CHUNK)


def prepare_kernel(where, orbitals, sel_a, sel_b, *chunks):
    lower = where[0] < 2
    a, b = orbitals[0:2, :], orbitals[2:4, :]
    sel_a[...] = jnp.where(lower, a, b)
    sel_b[...] = jnp.where(lower, b, a)
    for k in range(4):
        chunks[k][...] = orbitals[:, chunk_of(where, k)]


def stack_kernel(where, two, low_a, low_b, out):
    out[0:4, :] = two[...]
    out[4:6, :] = low_a[...]
    out[6:8, :] = low_b[...]


def merge_kernel(where, near0, near2, low0, low2, across, near, far, owed_a, owed_b):
    first = where[0] % 2 == 0
    near[...] = near0[...] + across[0:4, :]
    far[...] = near2[...] + across[4:8, :]
    for out, low, row in ((owed_a, low0, 8), (owed_b, low2, 9)):
        a, b = low[...], across[row : row + 1, :]
        out[0:1, :] = jnp.where(first, a, b)
        out[1:2, :] = jnp.where(first, b, a)


def finalize_kernel(where, near, far, owed_a, owed_b, vectors, *chunks):
    lower = where[0] < 2
    a, b = owed_a[...], owed_b[...]
    total = near[...] + far[...]
    vectors[0:2, :] = total[0:2, :] + jnp.where(lower, a, b)
    vectors[2:4, :] = total[2:4, :] + jnp.where(lower, b, a)
    for k in range(4):
        chunks[k][...] = vectors[:, chunk_of(where, k)]


def margin_kernel(where, own0, oth0, own1, oth1, own2, oth2, own3, oth3, v0, v1, v2, v3, pieces, block):
    z, y, h = where[1], where[2], where[3]

    def halves(a):
        top = a.astype(BF16)
        return top, (a - top.astype(F32)).astype(BF16)

    vt, vl = halves(jnp.concatenate([v0[...], v1[...], v2[...], v3[...]], axis=0))
    dims = (((1,), (1,)), ((), ()))
    parts = jnp.concatenate([r[...] for r in (own0, oth0, own1, oth1, own2, oth2, own3, oth3)], axis=0)
    ft, fl = halves(parts)
    got = (
        lax.dot_general(ft, vt, dims, preferred_element_type=F32)
        + lax.dot_general(fl, vt, dims, preferred_element_type=F32)
        + lax.dot_general(ft, vl, dims, preferred_element_type=F32)
    )
    for dy in range(4):
        for dz in range(4):
            row = 32 * dy + 4 * dz
            pair = got[row : row + 4, :], got[row + 16 : row + 20, :]
            at = (z ^ dz) * 4 + (y + 4 - dy) % 4
            block[at, 0:4, :] = jnp.where(h == 0, pair[0], pair[1])
            block[at, 4:8, :] = jnp.where(h == 0, pair[1], pair[0])
    out = block[...].reshape(128, 16).T * (1.0 / NCELL)
    turned = [out] + [pltpu.roll(out, 32 * r, 1) for r in (1, 2, 3)]
    third_of = lax.broadcasted_iota(jnp.int32, (16, 128), 1) // 32
    keep = third_of == lax.broadcasted_iota(jnp.int32, (16, 128), 0) % 4
    for q_to in range(4):
        picked = turned[(3 - q_to) % 4]
        for j in range(3):
            picked = jnp.where(third_of == j, turned[(j - q_to) % 4], picked)
        picked = jnp.where(keep, picked, 0.0)
        for dz in range(4):
            row = jnp.sum(picked[4 * dz : 4 * dz + 4, :], axis=0, keepdims=True)
            pieces[pl.ds((z ^ dz) * 4 + q_to, 1), :] = row


def move(value, target):
    nb, nq = lax.axis_size("band"), lax.axis_size("grid")
    pairs = []
    for b in range(nb):
        for q in range(nq):
            z, y, h, q_to = target(b // 8, b // 2 % 4, b % 2, q)
            pairs.append((b * nq + q, ((z % 4) * 8 + (y % 4) * 2 + h) * nq + q_to))
    return lax.ppermute(value, BOTH, pairs)


def along_z(value, flip):
    return move(value, lambda z, y, h, q: (z ^ flip, y, h, q))


def along_y(value, k):
    return move(value, lambda z, y, h, q: (z, y + k, h, q))


def within(value, flip):
    return move(value, lambda z, y, h, q: (z, y, h, q ^ flip))


def around(value, blocks, flip):
    def target(z, y, h, q):
        b = (z * 8 + y * 2 + h + blocks) % 32
        return b // 8, b // 2 % 4, b % 2, q ^ flip

    return move(value, target)


def step(orbitals):
    b = lax.axis_index("band").astype(jnp.int32)
    q = lax.axis_index("grid").astype(jnp.int32)
    where = jnp.stack([q, b // 8, b // 2 % 4, b % 2])
    two = within(orbitals, 2)
    prepare = small_call(prepare_kernel, [(2, QCELL)] * 2 + [(4, CHUNK)] * 4)
    sel_a, sel_b, *zc = prepare(where, orbitals)
    low_a = around(sel_a, 1, 0)
    low_b = around(sel_b, 1, 2)
    one = within(orbitals, 1)
    pieces = [zc[0]] + [along_z(zc[k], k) for k in (1, 2, 3)]
    tables = plane_tables()
    together = jnp.concatenate(pieces, axis=0)
    two, together = lax.optimization_barrier((two, together))
    (stacked,) = small_call(stack_kernel, [(8, QCELL)])(where, two, low_a, low_b)
    core = within(stacked, 1)
    other = move(together, lambda z, y, h, q: (z, y, 1 - h, q))
    own1 = along_y(together, 1)
    own3 = along_y(together, 3)
    right, left, field = spectrum(q, (orbitals, two, one, low_a, low_b, core), tables[:2])
    oth1 = along_y(other, 1)
    oth3 = along_y(other, 3)
    own2 = along_y(own1, 1)
    near0, near2, cross, low0, low2 = terms(q, right, left, field, tables[2:])
    across = within(cross, 1)
    merge = small_call(merge_kernel, [(4, QCELL)] * 2 + [(2, QCELL)] * 2)
    near, both, owe_a, owe_b = merge(where, near0, near2, low0, low2, across)
    far = within(both, 2)
    owed_a = around(owe_a, -1, 0)
    owed_b = around(owe_b, -1, 2)
    oth2 = along_y(oth1, 1)
    finalize = small_call(finalize_kernel, [(4, QCELL)] + [(4, CHUNK)] * 4)
    vectors, *vc = finalize(where, near, far, owed_a, owed_b)
    given = [vc[0]] + [along_z(vc[k], k) for k in (1, 2, 3)]
    margin_part = small_call(margin_kernel, [(16, 128)], [pltpu.VMEM((16, 8, 16), F32)], 20)
    (sums,) = margin_part(where, together, other, own1, oth1, own2, oth2, own3, oth3, *given)
    groups = [[(z * 8 + r) * 4 + p for z in range(4) for p in range(4)] for r in range(8)]
    sums = lax.all_to_all(sums, BOTH, 0, 0, tiled=True, axis_index_groups=groups)
    margin = jnp.sum(sums, axis=0).reshape(4, 32).T
    return vectors, margin


def solution(mesh):
    return jax.shard_map(
        step,
        mesh=mesh,
        in_specs=(P("band", "grid"),),
        out_specs=(P("band", "grid"), P("grid", "band")),
        check_vma=False,
    )
```

```python
import math

import jax
import jax.numpy as jnp
import numpy as np
from jax import lax
from jax.experimental import pallas as pl
from jax.experimental.pallas import tpu as pltpu
from jax.sharding import PartitionSpec as P

NG = 48
NCELL = 110592
PLANE = NG * NG
SLAB = 768
QX = 12
QCELL = QX * PLANE
F32 = jnp.float32
BF16 = jnp.bfloat16
R2 = math.sqrt(0.5)
C1 = math.cos(math.pi / 8)
C3 = math.cos(3 * math.pi / 8)
S3 = math.sqrt(3.0) / 2

ORDER = [("C", b) for b in range(9)] + [("S", b) for b in range(1, 8)]
SWAPPED = [("C", 0)] + [("S", b) for b in range(1, 8)] + [("C", 8)] + [("C", b) for b in range(1, 8)]


def sixteen(order):
    u = np.arange(16)
    cols = []
    for kind, b in order:
        col = np.cos(2 * np.pi * b * u / 16) if kind == "C" else np.sin(2 * np.pi * b * u / 16)
        cols.append(col / np.linalg.norm(col))
    return np.stack(cols, 1)


def forty_eight():
    z = np.arange(NG)
    cols, freqs = [], []
    for g in range(25):
        for kind in ("C", "S") if 0 < g < 24 else ("C",):
            col = np.cos(2 * np.pi * g * z / NG) if kind == "C" else np.sin(2 * np.pi * g * z / NG)
            cols.append(col / np.linalg.norm(col))
            freqs.append(g)
    return np.stack(cols, 1), np.array(freqs)


def folded(g):
    return (g + 24) % 48 - 24


def x_basis():
    keys, freqs, norms = [], [], []
    for b in range(9):
        keys.append(("A", "C", b)); freqs.append(3 * b); norms.append(48 if b in (0, 8) else 24)
    for b in range(1, 8):
        keys.append(("A", "S", b)); freqs.append(3 * b); norms.append(24)
    for b in (0, 8):
        for t in "cs":
            keys.append((t, "C", b)); freqs.append(16 + 3 * b); norms.append(24)
    for b in range(1, 8):
        for sign in (1, -1):
            for kind in ("cos", "sin"):
                keys.append((kind, sign, b)); freqs.append(16 + 3 * sign * b); norms.append(24)
    return keys, np.array(freqs), np.array(norms)


def kernel_values():
    _, gx, nx = x_basis()
    _, gz = forty_eight()
    gy = []
    for slab in "Auv":
        for kind, b in ORDER:
            if slab == "A":
                gy.append(3 * b)
            elif b in (0, 8):
                gy.append(16 + 3 * b)
            else:
                plus = (slab == "u") == (kind == "C")
                gy.append(16 + 3 * b if plus else 16 - 3 * b)
    gy = np.array(gy)
    q = (folded(gx)[:, None, None] ** 2 + folded(gy)[None, :, None] ** 2 + folded(gz)[None, None, :] ** 2).astype(np.float64)
    kern = np.where(q > 0, 40.0 * (1.0 - np.exp(-q / 16.0)) / np.where(q > 0, q, 1.0), 0.0)
    return (kern / (3.0 * nx[:, None, None])).reshape(NG, PLANE).astype(np.float32)


def thirds():
    u = np.arange(SLAB) // NG
    rows = [np.cos(2 * np.pi * (m + u) / 3) for m in range(3)] + [np.sin(2 * np.pi * (m + u) / 3) for m in range(3)]
    return np.concatenate([np.stack(rows), np.zeros((2, SLAB))]).astype(np.float32)


def factor_tables():
    za, _ = forty_eight()
    ta, ts = sixteen(ORDER), sixteen(SWAPPED)
    tens = np.stack([np.repeat(t, NG, 1) for t in (ta, ts, ta.T, ts.T)])
    zs = np.stack([np.tile(z, (1, 16)) for z in (za, za.T)])
    return [a.astype(np.float32) for a in (tens, zs)]


def tables_kernel(tens, zs, hi_there, lo_there, hi_back, lo_back):
    for way, (hi, lo) in enumerate(((hi_there, lo_there), (hi_back, lo_back))):
        for which in range(2):

            def block(u, carry):
                w = zs[way] * tens[2 * way + which, pl.ds(u, 1), :]
                top = w.astype(BF16)
                rows = pl.ds(pl.multiple_of(u * NG, 16), NG)
                hi[which, rows, :] = top
                lo[which, rows, :] = (w - top.astype(F32)).astype(BF16)
                return carry

            lax.fori_loop(0, 16, block, 0)


def plane_tables():
    out = [jax.ShapeDtypeStruct((2, SLAB, SLAB), BF16)] * 4
    return pl.pallas_call(
        tables_kernel, out_shape=out, name="plane_tables",
        compiler_params=pltpu.CompilerParams(vmem_limit_bytes=16 << 20),
    )(*[jnp.asarray(a) for a in factor_tables()])


def t16(f):
    o = [f[u] - f[u + 8] for u in range(8)]
    e = [f[u] + f[u + 8] for u in range(8)]
    ee = [e[u] + e[u + 4] for u in range(4)]
    eo = [e[u] - e[u + 4] for u in range(4)]
    c, s = {}, {}
    p0, p1 = ee[0] + ee[2], ee[1] + ee[3]
    c[0], c[8], c[4], s[4] = p0 + p1, p0 - p1, ee[0] - ee[2], ee[1] - ee[3]
    d, a = R2 * (eo[1] - eo[3]), R2 * (eo[1] + eo[3])
    c[2], c[6], s[2], s[6] = eo[0] + d, eo[0] - d, a + eo[2], a - eo[2]
    d1, d2, d3 = (o[u] - o[8 - u] for u in (1, 2, 3))
    s1, s2, s3 = (o[u] + o[8 - u] for u in (1, 2, 3))
    d2, s2 = R2 * d2, R2 * s2
    e1, e3 = o[0] + d2, o[0] - d2
    o1, o3 = C1 * d1 + C3 * d3, C3 * d1 - C1 * d3
    c[1], c[7], c[3], c[5] = e1 + o1, e1 - o1, e3 + o3, e3 - o3
    x1, x3 = o[4] + s2, o[4] - s2
    y1, y3 = C3 * s1 + C1 * s3, C1 * s1 - C3 * s3
    s[1], s[7], s[3], s[5] = y1 + x1, y1 - x1, y3 - x3, y3 + x3
    return c, s


def t16_back(c, s):
    e1, o1, e3, o3 = c[1] + c[7], c[1] - c[7], c[3] + c[5], c[3] - c[5]
    o0, d2 = e1 + e3, R2 * (e1 - e3)
    d1, d3 = C1 * o1 + C3 * o3, C3 * o1 - C1 * o3
    y1, x1, y3, x3 = s[1] + s[7], s[1] - s[7], s[3] + s[5], s[5] - s[3]
    o4, s2 = x1 + x3, R2 * (x1 - x3)
    s1, s3 = C3 * y1 + C1 * y3, C1 * y1 - C3 * y3
    o = [o0, d1 + s1, d2 + s2, d3 + s3, o4, s3 - d3, s2 - d2, s1 - d1]
    d, a = R2 * (c[2] - c[6]), R2 * (s[2] + s[6])
    eo = [c[2] + c[6], d + a, s[2] - s[6], a - d]
    p0, p1 = c[0] + c[8], c[0] - c[8]
    ee = [p0 + c[4], p1 + s[4], p0 - c[4], p1 - s[4]]
    e = [ee[u] + eo[u] for u in range(4)] + [ee[u] - eo[u] for u in range(4)]
    return [e[u] + o[u] for u in range(8)] + [e[u] - o[u] for u in range(8)]


def convolve_x(f, table):
    keys, _, _ = x_basis()
    row = {key: k for k, key in enumerate(keys)}
    place = {(x % 3, x % 16): x for x in range(NG)}
    part = {"A": [], "c": [], "s": []}
    for u in range(16):
        f0, f1, f2 = (f[place[t, u]] for t in range(3))
        a = f1 + f2
        part["A"].append(f0 + a)
        part["c"].append(f0 - 0.5 * a)
        part["s"].append(S3 * (f1 - f2))
    c, s = t16(part["A"])
    c = {b: v * table(row["A", "C", b]) for b, v in c.items()}
    s = {b: v * table(row["A", "S", b]) for b, v in s.items()}
    back_a = t16_back(c, s)
    cc, cs = t16(part["c"])
    sc, ss = t16(part["s"])
    for b in (0, 8):
        cc[b] = cc[b] * table(row["c", "C", b])
        sc[b] = sc[b] * table(row["s", "C", b])
    for b in range(1, 8):
        p = (cc[b] - ss[b]) * table(row["cos", 1, b])
        m = (cc[b] + ss[b]) * table(row["cos", -1, b])
        cc[b], ss[b] = p + m, m - p
        p = (sc[b] + cs[b]) * table(row["sin", 1, b])
        m = (sc[b] - cs[b]) * table(row["sin", -1, b])
        sc[b], cs[b] = p + m, p - m
    back_c, back_s = t16_back(cc, cs), t16_back(sc, ss)
    out = [None] * NG
    for u in range(16):
        a, c_, s_ = back_a[u], back_c[u], S3 * back_s[u]
        h = a - 0.5 * c_
        out[place[0, u]] = a + c_
        out[place[1, u]] = h + s_
        out[place[2, u]] = h - s_
    return out


def split(hi, lo, rows, m, value):
    top = value.astype(BF16)
    span = slice(m * SLAB, (m + 1) * SLAB)
    hi[rows, span] = top
    lo[rows, span] = (value - top.astype(F32)).astype(BF16)


def product(hi, lo, whi, wlo, m, k, cols):
    span = slice(m * SLAB, (m + 1) * SLAB)
    a, b = hi[:, span], lo[:, span]
    lhs = jnp.concatenate([a, b, a], axis=1)
    w = jnp.concatenate([whi[k, :, cols], whi[k, :, cols], wlo[k, :, cols]], axis=0)
    return jnp.dot(lhs, w, preferred_element_type=F32)


def spectrum_kernel(q_ref, own, two, one, low_a, low_b, core, kern, third, whi, wlo, right, left, field, hi, lo):
    q = q_ref[0]
    sources = (
        (own, 0, low_a, 0),
        (one, 0, core, 4),
        (two, 0, low_b, 0),
        (core, 0, core, 6),
    )
    for delta, (bands_ref, first, low_ref, low_first) in enumerate(sources):
        base = (q ^ delta) * QX

        def place(x, carry):
            span = pl.ds(pl.multiple_of(x * PLANE, 128), PLANE)
            bands = bands_ref[first : first + 4, span]
            right[base + x, 0:4, :] = bands
            right[base + x, 4:8, :] = bands
            left[base + x, 0:4, :] = jnp.broadcast_to(bands_ref[pl.ds(first + q, 1), span], (4, PLANE))
            left[base + x, 4:8, :] = jnp.broadcast_to(low_ref[pl.ds(low_first + q % 2, 1), span], (4, PLANE))
            return carry

        lax.fori_loop(0, QX, place, 0)

    def densities(i, carry):
        x = pl.ds(2 * i, 2)
        rows = pl.ds(pl.multiple_of(16 * i, 16), 16)
        f = []
        for m in range(3):
            span = slice(m * SLAB, (m + 1) * SLAB)
            f.append((right[x, :, span] * left[x, :, span]).reshape(16, SLAB))
        split(hi, lo, rows, 0, f[0] + f[1] + f[2])
        split(hi, lo, rows, 1, f[0] * third[0:1, :] + f[1] * third[1:2, :] + f[2] * third[2:3, :])
        split(hi, lo, rows, 2, f[0] * third[3:4, :] + f[1] * third[4:5, :] + f[2] * third[5:6, :])
        return carry

    lax.fori_loop(0, NG // 2, densities, 0)

    for j in range(3):
        cols = slice(j * 256, (j + 1) * 256)
        field[:, cols] = product(hi, lo, whi, wlo, 0, 0, cols)
        c = product(hi, lo, whi, wlo, 1, 0, cols)
        s = product(hi, lo, whi, wlo, 2, 1, cols)
        field[:, SLAB + j * 256 : SLAB + (j + 1) * 256] = c - s
        field[:, 2 * SLAB + j * 256 : 2 * SLAB + (j + 1) * 256] = c + s

    def along_x(i, carry):
        span = pl.ds(pl.multiple_of(128 * i, 128), 128)
        f = [field[8 * x : 8 * x + 8, span] for x in range(NG)]
        out = convolve_x(f, lambda k: kern[k : k + 1, span])
        for x in range(NG):
            field[8 * x : 8 * x + 8, span] = out[x]
        return carry

    lax.fori_loop(0, PLANE // 128, along_x, 0)


def terms_kernel(q_ref, right, left, field, third, whi, wlo, near0, near2, cross, low0, low2, hi, lo, back):
    q = q_ref[0]

    def unmix(i, carry):
        rows = pl.ds(pl.multiple_of(16 * i, 16), 16)
        u = field[rows, SLAB : 2 * SLAB]
        v = field[rows, 2 * SLAB : 3 * SLAB]
        split(hi, lo, rows, 0, field[rows, 0:SLAB])
        split(hi, lo, rows, 1, u + v)
        split(hi, lo, rows, 2, v - u)
        return carry

    lax.fori_loop(0, NG // 2, unmix, 0)
    for j in range(3):
        cols = slice(j * 256, (j + 1) * 256)
        for m, k in ((0, 0), (1, 0), (2, 1)):
            back[:, m * SLAB + j * 256 : m * SLAB + (j + 1) * 256] = product(hi, lo, whi, wlo, m, k, cols)

    mine = (lax.broadcasted_iota(jnp.int32, (8, SLAB), 0) == q).astype(F32)

    for delta in range(4):
        base = (q ^ delta) * QX

        def finish(i, carry):
            x = base + i
            rows = pl.ds(pl.multiple_of(x * 8, 8), 8)
            a = back[rows, 0:SLAB]
            c = back[rows, SLAB : 2 * SLAB]
            s = back[rows, 2 * SLAB : 3 * SLAB]
            for m in range(3):
                span = slice(m * SLAB, (m + 1) * SLAB)
                v = a + c * third[m : m + 1, :] + s * third[3 + m : 4 + m, :]
                pr = v * right[x, :, span]
                pr = pr + pltpu.roll(pr, 6, 0)
                pr = pr + pltpu.roll(pr, 7, 0)
                po = pltpu.roll(v * left[x, :, span], 4, 0) + mine * pr[0:1, :]
                at = pl.ds(pl.multiple_of(i * PLANE + m * SLAB, SLAB), SLAB)
                bands, low = -po[0:4, :], -pr[4:5, :]
                if delta % 2:
                    cross[delta // 2 * 4 : delta // 2 * 4 + 4, at] = bands
                    cross[8 + delta // 2 : 9 + delta // 2, at] = low
                else:
                    (near0, near2)[delta // 2][:, at] = bands
                    (low0, low2)[delta // 2][:, at] = low
            return carry

        lax.fori_loop(0, QX, finish, 0)


VMEM_SPEC = pl.BlockSpec(memory_space=pltpu.VMEM)
SMEM_SPEC = pl.BlockSpec(memory_space=pltpu.SMEM)
SPLIT = [pltpu.VMEM((NG * 8, PLANE), BF16)] * 2


def spectrum(q, bands, tables):
    return pl.pallas_call(
        spectrum_kernel,
        out_shape=[jax.ShapeDtypeStruct((NG, 8, PLANE), F32)] * 2 + [jax.ShapeDtypeStruct((NG * 8, PLANE), F32)],
        in_specs=[SMEM_SPEC] + [VMEM_SPEC] * 10,
        out_specs=[VMEM_SPEC] * 3,
        scratch_shapes=SPLIT,
        name="spectrum",
        compiler_params=pltpu.CompilerParams(vmem_limit_bytes=24 << 20),
    )(q.reshape(1), *bands, jnp.asarray(kernel_values()), jnp.asarray(thirds()), *tables)


def terms(q, right, left, field, tables):
    return pl.pallas_call(
        terms_kernel,
        out_shape=[jax.ShapeDtypeStruct(shape, F32) for shape in [(4, QCELL)] * 2 + [(10, QCELL)] + [(1, QCELL)] * 2],
        in_specs=[SMEM_SPEC] + [VMEM_SPEC] * 6,
        out_specs=[VMEM_SPEC] * 5,
        scratch_shapes=SPLIT + [pltpu.VMEM((NG * 8, PLANE), F32)],
        name="terms",
        compiler_params=pltpu.CompilerParams(vmem_limit_bytes=28 << 20),
    )(q.reshape(1), right, left, field, jnp.asarray(thirds()), *tables)


BOTH = ("band", "grid")
CHUNK = QCELL // 4


def small_call(body, outs, scratch=(), limit=8):
    vmem = pl.BlockSpec(memory_space=pltpu.VMEM)

    def call(where, *arrays):
        return pl.pallas_call(
            body,
            out_shape=[jax.ShapeDtypeStruct(shape, F32) for shape in outs],
            in_specs=[pl.BlockSpec(memory_space=pltpu.SMEM)] + [vmem] * len(arrays),
            out_specs=[vmem] * len(outs),
            scratch_shapes=list(scratch),
            compiler_params=pltpu.CompilerParams(vmem_limit_bytes=limit << 20),
        )(where, *arrays)

    return call


def chunk_of(where, k):
    return pl.ds(pl.multiple_of((where[2] ^ k) * CHUNK, 128), CHUNK)


def prepare_kernel(where, orbitals, sel_a, sel_b, *chunks):
    lower = where[0] < 2
    a, b = orbitals[0:2, :], orbitals[2:4, :]
    sel_a[...] = jnp.where(lower, a, b)
    sel_b[...] = jnp.where(lower, b, a)
    for k in range(4):
        chunks[k][...] = orbitals[:, chunk_of(where, k)]


def stack_kernel(where, two, low_a, low_b, out):
    out[0:4, :] = two[...]
    out[4:6, :] = low_a[...]
    out[6:8, :] = low_b[...]


def merge_kernel(where, near0, near2, low0, low2, across, near, far, owed_a, owed_b):
    first = where[0] % 2 == 0
    near[...] = near0[...] + across[0:4, :]
    far[...] = near2[...] + across[4:8, :]
    for out, low, row in ((owed_a, low0, 8), (owed_b, low2, 9)):
        a, b = low[...], across[row : row + 1, :]
        out[0:1, :] = jnp.where(first, a, b)
        out[1:2, :] = jnp.where(first, b, a)


def finalize_kernel(where, near, far, owed_a, owed_b, vectors, *chunks):
    lower = where[0] < 2
    a, b = owed_a[...], owed_b[...]
    total = near[...] + far[...]
    vectors[0:2, :] = total[0:2, :] + jnp.where(lower, a, b)
    vectors[2:4, :] = total[2:4, :] + jnp.where(lower, b, a)
    for k in range(4):
        chunks[k][...] = vectors[:, chunk_of(where, k)]


def pair_kernel(where, f0, f1, f2, f3, other, out):
    first = where[3] == 0
    for k, f in enumerate((f0, f1, f2, f3)):
        a, b = f[...], other[4 * k : 4 * k + 4, :]
        out[8 * k : 8 * k + 4, :] = jnp.where(first, a, b)
        out[8 * k + 4 : 8 * k + 8, :] = jnp.where(first, b, a)


def margin_kernel(where, p0, p1, p3, p2a, p2b, v0, v1, v2, v3, pieces, block):
    z, y = where[1], where[2]

    def halves(a):
        top = a.astype(BF16)
        return top, (a - top.astype(F32)).astype(BF16)

    vt, vl = halves(jnp.concatenate([v0[...], v1[...], v2[...], v3[...]], axis=0))
    dims = (((1,), (1,)), ((), ()))
    parts = jnp.concatenate([p0[...], p1[...], p2a[...], p2b[...], p3[...]], axis=0)
    ft, fl = halves(parts)
    got = (
        lax.dot_general(ft, vt, dims, preferred_element_type=F32)
        + lax.dot_general(fl, vt, dims, preferred_element_type=F32)
        + lax.dot_general(ft, vl, dims, preferred_element_type=F32)
    )
    for dz in range(4):
        for dy in range(4):
            row = 32 * dz + 8 * dy
            block[(z + 4 - dz) % 4 * 4 + (y ^ dy), :, :] = got[row : row + 8, :]
    out = block[...].reshape(128, 16).T * (1.0 / NCELL)
    turned = [out] + [pltpu.roll(out, 32 * r, 1) for r in (1, 2, 3)]
    third_of = lax.broadcasted_iota(jnp.int32, (16, 128), 1) // 32
    keep = third_of == lax.broadcasted_iota(jnp.int32, (16, 128), 0) % 4
    for q_to in range(4):
        picked = turned[(3 - q_to) % 4]
        for j in range(3):
            picked = jnp.where(third_of == j, turned[(j - q_to) % 4], picked)
        picked = jnp.where(keep, picked, 0.0)
        for dy in range(4):
            row = jnp.sum(picked[4 * dy : 4 * dy + 4, :], axis=0, keepdims=True)
            pieces[pl.ds((y ^ dy) * 4 + q_to, 1), :] = row


def move(value, target):
    nb, nq = lax.axis_size("band"), lax.axis_size("grid")
    pairs = []
    for b in range(nb):
        for q in range(nq):
            z, y, h, q_to = target(b // 8, b // 2 % 4, b % 2, q)
            pairs.append((b * nq + q, ((z % 4) * 8 + (y % 4) * 2 + h) * nq + q_to))
    return lax.ppermute(value, BOTH, pairs)


def along_y(value, flip):
    return move(value, lambda z, y, h, q: (z, y ^ flip, h, q))


def along_z(value, k):
    return move(value, lambda z, y, h, q: (z + k, y, h, q))


def within(value, flip):
    return move(value, lambda z, y, h, q: (z, y, h, q ^ flip))


def around(value, blocks, flip):
    def target(z, y, h, q):
        b = (z * 8 + y * 2 + h + blocks) % 32
        return b // 8, b // 2 % 4, b % 2, q ^ flip

    return move(value, target)


def step(orbitals):
    b = lax.axis_index("band").astype(jnp.int32)
    q = lax.axis_index("grid").astype(jnp.int32)
    where = jnp.stack([q, b // 8, b // 2 % 4, b % 2])
    two = within(orbitals, 2)
    prepare = small_call(prepare_kernel, [(2, QCELL)] * 2 + [(4, CHUNK)] * 4)
    sel_a, sel_b, *pc = prepare(where, orbitals)
    low_a = around(sel_a, 1, 0)
    low_b = around(sel_b, 1, 2)
    one = within(orbitals, 1)
    pieces = [pc[0]] + [along_y(pc[k], k) for k in (1, 2, 3)]
    tables = plane_tables()
    together = jnp.concatenate(pieces, axis=0)
    two, together = lax.optimization_barrier((two, together))
    (stacked,) = small_call(stack_kernel, [(8, QCELL)])(where, two, low_a, low_b)
    core = within(stacked, 1)
    other = move(together, lambda z, y, h, q: (z, y, 1 - h, q))
    right, left, field = spectrum(q, (orbitals, two, one, low_a, low_b, core), tables[:2])
    (p0,) = small_call(pair_kernel, [(32, CHUNK)])(where, *pieces, other)
    p1 = along_z(p0, 1)
    p3 = along_z(p0, 3)
    near0, near2, cross, low0, low2 = terms(q, right, left, field, tables[2:])
    across = within(cross, 1)
    merge = small_call(merge_kernel, [(4, QCELL)] * 2 + [(2, QCELL)] * 2)
    near, both, owe_a, owe_b = merge(where, near0, near2, low0, low2, across)
    far = within(both, 2)
    owed_a = around(owe_a, -1, 0)
    owed_b = around(owe_b, -1, 2)
    p2a = along_z(p1[:16], 1)
    p2b = along_z(p3[16:], 3)
    finalize = small_call(finalize_kernel, [(4, QCELL)] + [(4, CHUNK)] * 4)
    vectors, *vc = finalize(where, near, far, owed_a, owed_b)
    given = [vc[0]] + [along_y(vc[k], k) for k in (1, 2, 3)]
    margin_part = small_call(margin_kernel, [(16, 128)], [pltpu.VMEM((16, 8, 16), F32)], 20)
    (sums,) = margin_part(where, p0, p1, p3, p2a, p2b, *given)
    groups = [[(z * 8 + y * 2 + h) * 4 + p for y in range(4) for p in range(4)] for z in range(4) for h in range(2)]
    sums = lax.all_to_all(sums, BOTH, 0, 0, tiled=True, axis_index_groups=groups)
    margin = jnp.sum(sums, axis=0).reshape(4, 32).T
    return vectors, margin


def solution(mesh):
    return jax.shard_map(
        step,
        mesh=mesh,
        in_specs=(P("band", "grid"),),
        out_specs=(P("band", "grid"), P("grid", "band")),
        check_vma=False,
    )
```

```python
import math

import jax
import jax.numpy as jnp
import numpy as np
from jax import lax
from jax.experimental import pallas as pl
from jax.experimental.pallas import tpu as pltpu
from jax.sharding import PartitionSpec as P

NG = 48
NCELL = 110592
PLANE = NG * NG
SLAB = 768
QX = 12
QCELL = QX * PLANE
F32 = jnp.float32
BF16 = jnp.bfloat16
R2 = math.sqrt(0.5)
C1 = math.cos(math.pi / 8)
C3 = math.cos(3 * math.pi / 8)
S3 = math.sqrt(3.0) / 2

ORDER = [("C", b) for b in range(9)] + [("S", b) for b in range(1, 8)]
SWAPPED = [("C", 0)] + [("S", b) for b in range(1, 8)] + [("C", 8)] + [("C", b) for b in range(1, 8)]


def sixteen(order):
    u = np.arange(16)
    cols = []
    for kind, b in order:
        col = np.cos(2 * np.pi * b * u / 16) if kind == "C" else np.sin(2 * np.pi * b * u / 16)
        cols.append(col / np.linalg.norm(col))
    return np.stack(cols, 1)


def forty_eight():
    z = np.arange(NG)
    cols, freqs = [], []
    for g in range(25):
        for kind in ("C", "S") if 0 < g < 24 else ("C",):
            col = np.cos(2 * np.pi * g * z / NG) if kind == "C" else np.sin(2 * np.pi * g * z / NG)
            cols.append(col / np.linalg.norm(col))
            freqs.append(g)
    return np.stack(cols, 1), np.array(freqs)


def folded(g):
    return (g + 24) % 48 - 24


def x_basis():
    keys, freqs, norms = [], [], []
    for b in range(9):
        keys.append(("A", "C", b)); freqs.append(3 * b); norms.append(48 if b in (0, 8) else 24)
    for b in range(1, 8):
        keys.append(("A", "S", b)); freqs.append(3 * b); norms.append(24)
    for b in (0, 8):
        for t in "cs":
            keys.append((t, "C", b)); freqs.append(16 + 3 * b); norms.append(24)
    for b in range(1, 8):
        for sign in (1, -1):
            for kind in ("cos", "sin"):
                keys.append((kind, sign, b)); freqs.append(16 + 3 * sign * b); norms.append(24)
    return keys, np.array(freqs), np.array(norms)


def kernel_values():
    _, gx, nx = x_basis()
    _, gz = forty_eight()
    gy = []
    for slab in "Auv":
        for kind, b in ORDER:
            if slab == "A":
                gy.append(3 * b)
            elif b in (0, 8):
                gy.append(16 + 3 * b)
            else:
                plus = (slab == "u") == (kind == "C")
                gy.append(16 + 3 * b if plus else 16 - 3 * b)
    gy = np.array(gy)
    q = (folded(gx)[:, None, None] ** 2 + folded(gy)[None, :, None] ** 2 + folded(gz)[None, None, :] ** 2).astype(np.float64)
    kern = np.where(q > 0, 40.0 * (1.0 - np.exp(-q / 16.0)) / np.where(q > 0, q, 1.0), 0.0)
    return (kern / (3.0 * nx[:, None, None])).reshape(NG, PLANE).astype(np.float32)


def thirds():
    u = np.arange(SLAB) // NG
    rows = [np.cos(2 * np.pi * (m + u) / 3) for m in range(3)] + [np.sin(2 * np.pi * (m + u) / 3) for m in range(3)]
    return np.concatenate([np.stack(rows), np.zeros((2, SLAB))]).astype(np.float32)


def factor_tables():
    za, _ = forty_eight()
    ta, ts = sixteen(ORDER), sixteen(SWAPPED)
    tens = np.stack([np.repeat(t, NG, 1) for t in (ta, ts, ta.T, ts.T)])
    zs = np.stack([np.tile(z, (1, 16)) for z in (za, za.T)])
    return [a.astype(np.float32) for a in (tens, zs)]


def tables_kernel(tens, zs, hi_there, lo_there, hi_back, lo_back):
    for way, (hi, lo) in enumerate(((hi_there, lo_there), (hi_back, lo_back))):
        for which in range(2):

            def block(u, carry):
                w = zs[way] * tens[2 * way + which, pl.ds(u, 1), :]
                top = w.astype(BF16)
                rows = pl.ds(pl.multiple_of(u * NG, 16), NG)
                hi[which, rows, :] = top
                lo[which, rows, :] = (w - top.astype(F32)).astype(BF16)
                return carry

            lax.fori_loop(0, 16, block, 0)


def plane_tables():
    out = [jax.ShapeDtypeStruct((2, SLAB, SLAB), BF16)] * 4
    return pl.pallas_call(
        tables_kernel, out_shape=out, name="plane_tables",
        compiler_params=pltpu.CompilerParams(vmem_limit_bytes=16 << 20),
    )(*[jnp.asarray(a) for a in factor_tables()])


def t16(f):
    o = [f[u] - f[u + 8] for u in range(8)]
    e = [f[u] + f[u + 8] for u in range(8)]
    ee = [e[u] + e[u + 4] for u in range(4)]
    eo = [e[u] - e[u + 4] for u in range(4)]
    c, s = {}, {}
    p0, p1 = ee[0] + ee[2], ee[1] + ee[3]
    c[0], c[8], c[4], s[4] = p0 + p1, p0 - p1, ee[0] - ee[2], ee[1] - ee[3]
    d, a = R2 * (eo[1] - eo[3]), R2 * (eo[1] + eo[3])
    c[2], c[6], s[2], s[6] = eo[0] + d, eo[0] - d, a + eo[2], a - eo[2]
    d1, d2, d3 = (o[u] - o[8 - u] for u in (1, 2, 3))
    s1, s2, s3 = (o[u] + o[8 - u] for u in (1, 2, 3))
    d2, s2 = R2 * d2, R2 * s2
    e1, e3 = o[0] + d2, o[0] - d2
    o1, o3 = C1 * d1 + C3 * d3, C3 * d1 - C1 * d3
    c[1], c[7], c[3], c[5] = e1 + o1, e1 - o1, e3 + o3, e3 - o3
    x1, x3 = o[4] + s2, o[4] - s2
    y1, y3 = C3 * s1 + C1 * s3, C1 * s1 - C3 * s3
    s[1], s[7], s[3], s[5] = y1 + x1, y1 - x1, y3 - x3, y3 + x3
    return c, s


def t16_back(c, s):
    e1, o1, e3, o3 = c[1] + c[7], c[1] - c[7], c[3] + c[5], c[3] - c[5]
    o0, d2 = e1 + e3, R2 * (e1 - e3)
    d1, d3 = C1 * o1 + C3 * o3, C3 * o1 - C1 * o3
    y1, x1, y3, x3 = s[1] + s[7], s[1] - s[7], s[3] + s[5], s[5] - s[3]
    o4, s2 = x1 + x3, R2 * (x1 - x3)
    s1, s3 = C3 * y1 + C1 * y3, C1 * y1 - C3 * y3
    o = [o0, d1 + s1, d2 + s2, d3 + s3, o4, s3 - d3, s2 - d2, s1 - d1]
    d, a = R2 * (c[2] - c[6]), R2 * (s[2] + s[6])
    eo = [c[2] + c[6], d + a, s[2] - s[6], a - d]
    p0, p1 = c[0] + c[8], c[0] - c[8]
    ee = [p0 + c[4], p1 + s[4], p0 - c[4], p1 - s[4]]
    e = [ee[u] + eo[u] for u in range(4)] + [ee[u] - eo[u] for u in range(4)]
    return [e[u] + o[u] for u in range(8)] + [e[u] - o[u] for u in range(8)]


def convolve_x(f, table):
    keys, _, _ = x_basis()
    row = {key: k for k, key in enumerate(keys)}
    place = {(x % 3, x % 16): x for x in range(NG)}
    part = {"A": [], "c": [], "s": []}
    for u in range(16):
        f0, f1, f2 = (f[place[t, u]] for t in range(3))
        a = f1 + f2
        part["A"].append(f0 + a)
        part["c"].append(f0 - 0.5 * a)
        part["s"].append(S3 * (f1 - f2))
    c, s = t16(part["A"])
    c = {b: v * table(row["A", "C", b]) for b, v in c.items()}
    s = {b: v * table(row["A", "S", b]) for b, v in s.items()}
    back_a = t16_back(c, s)
    cc, cs = t16(part["c"])
    sc, ss = t16(part["s"])
    for b in (0, 8):
        cc[b] = cc[b] * table(row["c", "C", b])
        sc[b] = sc[b] * table(row["s", "C", b])
    for b in range(1, 8):
        p = (cc[b] - ss[b]) * table(row["cos", 1, b])
        m = (cc[b] + ss[b]) * table(row["cos", -1, b])
        cc[b], ss[b] = p + m, m - p
        p = (sc[b] + cs[b]) * table(row["sin", 1, b])
        m = (sc[b] - cs[b]) * table(row["sin", -1, b])
        sc[b], cs[b] = p + m, p - m
    back_c, back_s = t16_back(cc, cs), t16_back(sc, ss)
    out = [None] * NG
    for u in range(16):
        a, c_, s_ = back_a[u], back_c[u], S3 * back_s[u]
        h = a - 0.5 * c_
        out[place[0, u]] = a + c_
        out[place[1, u]] = h + s_
        out[place[2, u]] = h - s_
    return out


def split(hi, lo, rows, m, value):
    top = value.astype(BF16)
    span = slice(m * SLAB, (m + 1) * SLAB)
    hi[rows, span] = top
    lo[rows, span] = (value - top.astype(F32)).astype(BF16)


def product(hi, lo, whi, wlo, m, k, cols):
    span = slice(m * SLAB, (m + 1) * SLAB)
    a, b = hi[:, span], lo[:, span]
    lhs = jnp.concatenate([a, b, a], axis=1)
    w = jnp.concatenate([whi[k, :, cols], whi[k, :, cols], wlo[k, :, cols]], axis=0)
    return jnp.dot(lhs, w, preferred_element_type=F32)


def spectrum_kernel(q_ref, own, two, one, low_a, low_b, core, kern, third, whi, wlo, right, left, field, hi, lo):
    q = q_ref[0]
    sources = (
        (own, 0, low_a, 0),
        (one, 0, core, 4),
        (two, 0, low_b, 0),
        (core, 0, core, 6),
    )
    for delta, (bands_ref, first, low_ref, low_first) in enumerate(sources):
        base = (q ^ delta) * QX

        def place(x, carry):
            span = pl.ds(pl.multiple_of(x * PLANE, 128), PLANE)
            bands = bands_ref[first : first + 4, span]
            right[base + x, 0:4, :] = bands
            right[base + x, 4:8, :] = bands
            left[base + x, 0:4, :] = jnp.broadcast_to(bands_ref[pl.ds(first + q, 1), span], (4, PLANE))
            left[base + x, 4:8, :] = jnp.broadcast_to(low_ref[pl.ds(low_first + q % 2, 1), span], (4, PLANE))
            return carry

        lax.fori_loop(0, QX, place, 0)

    def densities(i, carry):
        x = pl.ds(2 * i, 2)
        rows = pl.ds(pl.multiple_of(16 * i, 16), 16)
        f = []
        for m in range(3):
            span = slice(m * SLAB, (m + 1) * SLAB)
            f.append((right[x, :, span] * left[x, :, span]).reshape(16, SLAB))
        split(hi, lo, rows, 0, f[0] + f[1] + f[2])
        split(hi, lo, rows, 1, f[0] * third[0:1, :] + f[1] * third[1:2, :] + f[2] * third[2:3, :])
        split(hi, lo, rows, 2, f[0] * third[3:4, :] + f[1] * third[4:5, :] + f[2] * third[5:6, :])
        return carry

    lax.fori_loop(0, NG // 2, densities, 0)

    for j in range(3):
        cols = slice(j * 256, (j + 1) * 256)
        field[:, cols] = product(hi, lo, whi, wlo, 0, 0, cols)
        c = product(hi, lo, whi, wlo, 1, 0, cols)
        s = product(hi, lo, whi, wlo, 2, 1, cols)
        field[:, SLAB + j * 256 : SLAB + (j + 1) * 256] = c - s
        field[:, 2 * SLAB + j * 256 : 2 * SLAB + (j + 1) * 256] = c + s

    def along_x(i, carry):
        span = pl.ds(pl.multiple_of(128 * i, 128), 128)
        f = [field[8 * x : 8 * x + 8, span] for x in range(NG)]
        out = convolve_x(f, lambda k: kern[k : k + 1, span])
        for x in range(NG):
            field[8 * x : 8 * x + 8, span] = out[x]
        return carry

    lax.fori_loop(0, PLANE // 128, along_x, 0)


def terms_kernel(q_ref, right, left, field, third, whi, wlo, near0, near2, cross, low0, low2, hi, lo, back):
    q = q_ref[0]

    def unmix(i, carry):
        rows = pl.ds(pl.multiple_of(16 * i, 16), 16)
        u = field[rows, SLAB : 2 * SLAB]
        v = field[rows, 2 * SLAB : 3 * SLAB]
        split(hi, lo, rows, 0, field[rows, 0:SLAB])
        split(hi, lo, rows, 1, u + v)
        split(hi, lo, rows, 2, v - u)
        return carry

    lax.fori_loop(0, NG // 2, unmix, 0)
    for j in range(3):
        cols = slice(j * 256, (j + 1) * 256)
        for m, k in ((0, 0), (1, 0), (2, 1)):
            back[:, m * SLAB + j * 256 : m * SLAB + (j + 1) * 256] = product(hi, lo, whi, wlo, m, k, cols)

    mine = (lax.broadcasted_iota(jnp.int32, (8, SLAB), 0) == q).astype(F32)

    for delta in range(4):
        base = (q ^ delta) * QX

        def finish(i, carry):
            x = base + i
            rows = pl.ds(pl.multiple_of(x * 8, 8), 8)
            a = back[rows, 0:SLAB]
            c = back[rows, SLAB : 2 * SLAB]
            s = back[rows, 2 * SLAB : 3 * SLAB]
            for m in range(3):
                span = slice(m * SLAB, (m + 1) * SLAB)
                v = a + c * third[m : m + 1, :] + s * third[3 + m : 4 + m, :]
                pr = v * right[x, :, span]
                pr = pr + pltpu.roll(pr, 6, 0)
                pr = pr + pltpu.roll(pr, 7, 0)
                po = pltpu.roll(v * left[x, :, span], 4, 0) + mine * pr[0:1, :]
                at = pl.ds(pl.multiple_of(i * PLANE + m * SLAB, SLAB), SLAB)
                bands, low = -po[0:4, :], -pr[4:5, :]
                if delta % 2:
                    cross[delta // 2 * 4 : delta // 2 * 4 + 4, at] = bands
                    cross[8 + delta // 2 : 9 + delta // 2, at] = low
                else:
                    (near0, near2)[delta // 2][:, at] = bands
                    (low0, low2)[delta // 2][:, at] = low
            return carry

        lax.fori_loop(0, QX, finish, 0)


VMEM_SPEC = pl.BlockSpec(memory_space=pltpu.VMEM)
SMEM_SPEC = pl.BlockSpec(memory_space=pltpu.SMEM)
SPLIT = [pltpu.VMEM((NG * 8, PLANE), BF16)] * 2


def spectrum(q, bands, tables):
    return pl.pallas_call(
        spectrum_kernel,
        out_shape=[jax.ShapeDtypeStruct((NG, 8, PLANE), F32)] * 2 + [jax.ShapeDtypeStruct((NG * 8, PLANE), F32)],
        in_specs=[SMEM_SPEC] + [VMEM_SPEC] * 10,
        out_specs=[VMEM_SPEC] * 3,
        scratch_shapes=SPLIT,
        name="spectrum",
        compiler_params=pltpu.CompilerParams(vmem_limit_bytes=24 << 20),
    )(q.reshape(1), *bands, jnp.asarray(kernel_values()), jnp.asarray(thirds()), *tables)


def terms(q, right, left, field, tables):
    return pl.pallas_call(
        terms_kernel,
        out_shape=[jax.ShapeDtypeStruct(shape, F32) for shape in [(4, QCELL)] * 2 + [(10, QCELL)] + [(1, QCELL)] * 2],
        in_specs=[SMEM_SPEC] + [VMEM_SPEC] * 6,
        out_specs=[VMEM_SPEC] * 5,
        scratch_shapes=SPLIT + [pltpu.VMEM((NG * 8, PLANE), F32)],
        name="terms",
        compiler_params=pltpu.CompilerParams(vmem_limit_bytes=28 << 20),
    )(q.reshape(1), right, left, field, jnp.asarray(thirds()), *tables)


BOTH = ("band", "grid")
CHUNK = QCELL // 4


def small_call(body, outs, scratch=(), limit=8):
    vmem = pl.BlockSpec(memory_space=pltpu.VMEM)

    def call(where, *arrays):
        return pl.pallas_call(
            body,
            out_shape=[jax.ShapeDtypeStruct(shape, F32) for shape in outs],
            in_specs=[pl.BlockSpec(memory_space=pltpu.SMEM)] + [vmem] * len(arrays),
            out_specs=[vmem] * len(outs),
            scratch_shapes=list(scratch),
            compiler_params=pltpu.CompilerParams(vmem_limit_bytes=limit << 20),
        )(where, *arrays)

    return call


def chunk_of(where, k):
    return pl.ds(pl.multiple_of((where[2] ^ k) * CHUNK, 128), CHUNK)


def rows_kernel(where, orbitals, sel_a, sel_b):
    lower = where[0] < 2
    a, b = orbitals[0:2, :], orbitals[2:4, :]
    sel_a[...] = jnp.where(lower, a, b)
    sel_b[...] = jnp.where(lower, b, a)


def chunks_kernel(where, orbitals, *chunks):
    for k in range(4):
        chunks[k][...] = orbitals[:, chunk_of(where, k)]


def stack_kernel(where, two, low_a, low_b, out):
    out[0:4, :] = two[...]
    out[4:6, :] = low_a[...]
    out[6:8, :] = low_b[...]


def merge_kernel(where, near0, near2, low0, low2, across, near, far, owed_a, owed_b):
    first = where[0] % 2 == 0
    near[...] = near0[...] + across[0:4, :]
    far[...] = near2[...] + across[4:8, :]
    for out, low, row in ((owed_a, low0, 8), (owed_b, low2, 9)):
        a, b = low[...], across[row : row + 1, :]
        out[0:1, :] = jnp.where(first, a, b)
        out[1:2, :] = jnp.where(first, b, a)


def total_of(where, near, far, owed_a, owed_b, span):
    lower = where[0] < 2
    a, b = owed_a[:, span], owed_b[:, span]
    owed = jnp.concatenate([jnp.where(lower, a, b), jnp.where(lower, b, a)], axis=0)
    return near[:, span] + far[:, span] + owed


def finalize_kernel(where, near, far, owed_a, owed_b, *chunks):
    for k in (1, 2, 3, 0):
        chunks[k][...] = total_of(where, near, far, owed_a, owed_b, chunk_of(where, k))


def vectors_kernel(where, near, far, owed_a, owed_b, vectors):
    for c in range(4):
        span = pl.ds(c * CHUNK, CHUNK)
        vectors[:, span] = total_of(where, near, far, owed_a, owed_b, span)


def pair_kernel(where, f0, f1, f2, f3, other, out):
    first = where[3] == 0
    for k, f in enumerate((f0, f1, f2, f3)):
        a, b = f[...], other[4 * k : 4 * k + 4, :]
        out[8 * k : 8 * k + 4, :] = jnp.where(first, a, b)
        out[8 * k + 4 : 8 * k + 8, :] = jnp.where(first, b, a)


def margin_kernel(where, p0, p1, p3, p2a, p2b, v0, v1, v2, v3, pieces, block):
    z, y = where[1], where[2]

    def halves(a):
        top = a.astype(BF16)
        return top, (a - top.astype(F32)).astype(BF16)

    vt, vl = halves(jnp.concatenate([v0[...], v1[...], v2[...], v3[...]], axis=0))
    dims = (((1,), (1,)), ((), ()))
    parts = jnp.concatenate([p0[...], p1[...], p2a[...], p2b[...], p3[...]], axis=0)
    ft, fl = halves(parts)
    got = (
        lax.dot_general(ft, vt, dims, preferred_element_type=F32)
        + lax.dot_general(fl, vt, dims, preferred_element_type=F32)
        + lax.dot_general(ft, vl, dims, preferred_element_type=F32)
    )
    for dz in range(4):
        for dy in range(4):
            row = 32 * dz + 8 * dy
            block[(z + 4 - dz) % 4 * 4 + (y ^ dy), :, :] = got[row : row + 8, :]
    out = block[...].reshape(128, 16).T * (1.0 / NCELL)
    turned = [out] + [pltpu.roll(out, 32 * r, 1) for r in (1, 2, 3)]
    third_of = lax.broadcasted_iota(jnp.int32, (16, 128), 1) // 32
    keep = third_of == lax.broadcasted_iota(jnp.int32, (16, 128), 0) % 4
    for q_to in range(4):
        picked = turned[(3 - q_to) % 4]
        for j in range(3):
            picked = jnp.where(third_of == j, turned[(j - q_to) % 4], picked)
        picked = jnp.where(keep, picked, 0.0)
        for dy in range(4):
            row = jnp.sum(picked[4 * dy : 4 * dy + 4, :], axis=0, keepdims=True)
            pieces[pl.ds((y ^ dy) * 4 + q_to, 1), :] = row


def move(value, target):
    nb, nq = lax.axis_size("band"), lax.axis_size("grid")
    pairs = []
    for b in range(nb):
        for q in range(nq):
            z, y, h, q_to = target(b // 8, b // 2 % 4, b % 2, q)
            pairs.append((b * nq + q, ((z % 4) * 8 + (y % 4) * 2 + h) * nq + q_to))
    return lax.ppermute(value, BOTH, pairs)


def along_y(value, flip):
    return move(value, lambda z, y, h, q: (z, y ^ flip, h, q))


def along_z(value, k):
    return move(value, lambda z, y, h, q: (z + k, y, h, q))


def within(value, flip):
    return move(value, lambda z, y, h, q: (z, y, h, q ^ flip))


def around(value, blocks, flip):
    def target(z, y, h, q):
        b = (z * 8 + y * 2 + h + blocks) % 32
        return b // 8, b // 2 % 4, b % 2, q ^ flip

    return move(value, target)


def step(orbitals):
    b = lax.axis_index("band").astype(jnp.int32)
    q = lax.axis_index("grid").astype(jnp.int32)
    where = jnp.stack([q, b // 8, b // 2 % 4, b % 2])
    rows = small_call(rows_kernel, [(2, QCELL)] * 2)
    sel_a, sel_b = rows(where, orbitals)
    low_a = around(sel_a, 1, 0)
    low_b = around(sel_b, 1, 2)
    two = within(orbitals, 2)
    one = within(orbitals, 1)
    pc = small_call(chunks_kernel, [(4, CHUNK)] * 4)(where, orbitals)
    pieces = [pc[0]] + [along_y(pc[k], k) for k in (1, 2, 3)]
    tables = plane_tables()
    together = jnp.concatenate(pieces, axis=0)
    (stacked,) = small_call(stack_kernel, [(8, QCELL)])(where, two, low_a, low_b)
    core = within(stacked, 1)
    other = move(together, lambda z, y, h, q: (z, y, 1 - h, q))
    right, left, field = spectrum(q, (orbitals, two, one, low_a, low_b, core), tables[:2])
    (p0,) = small_call(pair_kernel, [(32, CHUNK)])(where, *pieces, other)
    p1 = along_z(p0, 1)
    p3 = along_z(p0, 3)
    near0, near2, cross, low0, low2 = terms(q, right, left, field, tables[2:])
    across = within(cross, 1)
    merge = small_call(merge_kernel, [(4, QCELL)] * 2 + [(2, QCELL)] * 2)
    near, both, owe_a, owe_b = merge(where, near0, near2, low0, low2, across)
    far = within(both, 2)
    owed_a = around(owe_a, -1, 0)
    owed_b = around(owe_b, -1, 2)
    p2a = along_z(p1[:16], 1)
    p2b = along_z(p3[16:], 3)
    finalize = small_call(finalize_kernel, [(4, CHUNK)] * 4)
    vc = finalize(where, near, far, owed_a, owed_b)
    (vectors,) = small_call(vectors_kernel, [(4, QCELL)])(where, near, far, owed_a, owed_b)
    given = [vc[0]] + [along_y(vc[k], k) for k in (1, 2, 3)]
    margin_part = small_call(margin_kernel, [(16, 128)], [pltpu.VMEM((16, 8, 16), F32)], 20)
    (sums,) = margin_part(where, p0, p1, p3, p2a, p2b, *given)
    groups = [[(z * 8 + y * 2 + h) * 4 + p for y in range(4) for p in range(4)] for z in range(4) for h in range(2)]
    sums = lax.all_to_all(sums, BOTH, 0, 0, tiled=True, axis_index_groups=groups)
    margin = jnp.sum(sums, axis=0).reshape(4, 32).T
    return vectors, margin


def solution(mesh):
    return jax.shard_map(
        step,
        mesh=mesh,
        in_specs=(P("band", "grid"),),
        out_specs=(P("band", "grid"), P("grid", "band")),
        check_vma=False,
    )
```

```python
import math

import jax
import jax.numpy as jnp
import numpy as np
from jax import lax
from jax.experimental import pallas as pl
from jax.experimental.pallas import tpu as pltpu
from jax.sharding import PartitionSpec as P

NG = 48
NCELL = 110592
PLANE = NG * NG
SLAB = 768
QX = 12
QCELL = QX * PLANE
F32 = jnp.float32
BF16 = jnp.bfloat16
R2 = math.sqrt(0.5)
C1 = math.cos(math.pi / 8)
C3 = math.cos(3 * math.pi / 8)
S3 = math.sqrt(3.0) / 2

ORDER = [("C", b) for b in range(9)] + [("S", b) for b in range(1, 8)]
SWAPPED = [("C", 0)] + [("S", b) for b in range(1, 8)] + [("C", 8)] + [("C", b) for b in range(1, 8)]


def sixteen(order):
    u = np.arange(16)
    cols = []
    for kind, b in order:
        col = np.cos(2 * np.pi * b * u / 16) if kind == "C" else np.sin(2 * np.pi * b * u / 16)
        cols.append(col / np.linalg.norm(col))
    return np.stack(cols, 1)


def folded(g):
    return (g + 24) % 48 - 24


def x_basis():
    keys, freqs, norms = [], [], []
    for b in range(9):
        keys.append(("A", "C", b)); freqs.append(3 * b); norms.append(48 if b in (0, 8) else 24)
    for b in range(1, 8):
        keys.append(("A", "S", b)); freqs.append(3 * b); norms.append(24)
    for b in (0, 8):
        for t in "cs":
            keys.append((t, "C", b)); freqs.append(16 + 3 * b); norms.append(24)
    for b in range(1, 8):
        for sign in (1, -1):
            for kind in ("cos", "sin"):
                keys.append((kind, sign, b)); freqs.append(16 + 3 * sign * b); norms.append(24)
    return keys, np.array(freqs), np.array(norms)


def lane_freqs(group):
    out = []
    for kind, b in ORDER:
        if group == "A":
            out.append(3 * b)
        elif b in (0, 8):
            out.append(16 + 3 * b)
        else:
            out.append(16 + 3 * b if (group == "u") == (kind == "C") else 16 - 3 * b)
    return np.array(out)


def kernel_values():
    _, gx, nx = x_basis()
    g = np.stack([lane_freqs(group) for group in "Auv"])
    gy, gz = g[:, None, :, None], g[None, :, None, :]
    q = folded(gx)[:, None, None, None, None] ** 2 + (folded(gy) ** 2 + folded(gz) ** 2)[None]
    q = q.astype(np.float64)
    kern = np.where(q > 0, 40.0 * (1.0 - np.exp(-q / 16.0)) / np.where(q > 0, q, 1.0), 0.0)
    return (kern / (9.0 * nx[:, None, None, None, None])).reshape(NG, PLANE).astype(np.float32)


PLACES = np.array([0, 3, 6, 1, 4, 7, 2, 5])
LANE_Y = np.repeat(np.concatenate([PLACES, 8 + PLACES]), 16)
LANE_Z = np.tile(np.arange(16), 16)


def thirds():
    rows = []
    for lane in (LANE_Y, LANE_Z):
        rows += [np.cos(2 * np.pi * (m + lane) / 3) for m in range(3)]
        rows += [np.sin(2 * np.pi * (m + lane) / 3) for m in range(3)]
    return np.concatenate([np.stack(rows), np.zeros((4, 256))]).astype(np.float32)


def factor_tables():
    bases = sixteen(ORDER), sixteen(SWAPPED)
    slow = [np.repeat(t[LANE_Y[::16]], 16, 1) for t in bases] + [t.T[:, LANE_Y] for t in bases]
    fast = [np.tile(t, (1, 16)) for t in bases] + [np.tile(t.T, (1, 16)) for t in bases]
    return np.stack(slow).astype(np.float32), np.stack(fast).astype(np.float32)


def tables_kernel(slow, fast, hi_there, lo_there, hi_back, lo_back):
    for way, (hi, lo) in enumerate(((hi_there, lo_there), (hi_back, lo_back))):
        for k in range(4):
            for u in range(16):
                w = fast[2 * way + k % 2] * slow[2 * way + k // 2, u : u + 1, :]
                top = w.astype(BF16)
                hi[k, 16 * u : 16 * u + 16, :] = top
                lo[k, 16 * u : 16 * u + 16, :] = (w - top.astype(F32)).astype(BF16)


def plane_tables():
    out = [jax.ShapeDtypeStruct((4, 256, 256), BF16)] * 4
    return pl.pallas_call(
        tables_kernel, out_shape=out, name="plane_tables",
        compiler_params=pltpu.CompilerParams(vmem_limit_bytes=8 << 20),
    )(*[jnp.asarray(a) for a in factor_tables()])


def t16(f):
    o = [f[u] - f[u + 8] for u in range(8)]
    e = [f[u] + f[u + 8] for u in range(8)]
    ee = [e[u] + e[u + 4] for u in range(4)]
    eo = [e[u] - e[u + 4] for u in range(4)]
    c, s = {}, {}
    p0, p1 = ee[0] + ee[2], ee[1] + ee[3]
    c[0], c[8], c[4], s[4] = p0 + p1, p0 - p1, ee[0] - ee[2], ee[1] - ee[3]
    d, a = R2 * (eo[1] - eo[3]), R2 * (eo[1] + eo[3])
    c[2], c[6], s[2], s[6] = eo[0] + d, eo[0] - d, a + eo[2], a - eo[2]
    d1, d2, d3 = (o[u] - o[8 - u] for u in (1, 2, 3))
    s1, s2, s3 = (o[u] + o[8 - u] for u in (1, 2, 3))
    d2, s2 = R2 * d2, R2 * s2
    e1, e3 = o[0] + d2, o[0] - d2
    o1, o3 = C1 * d1 + C3 * d3, C3 * d1 - C1 * d3
    c[1], c[7], c[3], c[5] = e1 + o1, e1 - o1, e3 + o3, e3 - o3
    x1, x3 = o[4] + s2, o[4] - s2
    y1, y3 = C3 * s1 + C1 * s3, C1 * s1 - C3 * s3
    s[1], s[7], s[3], s[5] = y1 + x1, y1 - x1, y3 - x3, y3 + x3
    return c, s


def t16_back(c, s):
    e1, o1, e3, o3 = c[1] + c[7], c[1] - c[7], c[3] + c[5], c[3] - c[5]
    o0, d2 = e1 + e3, R2 * (e1 - e3)
    d1, d3 = C1 * o1 + C3 * o3, C3 * o1 - C1 * o3
    y1, x1, y3, x3 = s[1] + s[7], s[1] - s[7], s[3] + s[5], s[5] - s[3]
    o4, s2 = x1 + x3, R2 * (x1 - x3)
    s1, s3 = C3 * y1 + C1 * y3, C1 * y1 - C3 * y3
    o = [o0, d1 + s1, d2 + s2, d3 + s3, o4, s3 - d3, s2 - d2, s1 - d1]
    d, a = R2 * (c[2] - c[6]), R2 * (s[2] + s[6])
    eo = [c[2] + c[6], d + a, s[2] - s[6], a - d]
    p0, p1 = c[0] + c[8], c[0] - c[8]
    ee = [p0 + c[4], p1 + s[4], p0 - c[4], p1 - s[4]]
    e = [ee[u] + eo[u] for u in range(4)] + [ee[u] - eo[u] for u in range(4)]
    return [e[u] + o[u] for u in range(8)] + [e[u] - o[u] for u in range(8)]


def convolve_x(f, table):
    keys, _, _ = x_basis()
    row = {key: k for k, key in enumerate(keys)}
    place = {(x % 3, x % 16): x for x in range(NG)}
    part = {"A": [], "c": [], "s": []}
    for u in range(16):
        f0, f1, f2 = (f[place[t, u]] for t in range(3))
        a = f1 + f2
        part["A"].append(f0 + a)
        part["c"].append(f0 - 0.5 * a)
        part["s"].append(S3 * (f1 - f2))
    c, s = t16(part["A"])
    c = {b: v * table(row["A", "C", b]) for b, v in c.items()}
    s = {b: v * table(row["A", "S", b]) for b, v in s.items()}
    back_a = t16_back(c, s)
    cc, cs = t16(part["c"])
    sc, ss = t16(part["s"])
    for b in (0, 8):
        cc[b] = cc[b] * table(row["c", "C", b])
        sc[b] = sc[b] * table(row["s", "C", b])
    for b in range(1, 8):
        p = (cc[b] - ss[b]) * table(row["cos", 1, b])
        m = (cc[b] + ss[b]) * table(row["cos", -1, b])
        cc[b], ss[b] = p + m, m - p
        p = (sc[b] + cs[b]) * table(row["sin", 1, b])
        m = (sc[b] - cs[b]) * table(row["sin", -1, b])
        sc[b], cs[b] = p + m, p - m
    back_c, back_s = t16_back(cc, cs), t16_back(sc, ss)
    out = [None] * NG
    for u in range(16):
        a, c_, s_ = back_a[u], back_c[u], S3 * back_s[u]
        h = a - 0.5 * c_
        out[place[0, u]] = a + c_
        out[place[1, u]] = h + s_
        out[place[2, u]] = h - s_
    return out


def group(k, j):
    return slice(k * SLAB + j * 256, k * SLAB + j * 256 + 256)


def split(hi, lo, rows, span, value):
    top = value.astype(BF16)
    hi[rows, span] = top
    lo[rows, span] = (value - top.astype(F32)).astype(BF16)


def product(hi, lo, whi, wlo, k, j):
    span = group(k, j)
    a, b = hi[:, span], lo[:, span]
    w = (k // 2) * 2 + j // 2
    lhs = jnp.concatenate([a, b, a], axis=1)
    rhs = jnp.concatenate([whi[w], whi[w], wlo[w]], axis=0)
    return jnp.dot(lhs, rhs, preferred_element_type=F32)


def turn(value, lanes):
    return pltpu.roll(value, lanes % 128, 1) if lanes % 128 else value


def to_thirds(f, third, first):
    c, s = third[first : first + 3], third[first + 3 : first + 6]
    return (
        f[0] + f[1] + f[2],
        f[0] * c[0] + f[1] * c[1] + f[2] * c[2],
        f[0] * s[0] + f[1] * s[1] + f[2] * s[2],
    )


def third_rows(third, h, rows):
    lanes = slice(128 * h, 128 * h + 128)
    return [jnp.broadcast_to(third[k : k + 1, lanes], (rows, 128)) for k in range(12)]


def from_thirds(a, c, s, third, first):
    return [a + c * third[first + m] + s * third[first + 3 + m] for m in range(3)]


def spectrum_kernel(q_ref, own, two, one, low_a, low_b, core, kern, third, whi, wlo, right, left, field, hi, lo):
    q = q_ref[0]
    sources = (
        (own, 0, low_a, 0),
        (one, 0, core, 4),
        (two, 0, low_b, 0),
        (core, 0, core, 6),
    )
    sub = lax.broadcasted_iota(jnp.int32, (8, 128), 0)
    to_right = sub % 4
    to_left = jnp.where(sub < 4, q, 4 + q % 2)
    place = lax.broadcasted_iota(jnp.int32, (8, 128), 1) // 16 % 3
    for delta, (bands_ref, first, low_ref, low_first) in enumerate(sources):
        base = (q ^ delta) * QX

        def densities(i, carry):
            rows = pl.ds(pl.multiple_of(8 * base + 16 * i, 16), 16)
            for h in range(2):
                pairs = []
                for half in range(2):
                    x = base + 2 * i + half
                    f = [[None] * 3 for _ in range(3)]
                    for m in range(3):
                        v = []
                        for n in range(3):
                            at = pl.ds(pl.multiple_of((2 * i + half) * PLANE + (m * SLAB + h * 384 + n * 128), 128), 128)
                            low = low_ref[low_first : low_first + 2, at]
                            v.append(jnp.concatenate([bands_ref[first : first + 4, at], low, low], axis=0))
                        for j in range(3):
                            got = jnp.where(place == j, v[0], jnp.where(place == (j + 1) % 3, v[1], v[2]))
                            got = turn(got, -16 * j)
                            r = jnp.take_along_axis(got, to_right, axis=0)
                            l = jnp.take_along_axis(got, to_left, axis=0)
                            span = slice(m * SLAB + j * 256 + h * 128, m * SLAB + j * 256 + h * 128 + 128)
                            right[x, :, span] = r
                            left[x, :, span] = l
                            f[m][j] = r * l
                    pairs.append(f)
                thirds_h = third_rows(third, h, 8)
                spec = []
                for f in pairs:
                    f = [to_thirds([f[m][j] for m in range(3)], thirds_h, 0) for j in range(3)]
                    spec.append([to_thirds([f[n][k] for n in range(3)], thirds_h, 6) for k in range(3)])
                for k in range(3):
                    for j in range(3):
                        span = slice(k * SLAB + j * 256 + h * 128, k * SLAB + j * 256 + h * 128 + 128)
                        split(hi, lo, rows, span, jnp.concatenate([spec[0][k][j], spec[1][k][j]], axis=0))
            return carry

        lax.fori_loop(0, QX // 2, densities, 0)

    for k in (0, 1):
        if k == 0:
            rows_of = [[product(hi, lo, whi, wlo, 0, j)] for j in range(3)]
        else:
            both = [(product(hi, lo, whi, wlo, 1, j), product(hi, lo, whi, wlo, 2, j)) for j in range(3)]
            rows_of = [[c - s, c + s] for c, s in both]
        for n in range(len(rows_of[0])):
            a, c, s = (rows_of[j][n] for j in range(3))
            field[:, group(k + n, 0)] = a
            field[:, group(k + n, 1)] = c - s
            field[:, group(k + n, 2)] = c + s

    def along_x(i, carry):
        span = pl.ds(pl.multiple_of(128 * i, 128), 128)
        f = [field[8 * x : 8 * x + 8, span] for x in range(NG)]
        out = convolve_x(f, lambda k: kern[k : k + 1, span])
        for x in range(NG):
            field[8 * x : 8 * x + 8, span] = out[x]
        return carry

    lax.fori_loop(0, PLANE // 128, along_x, 0)


def terms_kernel(q_ref, right, left, field, third, whi, wlo, near0, near2, cross, low0, low2, hi, lo, back):
    q = q_ref[0]

    def unmix(i, carry):
        rows = pl.ds(pl.multiple_of(16 * i, 16), 16)
        mixed = [[field[rows, group(k, j)] for j in range(3)] for k in range(3)]
        mixed = [[a, u + v, v - u] for a, u, v in mixed]
        for j in range(3):
            a, u, v = (mixed[k][j] for k in range(3))
            for k, value in enumerate((a, u + v, v - u)):
                split(hi, lo, rows, group(k, j), value)
        return carry

    lax.fori_loop(0, NG // 2, unmix, 0)
    for k in range(3):
        for j in range(3):
            back[:, group(k, j)] = product(hi, lo, whi, wlo, k, j)

    sub = lax.broadcasted_iota(jnp.int32, (8, 128), 0)
    mine = (sub == q).astype(F32)
    place = lax.broadcasted_iota(jnp.int32, (8, 128), 1) // 16 % 3

    for delta in range(4):
        base = (q ^ delta) * QX

        def finish(i, carry):
            for half in range(X_STEP):
                x = base + X_STEP * i + half
                rows = pl.ds(pl.multiple_of(x * 8, 8), 8)
                for h in range(2):
                    thirds_h = third_rows(third, h, 8)

                    def spot(k, j):
                        return slice(k * SLAB + j * 256 + h * 128, k * SLAB + j * 256 + h * 128 + 128)

                    v = [from_thirds(*(back[rows, spot(k, j)] for j in range(3)), thirds_h, 6) for k in range(3)]
                    v = [from_thirds(*(v[k][j] for k in range(3)), thirds_h, 0) for j in range(3)]
                    for m in range(3):
                        parts = []
                        for j in range(3):
                            pr = v[j][m] * right[x, :, spot(m, j)]
                            pr = pr + swapped(pr, sub, 1)
                            pr = pr + swapped(pr, sub, 2)
                            po = swapped(v[j][m] * left[x, :, spot(m, j)], sub, 4) + mine * pr
                            parts.append(turn(jnp.where(sub < 4, po, pr), 16 * j))
                        for n in range(3):
                            out = jnp.where(place == n, parts[0], jnp.where(place == (n + 1) % 3, parts[1], parts[2]))
                            start = (X_STEP * i + half) * PLANE + (m * SLAB + h * 384 + n * 128)
                            at = pl.ds(pl.multiple_of(start, 128), 128)
                            if delta % 2:
                                cross[delta // 2 * 4 : delta // 2 * 4 + 4, at] = out[0:4, :]
                                cross[8 + delta // 2 : 9 + delta // 2, at] = out[4:5, :]
                            else:
                                (near0, near2)[delta // 2][:, at] = out[0:4, :]
                                (low0, low2)[delta // 2][:, at] = out[4:5, :]
            return carry

        lax.fori_loop(0, QX // X_STEP, finish, 0)


def swapped(value, sub, flip):
    return jnp.take_along_axis(value, sub ^ flip, axis=0)


X_STEP = 2
VMEM_SPEC = pl.BlockSpec(memory_space=pltpu.VMEM)
SMEM_SPEC = pl.BlockSpec(memory_space=pltpu.SMEM)
SPLIT = [pltpu.VMEM((NG * 8, PLANE), BF16)] * 2


def spectrum(q, bands, tables):
    return pl.pallas_call(
        spectrum_kernel,
        out_shape=[jax.ShapeDtypeStruct((NG, 8, PLANE), F32)] * 2 + [jax.ShapeDtypeStruct((NG * 8, PLANE), F32)],
        in_specs=[SMEM_SPEC] + [VMEM_SPEC] * 10,
        out_specs=[VMEM_SPEC] * 3,
        scratch_shapes=SPLIT,
        name="spectrum",
        compiler_params=pltpu.CompilerParams(vmem_limit_bytes=24 << 20),
    )(q.reshape(1), *bands, jnp.asarray(kernel_values()), jnp.asarray(thirds()), *tables)


def terms(q, right, left, field, tables):
    return pl.pallas_call(
        terms_kernel,
        out_shape=[jax.ShapeDtypeStruct(shape, F32) for shape in [(4, QCELL)] * 2 + [(10, QCELL)] + [(1, QCELL)] * 2],
        in_specs=[SMEM_SPEC] + [VMEM_SPEC] * 6,
        out_specs=[VMEM_SPEC] * 5,
        scratch_shapes=SPLIT + [pltpu.VMEM((NG * 8, PLANE), F32)],
        name="terms",
        compiler_params=pltpu.CompilerParams(vmem_limit_bytes=28 << 20),
    )(q.reshape(1), right, left, field, jnp.asarray(thirds()), *tables)


BOTH = ("band", "grid")
CHUNK = QCELL // 4


def small_call(body, outs, scratch=(), limit=8):
    vmem = pl.BlockSpec(memory_space=pltpu.VMEM)

    def call(where, *arrays):
        return pl.pallas_call(
            body,
            out_shape=[jax.ShapeDtypeStruct(shape, F32) for shape in outs],
            in_specs=[pl.BlockSpec(memory_space=pltpu.SMEM)] + [vmem] * len(arrays),
            out_specs=[vmem] * len(outs),
            scratch_shapes=list(scratch),
            compiler_params=pltpu.CompilerParams(vmem_limit_bytes=limit << 20),
        )(where, *arrays)

    return call


def chunk_of(where, k):
    return pl.ds(pl.multiple_of((where[2] ^ k) * CHUNK, 128), CHUNK)


def rows_kernel(where, orbitals, sel_a, sel_b):
    lower = where[0] < 2
    a, b = orbitals[0:2, :], orbitals[2:4, :]
    sel_a[...] = jnp.where(lower, a, b)
    sel_b[...] = jnp.where(lower, b, a)


def chunks_kernel(where, orbitals, *chunks):
    for k in range(4):
        chunks[k][...] = orbitals[:, chunk_of(where, k)]


def stack_kernel(where, two, low_a, low_b, out):
    out[0:4, :] = two[...]
    out[4:6, :] = low_a[...]
    out[6:8, :] = low_b[...]


def merge_kernel(where, near0, near2, low0, low2, across, near, far, owed_a, owed_b):
    first = where[0] % 2 == 0
    near[...] = near0[...] + across[0:4, :]
    far[...] = near2[...] + across[4:8, :]
    for out, low, row in ((owed_a, low0, 8), (owed_b, low2, 9)):
        a, b = low[...], across[row : row + 1, :]
        out[0:1, :] = jnp.where(first, a, b)
        out[1:2, :] = jnp.where(first, b, a)


def total_of(where, near, far, owed_a, owed_b, span):
    lower = where[0] < 2
    a, b = owed_a[:, span], owed_b[:, span]
    owed = jnp.concatenate([jnp.where(lower, a, b), jnp.where(lower, b, a)], axis=0)
    return -(near[:, span] + far[:, span] + owed)


def finalize_kernel(where, near, far, owed_a, owed_b, *chunks):
    for k in (1, 2, 3, 0):
        chunks[k][...] = total_of(where, near, far, owed_a, owed_b, chunk_of(where, k))


def vectors_kernel(where, near, far, owed_a, owed_b, vectors):
    for c in range(4):
        span = pl.ds(c * CHUNK, CHUNK)
        vectors[:, span] = total_of(where, near, far, owed_a, owed_b, span)


def pair_kernel(where, f0, f1, f2, f3, other, out):
    first = where[3] == 0
    for k, f in enumerate((f0, f1, f2, f3)):
        a, b = f[...], other[4 * k : 4 * k + 4, :]
        out[8 * k : 8 * k + 4, :] = jnp.where(first, a, b)
        out[8 * k + 4 : 8 * k + 8, :] = jnp.where(first, b, a)


def margin_kernel(where, p0, p1, p2, p3, v0, v1, v2, v3, pieces, block):
    z, y = where[1], where[2]

    def halves(a):
        top = a.astype(BF16)
        return top, (a - top.astype(F32)).astype(BF16)

    vt, vl = halves(jnp.concatenate([v0[...], v1[...], v2[...], v3[...]], axis=0))
    dims = (((1,), (1,)), ((), ()))
    parts = jnp.concatenate([p0[...], p1[...], p2[...], p3[...]], axis=0)
    ft, fl = halves(parts)
    got = (
        lax.dot_general(ft, vt, dims, preferred_element_type=F32)
        + lax.dot_general(fl, vt, dims, preferred_element_type=F32)
        + lax.dot_general(ft, vl, dims, preferred_element_type=F32)
    )
    for dz in range(4):
        for dy in range(4):
            row = 32 * dz + 8 * dy
            block[(z + 4 - dz) % 4 * 4 + (y ^ dy), :, :] = got[row : row + 8, :]
    out = block[...].reshape(128, 16).T * (1.0 / NCELL)
    turned = [out] + [pltpu.roll(out, 32 * r, 1) for r in (1, 2, 3)]
    third_of = lax.broadcasted_iota(jnp.int32, (16, 128), 1) // 32
    keep = third_of == lax.broadcasted_iota(jnp.int32, (16, 128), 0) % 4
    for q_to in range(4):
        picked = turned[(3 - q_to) % 4]
        for j in range(3):
            picked = jnp.where(third_of == j, turned[(j - q_to) % 4], picked)
        picked = jnp.where(keep, picked, 0.0)
        for dy in range(4):
            row = jnp.sum(picked[4 * dy : 4 * dy + 4, :], axis=0, keepdims=True)
            pieces[pl.ds((y ^ dy) * 4 + q_to, 1), :] = row


def move(value, target):
    nb, nq = lax.axis_size("band"), lax.axis_size("grid")
    pairs = []
    for b in range(nb):
        for q in range(nq):
            z, y, h, q_to = target(b // 8, b // 2 % 4, b % 2, q)
            pairs.append((b * nq + q, ((z % 4) * 8 + (y % 4) * 2 + h) * nq + q_to))
    return lax.ppermute(value, BOTH, pairs)


def along_y(value, flip):
    return move(value, lambda z, y, h, q: (z, y ^ flip, h, q))


def along_z(value, k):
    return move(value, lambda z, y, h, q: (z + k, y, h, q))


def within(value, flip):
    return move(value, lambda z, y, h, q: (z, y, h, q ^ flip))


def around(value, blocks, flip):
    def target(z, y, h, q):
        b = (z * 8 + y * 2 + h + blocks) % 32
        return b // 8, b // 2 % 4, b % 2, q ^ flip

    return move(value, target)


def step(orbitals):
    b = lax.axis_index("band").astype(jnp.int32)
    q = lax.axis_index("grid").astype(jnp.int32)
    where = jnp.stack([q, b // 8, b // 2 % 4, b % 2])
    rows = small_call(rows_kernel, [(2, QCELL)] * 2)
    sel_a, sel_b = rows(where, orbitals)
    low_a = around(sel_a, 1, 0)
    low_b = around(sel_b, 1, 2)
    two = within(orbitals, 2)
    one = within(orbitals, 1)
    pc = small_call(chunks_kernel, [(4, CHUNK)] * 4)(where, orbitals)
    pieces = [pc[0]] + [along_y(pc[k], k) for k in (1, 2, 3)]
    tables = plane_tables()
    together = jnp.concatenate(pieces, axis=0)
    (stacked,) = small_call(stack_kernel, [(8, QCELL)])(where, two, low_a, low_b)
    core = within(stacked, 1)
    other = move(together, lambda z, y, h, q: (z, y, 1 - h, q))
    right, left, field = spectrum(q, (orbitals, two, one, low_a, low_b, core), tables[:2])
    (p0,) = small_call(pair_kernel, [(32, CHUNK)])(where, *pieces, other)
    p1 = along_z(p0, 1)
    p3 = along_z(p0, 3)
    near0, near2, cross, low0, low2 = terms(q, right, left, field, tables[2:])
    across = within(cross, 1)
    merge = small_call(merge_kernel, [(4, QCELL)] * 2 + [(2, QCELL)] * 2)
    near, both, owe_a, owe_b = merge(where, near0, near2, low0, low2, across)
    far = within(both, 2)
    owed_a = around(owe_a, -1, 0)
    owed_b = around(owe_b, -1, 2)
    p2 = along_z(p1, 1)
    finalize = small_call(finalize_kernel, [(4, CHUNK)] * 4)
    vc = finalize(where, near, far, owed_a, owed_b)
    (vectors,) = small_call(vectors_kernel, [(4, QCELL)])(where, near, far, owed_a, owed_b)
    given = [vc[0]] + [along_y(vc[k], k) for k in (1, 2, 3)]
    margin_part = small_call(margin_kernel, [(16, 128)], [pltpu.VMEM((16, 8, 16), F32)], 20)
    (sums,) = margin_part(where, p0, p1, p2, p3, *given)
    groups = [[(z * 8 + y * 2 + h) * 4 + p for y in range(4) for p in range(4)] for z in range(4) for h in range(2)]
    sums = lax.all_to_all(sums, BOTH, 0, 0, tiled=True, axis_index_groups=groups)
    margin = jnp.sum(sums, axis=0).reshape(4, 32).T
    return vectors, margin


def solution(mesh):
    return jax.shard_map(
        step,
        mesh=mesh,
        in_specs=(P("band", "grid"),),
        out_specs=(P("band", "grid"), P("grid", "band")),
        check_vma=False,
    )
```

```python
import math

import jax
import jax.numpy as jnp
import numpy as np
from jax import lax
from jax.experimental import pallas as pl
from jax.experimental.pallas import tpu as pltpu
from jax.sharding import PartitionSpec as P

NG = 48
NCELL = 110592
PLANE = NG * NG
SLAB = 768
QX = 12
QCELL = QX * PLANE
F32 = jnp.float32
BF16 = jnp.bfloat16
R2 = math.sqrt(0.5)
C1 = math.cos(math.pi / 8)
C3 = math.cos(3 * math.pi / 8)
S3 = math.sqrt(3.0) / 2

ORDER = [("C", b) for b in range(9)] + [("S", b) for b in range(1, 8)]
SWAPPED = [("C", 0)] + [("S", b) for b in range(1, 8)] + [("C", 8)] + [("C", b) for b in range(1, 8)]


def sixteen(order):
    u = np.arange(16)
    cols = []
    for kind, b in order:
        col = np.cos(2 * np.pi * b * u / 16) if kind == "C" else np.sin(2 * np.pi * b * u / 16)
        cols.append(col / np.linalg.norm(col))
    return np.stack(cols, 1)


def folded(g):
    return (g + 24) % 48 - 24


def x_basis():
    keys, freqs, norms = [], [], []
    for b in range(9):
        keys.append(("A", "C", b)); freqs.append(3 * b); norms.append(48 if b in (0, 8) else 24)
    for b in range(1, 8):
        keys.append(("A", "S", b)); freqs.append(3 * b); norms.append(24)
    for b in (0, 8):
        for t in "cs":
            keys.append((t, "C", b)); freqs.append(16 + 3 * b); norms.append(24)
    for b in range(1, 8):
        for sign in (1, -1):
            for kind in ("cos", "sin"):
                keys.append((kind, sign, b)); freqs.append(16 + 3 * sign * b); norms.append(24)
    return keys, np.array(freqs), np.array(norms)


def lane_freqs(group):
    out = []
    for kind, b in ORDER:
        if group == "A":
            out.append(3 * b)
        elif b in (0, 8):
            out.append(16 + 3 * b)
        else:
            out.append(16 + 3 * b if (group == "u") == (kind == "C") else 16 - 3 * b)
    return np.array(out)


def kernel_values():
    _, gx, nx = x_basis()
    g = np.stack([lane_freqs(group) for group in "Auv"])
    gy, gz = g[:, None, :, None], g[None, :, None, :]
    q = folded(gx)[:, None, None, None, None] ** 2 + (folded(gy) ** 2 + folded(gz) ** 2)[None]
    q = q.astype(np.float64)
    kern = np.where(q > 0, 40.0 * (1.0 - np.exp(-q / 16.0)) / np.where(q > 0, q, 1.0), 0.0)
    return (kern / (9.0 * nx[:, None, None, None, None])).reshape(NG, PLANE).astype(np.float32)


PLACES = np.array([0, 3, 6, 1, 4, 7, 2, 5])
LANE_Y = np.repeat(np.concatenate([PLACES, 8 + PLACES]), 16)
LANE_Z = np.tile(np.arange(16), 16)


def thirds():
    rows = []
    for lane in (LANE_Y, LANE_Z):
        rows += [np.cos(2 * np.pi * (m + lane) / 3) for m in range(3)]
        rows += [np.sin(2 * np.pi * (m + lane) / 3) for m in range(3)]
    return np.concatenate([np.stack(rows), np.zeros((4, 256))]).astype(np.float32)


def factor_tables():
    bases = sixteen(ORDER), sixteen(SWAPPED)
    slow = [np.repeat(t[LANE_Y[::16]], 16, 1) for t in bases] + [t.T[:, LANE_Y] for t in bases]
    fast = [np.tile(t, (1, 16)) for t in bases] + [np.tile(t.T, (1, 16)) for t in bases]
    return np.stack(slow).astype(np.float32), np.stack(fast).astype(np.float32)


def tables_kernel(slow, fast, hi_there, lo_there, hi_back, lo_back):
    for way, (hi, lo) in enumerate(((hi_there, lo_there), (hi_back, lo_back))):
        for k in range(4):
            for u in range(16):
                w = fast[2 * way + k % 2] * slow[2 * way + k // 2, u : u + 1, :]
                top = w.astype(BF16)
                hi[k, 16 * u : 16 * u + 16, :] = top
                lo[k, 16 * u : 16 * u + 16, :] = (w - top.astype(F32)).astype(BF16)


def plane_tables():
    out = [jax.ShapeDtypeStruct((4, 256, 256), BF16)] * 4
    return pl.pallas_call(
        tables_kernel, out_shape=out, name="plane_tables",
        compiler_params=pltpu.CompilerParams(vmem_limit_bytes=8 << 20),
    )(*[jnp.asarray(a) for a in factor_tables()])


def t16(f):
    o = [f[u] - f[u + 8] for u in range(8)]
    e = [f[u] + f[u + 8] for u in range(8)]
    ee = [e[u] + e[u + 4] for u in range(4)]
    eo = [e[u] - e[u + 4] for u in range(4)]
    c, s = {}, {}
    p0, p1 = ee[0] + ee[2], ee[1] + ee[3]
    c[0], c[8], c[4], s[4] = p0 + p1, p0 - p1, ee[0] - ee[2], ee[1] - ee[3]
    d, a = R2 * (eo[1] - eo[3]), R2 * (eo[1] + eo[3])
    c[2], c[6], s[2], s[6] = eo[0] + d, eo[0] - d, a + eo[2], a - eo[2]
    d1, d2, d3 = (o[u] - o[8 - u] for u in (1, 2, 3))
    s1, s2, s3 = (o[u] + o[8 - u] for u in (1, 2, 3))
    d2, s2 = R2 * d2, R2 * s2
    e1, e3 = o[0] + d2, o[0] - d2
    o1, o3 = C1 * d1 + C3 * d3, C3 * d1 - C1 * d3
    c[1], c[7], c[3], c[5] = e1 + o1, e1 - o1, e3 + o3, e3 - o3
    x1, x3 = o[4] + s2, o[4] - s2
    y1, y3 = C3 * s1 + C1 * s3, C1 * s1 - C3 * s3
    s[1], s[7], s[3], s[5] = y1 + x1, y1 - x1, y3 - x3, y3 + x3
    return c, s


def t16_back(c, s):
    e1, o1, e3, o3 = c[1] + c[7], c[1] - c[7], c[3] + c[5], c[3] - c[5]
    o0, d2 = e1 + e3, R2 * (e1 - e3)
    d1, d3 = C1 * o1 + C3 * o3, C3 * o1 - C1 * o3
    y1, x1, y3, x3 = s[1] + s[7], s[1] - s[7], s[3] + s[5], s[5] - s[3]
    o4, s2 = x1 + x3, R2 * (x1 - x3)
    s1, s3 = C3 * y1 + C1 * y3, C1 * y1 - C3 * y3
    o = [o0, d1 + s1, d2 + s2, d3 + s3, o4, s3 - d3, s2 - d2, s1 - d1]
    d, a = R2 * (c[2] - c[6]), R2 * (s[2] + s[6])
    eo = [c[2] + c[6], d + a, s[2] - s[6], a - d]
    p0, p1 = c[0] + c[8], c[0] - c[8]
    ee = [p0 + c[4], p1 + s[4], p0 - c[4], p1 - s[4]]
    e = [ee[u] + eo[u] for u in range(4)] + [ee[u] - eo[u] for u in range(4)]
    return [e[u] + o[u] for u in range(8)] + [e[u] - o[u] for u in range(8)]


def convolve_x(f, table):
    keys, _, _ = x_basis()
    row = {key: k for k, key in enumerate(keys)}
    place = {(x % 3, x % 16): x for x in range(NG)}
    part = {"A": [], "c": [], "s": []}
    for u in range(16):
        f0, f1, f2 = (f[place[t, u]] for t in range(3))
        a = f1 + f2
        part["A"].append(f0 + a)
        part["c"].append(f0 - 0.5 * a)
        part["s"].append(S3 * (f1 - f2))
    c, s = t16(part["A"])
    c = {b: v * table(row["A", "C", b]) for b, v in c.items()}
    s = {b: v * table(row["A", "S", b]) for b, v in s.items()}
    back_a = t16_back(c, s)
    cc, cs = t16(part["c"])
    sc, ss = t16(part["s"])
    for b in (0, 8):
        cc[b] = cc[b] * table(row["c", "C", b])
        sc[b] = sc[b] * table(row["s", "C", b])
    for b in range(1, 8):
        p = (cc[b] - ss[b]) * table(row["cos", 1, b])
        m = (cc[b] + ss[b]) * table(row["cos", -1, b])
        cc[b], ss[b] = p + m, m - p
        p = (sc[b] + cs[b]) * table(row["sin", 1, b])
        m = (sc[b] - cs[b]) * table(row["sin", -1, b])
        sc[b], cs[b] = p + m, p - m
    back_c, back_s = t16_back(cc, cs), t16_back(sc, ss)
    out = [None] * NG
    for u in range(16):
        a, c_, s_ = back_a[u], back_c[u], S3 * back_s[u]
        h = a - 0.5 * c_
        out[place[0, u]] = a + c_
        out[place[1, u]] = h + s_
        out[place[2, u]] = h - s_
    return out


def group(k, j):
    return slice(k * SLAB + j * 256, k * SLAB + j * 256 + 256)


def split(hi, lo, rows, span, value):
    top = value.astype(BF16)
    hi[rows, span] = top
    lo[rows, span] = (value - top.astype(F32)).astype(BF16)


def product(hi, lo, whi, wlo, k, j):
    span = group(k, j)
    a, b = hi[:, span], lo[:, span]
    w = (k // 2) * 2 + j // 2
    lhs = jnp.concatenate([a, b, a], axis=1)
    rhs = jnp.concatenate([whi[w], whi[w], wlo[w]], axis=0)
    return jnp.dot(lhs, rhs, preferred_element_type=F32)


def turn(value, lanes):
    return pltpu.roll(value, lanes % 128, 1) if lanes % 128 else value


def to_thirds(f, third, first):
    c, s = third[first : first + 3], third[first + 3 : first + 6]
    return (
        f[0] + f[1] + f[2],
        f[0] * c[0] + f[1] * c[1] + f[2] * c[2],
        f[0] * s[0] + f[1] * s[1] + f[2] * s[2],
    )


def third_rows(third, h, rows):
    lanes = slice(128 * h, 128 * h + 128)
    return [jnp.broadcast_to(third[k : k + 1, lanes], (rows, 128)) for k in range(12)]


def from_thirds(a, c, s, third, first):
    return [a + c * third[first + m] + s * third[first + 3 + m] for m in range(3)]


def spectrum_kernel(q_ref, own, two, one, low_a, low_b, core, kern, third, whi, wlo, right, left, field, hi, lo):
    q = q_ref[0]
    sources = (
        (own, 0, low_a, 0),
        (one, 0, core, 4),
        (two, 0, low_b, 0),
        (core, 0, core, 6),
    )
    sub = lax.broadcasted_iota(jnp.int32, (8, 128), 0)
    to_right = sub % 4
    to_left = jnp.where(sub < 4, q, 4 + q % 2)
    place = lax.broadcasted_iota(jnp.int32, (8, 128), 1) // 16 % 3
    for delta, (bands_ref, first, low_ref, low_first) in enumerate(sources):
        base = (q ^ delta) * QX

        def densities(i, carry):
            rows = pl.ds(pl.multiple_of(8 * base + 16 * i, 16), 16)
            for h in range(2):
                pairs = []
                for half in range(2):
                    x = base + 2 * i + half
                    f = [[None] * 3 for _ in range(3)]
                    for m in range(3):
                        v = []
                        for n in range(3):
                            at = pl.ds(pl.multiple_of((2 * i + half) * PLANE + (m * SLAB + h * 384 + n * 128), 128), 128)
                            low = low_ref[low_first : low_first + 2, at]
                            v.append(jnp.concatenate([bands_ref[first : first + 4, at], low, low], axis=0))
                        for j in range(3):
                            got = jnp.where(place == j, v[0], jnp.where(place == (j + 1) % 3, v[1], v[2]))
                            got = turn(got, -16 * j)
                            r = jnp.take_along_axis(got, to_right, axis=0)
                            l = jnp.take_along_axis(got, to_left, axis=0)
                            span = slice(m * SLAB + j * 256 + h * 128, m * SLAB + j * 256 + h * 128 + 128)
                            right[x, :, span] = r
                            left[x, :, span] = l
                            f[m][j] = r * l
                    pairs.append(f)
                thirds_h = third_rows(third, h, 8)
                spec = []
                for f in pairs:
                    f = [to_thirds([f[m][j] for m in range(3)], thirds_h, 0) for j in range(3)]
                    spec.append([to_thirds([f[n][k] for n in range(3)], thirds_h, 6) for k in range(3)])
                for k in range(3):
                    for j in range(3):
                        span = slice(k * SLAB + j * 256 + h * 128, k * SLAB + j * 256 + h * 128 + 128)
                        split(hi, lo, rows, span, jnp.concatenate([spec[0][k][j], spec[1][k][j]], axis=0))
            return carry

        lax.fori_loop(0, QX // 2, densities, 0)

    for k in (0, 1):
        if k == 0:
            rows_of = [[product(hi, lo, whi, wlo, 0, j)] for j in range(3)]
        else:
            both = [(product(hi, lo, whi, wlo, 1, j), product(hi, lo, whi, wlo, 2, j)) for j in range(3)]
            rows_of = [[c - s, c + s] for c, s in both]
        for n in range(len(rows_of[0])):
            a, c, s = (rows_of[j][n] for j in range(3))
            field[:, group(k + n, 0)] = a
            field[:, group(k + n, 1)] = c - s
            field[:, group(k + n, 2)] = c + s

    def along_x(i, carry):
        span = pl.ds(pl.multiple_of(128 * i, 128), 128)
        f = [field[8 * x : 8 * x + 8, span] for x in range(NG)]
        out = convolve_x(f, lambda k: kern[k : k + 1, span])
        for x in range(NG):
            field[8 * x : 8 * x + 8, span] = out[x]
        return carry

    lax.fori_loop(0, PLANE // 128, along_x, 0)


def terms_kernel(q_ref, right, left, field, third, whi, wlo, near0, near2, cross, low0, low2, hi, lo, back):
    q = q_ref[0]

    def unmix(i, carry):
        rows = pl.ds(pl.multiple_of(16 * i, 16), 16)
        mixed = [[field[rows, group(k, j)] for j in range(3)] for k in range(3)]
        mixed = [[a, u + v, v - u] for a, u, v in mixed]
        for j in range(3):
            a, u, v = (mixed[k][j] for k in range(3))
            for k, value in enumerate((a, u + v, v - u)):
                split(hi, lo, rows, group(k, j), value)
        return carry

    lax.fori_loop(0, NG // 2, unmix, 0)
    for k in range(3):
        for j in range(3):
            back[:, group(k, j)] = product(hi, lo, whi, wlo, k, j)

    sub = lax.broadcasted_iota(jnp.int32, (8, 128), 0)
    mine = (sub == q).astype(F32)
    place = lax.broadcasted_iota(jnp.int32, (8, 128), 1) // 16 % 3

    for delta in range(4):
        base = (q ^ delta) * QX

        def finish(i, carry):
            for half in range(X_STEP):
                x = base + X_STEP * i + half
                rows = pl.ds(pl.multiple_of(x * 8, 8), 8)
                for h in range(2):
                    thirds_h = third_rows(third, h, 8)

                    def spot(k, j):
                        return slice(k * SLAB + j * 256 + h * 128, k * SLAB + j * 256 + h * 128 + 128)

                    v = [from_thirds(*(back[rows, spot(k, j)] for j in range(3)), thirds_h, 6) for k in range(3)]
                    v = [from_thirds(*(v[k][j] for k in range(3)), thirds_h, 0) for j in range(3)]
                    for m in range(3):
                        parts = []
                        for j in range(3):
                            pr = v[j][m] * right[x, :, spot(m, j)]
                            pr = pr + swapped(pr, sub, 1)
                            pr = pr + swapped(pr, sub, 2)
                            po = swapped(v[j][m] * left[x, :, spot(m, j)], sub, 4) + mine * pr
                            parts.append(turn(jnp.where(sub < 4, po, pr), 16 * j))
                        for n in range(3):
                            out = jnp.where(place == n, parts[0], jnp.where(place == (n + 1) % 3, parts[1], parts[2]))
                            start = (X_STEP * i + half) * PLANE + (m * SLAB + h * 384 + n * 128)
                            at = pl.ds(pl.multiple_of(start, 128), 128)
                            if delta % 2:
                                cross[delta // 2 * 4 : delta // 2 * 4 + 4, at] = out[0:4, :]
                                cross[8 + delta // 2 : 9 + delta // 2, at] = out[4:5, :]
                            else:
                                (near0, near2)[delta // 2][:, at] = out[0:4, :]
                                (low0, low2)[delta // 2][:, at] = out[4:5, :]
            return carry

        lax.fori_loop(0, QX // X_STEP, finish, 0)


def swapped(value, sub, flip):
    return jnp.take_along_axis(value, sub ^ flip, axis=0)


X_STEP = 2
VMEM_SPEC = pl.BlockSpec(memory_space=pltpu.VMEM)
SMEM_SPEC = pl.BlockSpec(memory_space=pltpu.SMEM)
SPLIT = [pltpu.VMEM((NG * 8, PLANE), BF16)] * 2


def spectrum(q, bands, tables):
    return pl.pallas_call(
        spectrum_kernel,
        out_shape=[jax.ShapeDtypeStruct((NG, 8, PLANE), F32)] * 2 + [jax.ShapeDtypeStruct((NG * 8, PLANE), F32)],
        in_specs=[SMEM_SPEC] + [VMEM_SPEC] * 10,
        out_specs=[VMEM_SPEC] * 3,
        scratch_shapes=SPLIT,
        name="spectrum",
        compiler_params=pltpu.CompilerParams(vmem_limit_bytes=24 << 20),
    )(q.reshape(1), *bands, jnp.asarray(kernel_values()), jnp.asarray(thirds()), *tables)


def terms(q, right, left, field, tables):
    return pl.pallas_call(
        terms_kernel,
        out_shape=[jax.ShapeDtypeStruct(shape, F32) for shape in [(4, QCELL)] * 2 + [(10, QCELL)] + [(1, QCELL)] * 2],
        in_specs=[SMEM_SPEC] + [VMEM_SPEC] * 6,
        out_specs=[VMEM_SPEC] * 5,
        scratch_shapes=SPLIT + [pltpu.VMEM((NG * 8, PLANE), F32)],
        name="terms",
        compiler_params=pltpu.CompilerParams(vmem_limit_bytes=28 << 20),
    )(q.reshape(1), right, left, field, jnp.asarray(thirds()), *tables)


BOTH = ("band", "grid")
CHUNK = QCELL // 4


def small_call(body, outs, scratch=(), limit=8):
    vmem = pl.BlockSpec(memory_space=pltpu.VMEM)

    def call(where, *arrays):
        return pl.pallas_call(
            body,
            out_shape=[jax.ShapeDtypeStruct(shape, F32) for shape in outs],
            in_specs=[pl.BlockSpec(memory_space=pltpu.SMEM)] + [vmem] * len(arrays),
            out_specs=[vmem] * len(outs),
            scratch_shapes=list(scratch),
            compiler_params=pltpu.CompilerParams(vmem_limit_bytes=limit << 20),
        )(where, *arrays)

    return call


def chunk_of(where, k):
    return pl.ds(pl.multiple_of((where[2] ^ k) * CHUNK, 128), CHUNK)


def rows_kernel(where, orbitals, sel_a, sel_b):
    lower = where[0] < 2
    a, b = orbitals[0:2, :], orbitals[2:4, :]
    sel_a[...] = jnp.where(lower, a, b)
    sel_b[...] = jnp.where(lower, b, a)


def chunks_kernel(where, orbitals, *chunks):
    for k in range(4):
        chunks[k][...] = orbitals[:, chunk_of(where, k)]


def stack_kernel(where, two, low_a, low_b, out):
    out[0:4, :] = two[...]
    out[4:6, :] = low_a[...]
    out[6:8, :] = low_b[...]


def merge_kernel(where, near0, near2, low0, low2, across, near, far, owed_a, owed_b):
    first = where[0] % 2 == 0
    near[...] = near0[...] + across[0:4, :]
    far[...] = near2[...] + across[4:8, :]
    for out, low, row in ((owed_a, low0, 8), (owed_b, low2, 9)):
        a, b = low[...], across[row : row + 1, :]
        out[0:1, :] = jnp.where(first, a, b)
        out[1:2, :] = jnp.where(first, b, a)


def total_of(where, near, far, owed_a, owed_b, span):
    lower = where[0] < 2
    a, b = owed_a[:, span], owed_b[:, span]
    owed = jnp.concatenate([jnp.where(lower, a, b), jnp.where(lower, b, a)], axis=0)
    return -(near[:, span] + far[:, span] + owed)


def finalize_kernel(where, near, far, owed_a, owed_b, *chunks):
    for k in (1, 2, 3, 0):
        chunks[k][...] = total_of(where, near, far, owed_a, owed_b, chunk_of(where, k))


def vectors_kernel(where, near, far, owed_a, owed_b, vectors):
    for c in range(4):
        span = pl.ds(c * CHUNK, CHUNK)
        vectors[:, span] = total_of(where, near, far, owed_a, owed_b, span)


def margin_kernel(where, own0, oth0, own1, oth1, own2, oth2, own3, oth3, v0, v1, v2, v3, pieces, block):
    z, y, h = where[1], where[2], where[3]

    def halves(a):
        top = a.astype(BF16)
        return top, (a - top.astype(F32)).astype(BF16)

    vt, vl = halves(jnp.concatenate([v0[...], v1[...], v2[...], v3[...]], axis=0))
    dims = (((1,), (1,)), ((), ()))
    parts = jnp.concatenate([r[...] for r in (own0, oth0, own1, oth1, own2, oth2, own3, oth3)], axis=0)
    ft, fl = halves(parts)
    got = (
        lax.dot_general(ft, vt, dims, preferred_element_type=F32)
        + lax.dot_general(fl, vt, dims, preferred_element_type=F32)
        + lax.dot_general(ft, vl, dims, preferred_element_type=F32)
    )
    for dz in range(4):
        for dy in range(4):
            row = 32 * dz + 4 * dy
            pair = got[row : row + 4, :], got[row + 16 : row + 20, :]
            at = (z + 4 - dz) % 4 * 4 + (y ^ dy)
            block[at, 0:4, :] = jnp.where(h == 0, pair[0], pair[1])
            block[at, 4:8, :] = jnp.where(h == 0, pair[1], pair[0])
    out = block[...].reshape(128, 16).T * (1.0 / NCELL)
    turned = [out] + [pltpu.roll(out, 32 * r, 1) for r in (1, 2, 3)]
    third_of = lax.broadcasted_iota(jnp.int32, (16, 128), 1) // 32
    keep = third_of == lax.broadcasted_iota(jnp.int32, (16, 128), 0) % 4
    for q_to in range(4):
        picked = turned[(3 - q_to) % 4]
        for j in range(3):
            picked = jnp.where(third_of == j, turned[(j - q_to) % 4], picked)
        picked = jnp.where(keep, picked, 0.0)
        for dy in range(4):
            row = jnp.sum(picked[4 * dy : 4 * dy + 4, :], axis=0, keepdims=True)
            pieces[pl.ds((y ^ dy) * 4 + q_to, 1), :] = row


def move(value, target):
    nb, nq = lax.axis_size("band"), lax.axis_size("grid")
    pairs = []
    for b in range(nb):
        for q in range(nq):
            z, y, h, q_to = target(b // 8, b // 2 % 4, b % 2, q)
            pairs.append((b * nq + q, ((z % 4) * 8 + (y % 4) * 2 + h) * nq + q_to))
    return lax.ppermute(value, BOTH, pairs)


def along_y(value, flip):
    return move(value, lambda z, y, h, q: (z, y ^ flip, h, q))


def along_z(value, k):
    return move(value, lambda z, y, h, q: (z + k, y, h, q))


def within(value, flip):
    return move(value, lambda z, y, h, q: (z, y, h, q ^ flip))


def around(value, blocks, flip):
    def target(z, y, h, q):
        b = (z * 8 + y * 2 + h + blocks) % 32
        return b // 8, b // 2 % 4, b % 2, q ^ flip

    return move(value, target)


def step(orbitals):
    b = lax.axis_index("band").astype(jnp.int32)
    q = lax.axis_index("grid").astype(jnp.int32)
    where = jnp.stack([q, b // 8, b // 2 % 4, b % 2])
    rows = small_call(rows_kernel, [(2, QCELL)] * 2)
    sel_a, sel_b = rows(where, orbitals)
    low_a = around(sel_a, 1, 0)
    low_b = around(sel_b, 1, 2)
    two = within(orbitals, 2)
    one = within(orbitals, 1)
    pc = small_call(chunks_kernel, [(4, CHUNK)] * 4)(where, orbitals)
    pieces = [pc[0]] + [along_y(pc[k], k) for k in (1, 2, 3)]
    tables = plane_tables()
    together = jnp.concatenate(pieces, axis=0)
    (stacked,) = small_call(stack_kernel, [(8, QCELL)])(where, two, low_a, low_b)
    core = within(stacked, 1)
    other = move(together, lambda z, y, h, q: (z, y, 1 - h, q))
    own1 = along_z(together, 1)
    own3 = along_z(together, 3)
    right, left, field = spectrum(q, (orbitals, two, one, low_a, low_b, core), tables[:2])
    near0, near2, cross, low0, low2 = terms(q, right, left, field, tables[2:])
    across = within(cross, 1)
    other, _ = lax.optimization_barrier((other, near0))
    oth1 = along_z(other, 1)
    oth3 = along_z(other, 3)
    own2 = along_z(own1, 1)
    merge = small_call(merge_kernel, [(4, QCELL)] * 2 + [(2, QCELL)] * 2)
    near, both, owe_a, owe_b = merge(where, near0, near2, low0, low2, across)
    far = within(both, 2)
    owed_a = around(owe_a, -1, 0)
    owed_b = around(owe_b, -1, 2)
    oth2 = along_z(oth1, 1)
    finalize = small_call(finalize_kernel, [(4, CHUNK)] * 4)
    vc = finalize(where, near, far, owed_a, owed_b)
    (vectors,) = small_call(vectors_kernel, [(4, QCELL)])(where, near, far, owed_a, owed_b)
    given = [vc[0]] + [along_y(vc[k], k) for k in (1, 2, 3)]
    margin_part = small_call(margin_kernel, [(16, 128)], [pltpu.VMEM((16, 8, 16), F32)], 20)
    (sums,) = margin_part(where, together, other, own1, oth1, own2, oth2, own3, oth3, *given)
    groups = [[(z * 8 + y * 2 + h) * 4 + p for y in range(4) for p in range(4)] for z in range(4) for h in range(2)]
    sums = lax.all_to_all(sums, BOTH, 0, 0, tiled=True, axis_index_groups=groups)
    margin = jnp.sum(sums, axis=0).reshape(4, 32).T
    return vectors, margin


def solution(mesh):
    return jax.shard_map(
        step,
        mesh=mesh,
        in_specs=(P("band", "grid"),),
        out_specs=(P("band", "grid"), P("grid", "band")),
        check_vma=False,
    )
```

```python
import math

import jax
import jax.numpy as jnp
import numpy as np
from jax import lax
from jax.experimental import pallas as pl
from jax.experimental.pallas import tpu as pltpu
from jax.sharding import PartitionSpec as P

NG = 48
NCELL = 110592
PLANE = NG * NG
SLAB = 768
QX = 12
QCELL = QX * PLANE
F32 = jnp.float32
BF16 = jnp.bfloat16
R2 = math.sqrt(0.5)
C1 = math.cos(math.pi / 8)
C3 = math.cos(3 * math.pi / 8)
S3 = math.sqrt(3.0) / 2

ORDER = [("C", b) for b in range(9)] + [("S", b) for b in range(1, 8)]
SWAPPED = [("C", 0)] + [("S", b) for b in range(1, 8)] + [("C", 8)] + [("C", b) for b in range(1, 8)]


def sixteen(order):
    u = np.arange(16)
    cols = []
    for kind, b in order:
        col = np.cos(2 * np.pi * b * u / 16) if kind == "C" else np.sin(2 * np.pi * b * u / 16)
        cols.append(col / np.linalg.norm(col))
    return np.stack(cols, 1)


def folded(g):
    return (g + 24) % 48 - 24


def x_basis():
    keys, freqs, norms = [], [], []
    for b in range(9):
        keys.append(("A", "C", b)); freqs.append(3 * b); norms.append(48 if b in (0, 8) else 24)
    for b in range(1, 8):
        keys.append(("A", "S", b)); freqs.append(3 * b); norms.append(24)
    for b in (0, 8):
        for t in "cs":
            keys.append((t, "C", b)); freqs.append(16 + 3 * b); norms.append(24)
    for b in range(1, 8):
        for sign in (1, -1):
            for kind in ("cos", "sin"):
                keys.append((kind, sign, b)); freqs.append(16 + 3 * sign * b); norms.append(24)
    return keys, np.array(freqs), np.array(norms)


def lane_freqs(group):
    out = []
    for kind, b in ORDER:
        if group == "A":
            out.append(3 * b)
        elif b in (0, 8):
            out.append(16 + 3 * b)
        else:
            out.append(16 + 3 * b if (group == "u") == (kind == "C") else 16 - 3 * b)
    return np.array(out)


def kernel_values():
    _, gx, nx = x_basis()
    g = np.stack([lane_freqs(group) for group in "Auv"])
    gy, gz = g[:, None, :, None], g[None, :, None, :]
    q = folded(gx)[:, None, None, None, None] ** 2 + (folded(gy) ** 2 + folded(gz) ** 2)[None]
    q = q.astype(np.float64)
    kern = np.where(q > 0, 40.0 * (1.0 - np.exp(-q / 16.0)) / np.where(q > 0, q, 1.0), 0.0)
    return (kern / (9.0 * nx[:, None, None, None, None])).reshape(NG, PLANE).astype(np.float32)


PLACES = np.array([0, 3, 6, 1, 4, 7, 2, 5])
LANE_Y = np.repeat(np.concatenate([PLACES, 8 + PLACES]), 16)
LANE_Z = np.tile(np.arange(16), 16)


def thirds():
    rows = []
    for lane in (LANE_Y, LANE_Z):
        rows += [np.cos(2 * np.pi * (m + lane) / 3) for m in range(3)]
        rows += [np.sin(2 * np.pi * (m + lane) / 3) for m in range(3)]
    return np.concatenate([np.stack(rows), np.zeros((4, 256))]).astype(np.float32)


def factor_tables():
    bases = sixteen(ORDER), sixteen(SWAPPED)
    slow = [np.repeat(t[LANE_Y[::16]], 16, 1) for t in bases] + [t.T[:, LANE_Y] for t in bases]
    fast = [np.tile(t, (1, 16)) for t in bases] + [np.tile(t.T, (1, 16)) for t in bases]
    return np.stack(slow).astype(np.float32), np.stack(fast).astype(np.float32)


def tables_kernel(slow, fast, kern_in, third_in, hi_there, lo_there, hi_back, lo_back, kern, third):
    kern[...] = kern_in[...]
    third[...] = third_in[...]
    for way, (hi, lo) in enumerate(((hi_there, lo_there), (hi_back, lo_back))):
        for k in range(4):
            for u in range(16):
                w = fast[2 * way + k % 2] * slow[2 * way + k // 2, u : u + 1, :]
                top = w.astype(BF16)
                hi[k, 16 * u : 16 * u + 16, :] = top
                lo[k, 16 * u : 16 * u + 16, :] = (w - top.astype(F32)).astype(BF16)


def plane_tables():
    out = [jax.ShapeDtypeStruct((4, 256, 256), BF16)] * 4
    out += [jax.ShapeDtypeStruct((NG, PLANE), F32), jax.ShapeDtypeStruct((16, 256), F32)]
    return pl.pallas_call(
        tables_kernel, out_shape=out, name="plane_tables",
        compiler_params=pltpu.CompilerParams(vmem_limit_bytes=8 << 20),
    )(*[jnp.asarray(a) for a in (*factor_tables(), kernel_values(), thirds())])


def t16(f):
    o = [f[u] - f[u + 8] for u in range(8)]
    e = [f[u] + f[u + 8] for u in range(8)]
    ee = [e[u] + e[u + 4] for u in range(4)]
    eo = [e[u] - e[u + 4] for u in range(4)]
    c, s = {}, {}
    p0, p1 = ee[0] + ee[2], ee[1] + ee[3]
    c[0], c[8], c[4], s[4] = p0 + p1, p0 - p1, ee[0] - ee[2], ee[1] - ee[3]
    d, a = R2 * (eo[1] - eo[3]), R2 * (eo[1] + eo[3])
    c[2], c[6], s[2], s[6] = eo[0] + d, eo[0] - d, a + eo[2], a - eo[2]
    d1, d2, d3 = (o[u] - o[8 - u] for u in (1, 2, 3))
    s1, s2, s3 = (o[u] + o[8 - u] for u in (1, 2, 3))
    d2, s2 = R2 * d2, R2 * s2
    e1, e3 = o[0] + d2, o[0] - d2
    o1, o3 = C1 * d1 + C3 * d3, C3 * d1 - C1 * d3
    c[1], c[7], c[3], c[5] = e1 + o1, e1 - o1, e3 + o3, e3 - o3
    x1, x3 = o[4] + s2, o[4] - s2
    y1, y3 = C3 * s1 + C1 * s3, C1 * s1 - C3 * s3
    s[1], s[7], s[3], s[5] = y1 + x1, y1 - x1, y3 - x3, y3 + x3
    return c, s


def t16_back(c, s):
    e1, o1, e3, o3 = c[1] + c[7], c[1] - c[7], c[3] + c[5], c[3] - c[5]
    o0, d2 = e1 + e3, R2 * (e1 - e3)
    d1, d3 = C1 * o1 + C3 * o3, C3 * o1 - C1 * o3
    y1, x1, y3, x3 = s[1] + s[7], s[1] - s[7], s[3] + s[5], s[5] - s[3]
    o4, s2 = x1 + x3, R2 * (x1 - x3)
    s1, s3 = C3 * y1 + C1 * y3, C1 * y1 - C3 * y3
    o = [o0, d1 + s1, d2 + s2, d3 + s3, o4, s3 - d3, s2 - d2, s1 - d1]
    d, a = R2 * (c[2] - c[6]), R2 * (s[2] + s[6])
    eo = [c[2] + c[6], d + a, s[2] - s[6], a - d]
    p0, p1 = c[0] + c[8], c[0] - c[8]
    ee = [p0 + c[4], p1 + s[4], p0 - c[4], p1 - s[4]]
    e = [ee[u] + eo[u] for u in range(4)] + [ee[u] - eo[u] for u in range(4)]
    return [e[u] + o[u] for u in range(8)] + [e[u] - o[u] for u in range(8)]


def convolve_x(f, table):
    keys, _, _ = x_basis()
    row = {key: k for k, key in enumerate(keys)}
    place = {(x % 3, x % 16): x for x in range(NG)}
    part = {"A": [], "c": [], "s": []}
    for u in range(16):
        f0, f1, f2 = (f[place[t, u]] for t in range(3))
        a = f1 + f2
        part["A"].append(f0 + a)
        part["c"].append(f0 - 0.5 * a)
        part["s"].append(S3 * (f1 - f2))
    c, s = t16(part["A"])
    c = {b: v * table(row["A", "C", b]) for b, v in c.items()}
    s = {b: v * table(row["A", "S", b]) for b, v in s.items()}
    back_a = t16_back(c, s)
    cc, cs = t16(part["c"])
    sc, ss = t16(part["s"])
    for b in (0, 8):
        cc[b] = cc[b] * table(row["c", "C", b])
        sc[b] = sc[b] * table(row["s", "C", b])
    for b in range(1, 8):
        p = (cc[b] - ss[b]) * table(row["cos", 1, b])
        m = (cc[b] + ss[b]) * table(row["cos", -1, b])
        cc[b], ss[b] = p + m, m - p
        p = (sc[b] + cs[b]) * table(row["sin", 1, b])
        m = (sc[b] - cs[b]) * table(row["sin", -1, b])
        sc[b], cs[b] = p + m, p - m
    back_c, back_s = t16_back(cc, cs), t16_back(sc, ss)
    out = [None] * NG
    for u in range(16):
        a, c_, s_ = back_a[u], back_c[u], S3 * back_s[u]
        h = a - 0.5 * c_
        out[place[0, u]] = a + c_
        out[place[1, u]] = h + s_
        out[place[2, u]] = h - s_
    return out


def group(k, j):
    return slice(k * SLAB + j * 256, k * SLAB + j * 256 + 256)


def split(hi, lo, rows, span, value):
    top = value.astype(BF16)
    hi[rows, span] = top
    lo[rows, span] = (value - top.astype(F32)).astype(BF16)


def product(hi, lo, whi, wlo, k, j):
    span = group(k, j)
    a, b = hi[:, span], lo[:, span]
    w = (k // 2) * 2 + j // 2
    lhs = jnp.concatenate([a, b, a], axis=1)
    rhs = jnp.concatenate([whi[w], whi[w], wlo[w]], axis=0)
    return jnp.dot(lhs, rhs, preferred_element_type=F32)


def turn(value, lanes):
    return pltpu.roll(value, lanes % 128, 1) if lanes % 128 else value


def to_thirds(f, third, first):
    c, s = third[first : first + 3], third[first + 3 : first + 6]
    return (
        f[0] + f[1] + f[2],
        f[0] * c[0] + f[1] * c[1] + f[2] * c[2],
        f[0] * s[0] + f[1] * s[1] + f[2] * s[2],
    )


def third_rows(third, h, rows):
    lanes = slice(128 * h, 128 * h + 128)
    return [jnp.broadcast_to(third[k : k + 1, lanes], (rows, 128)) for k in range(12)]


def from_thirds(a, c, s, third, first):
    return [a + c * third[first + m] + s * third[first + 3 + m] for m in range(3)]


def spectrum_kernel(q_ref, own, one, two, three, low_a, core_a, low_b, core_b, kern, third, whi, wlo, right, left, field, hi, lo):
    q = q_ref[0]
    sources = (
        (own, low_a),
        (one, core_a),
        (two, low_b),
        (three, core_b),
    )
    sub = lax.broadcasted_iota(jnp.int32, (8, 128), 0)
    to_right = sub % 4
    to_left = jnp.where(sub < 4, q, 4 + q % 2)
    place = lax.broadcasted_iota(jnp.int32, (8, 128), 1) // 16 % 3
    for delta, (bands_ref, low_ref) in enumerate(sources):
        base = (q ^ delta) * QX

        def densities(i, carry):
            rows = pl.ds(pl.multiple_of(8 * base + 16 * i, 16), 16)
            for h in range(2):
                pairs = []
                for half in range(2):
                    x = base + 2 * i + half
                    f = [[None] * 3 for _ in range(3)]
                    for m in range(3):
                        v = []
                        for n in range(3):
                            at = pl.ds(pl.multiple_of((2 * i + half) * PLANE + (m * SLAB + h * 384 + n * 128), 128), 128)
                            low = low_ref[:, at]
                            v.append(jnp.concatenate([bands_ref[:, at], low, low], axis=0))
                        for j in range(3):
                            got = jnp.where(place == j, v[0], jnp.where(place == (j + 1) % 3, v[1], v[2]))
                            got = turn(got, -16 * j)
                            r = jnp.take_along_axis(got, to_right, axis=0)
                            l = jnp.take_along_axis(got, to_left, axis=0)
                            span = slice(m * SLAB + j * 256 + h * 128, m * SLAB + j * 256 + h * 128 + 128)
                            right[x, :, span] = r
                            left[x, :, span] = l
                            f[m][j] = r * l
                    pairs.append(f)
                thirds_h = third_rows(third, h, 8)
                spec = []
                for f in pairs:
                    f = [to_thirds([f[m][j] for m in range(3)], thirds_h, 0) for j in range(3)]
                    spec.append([to_thirds([f[n][k] for n in range(3)], thirds_h, 6) for k in range(3)])
                for k in range(3):
                    for j in range(3):
                        span = slice(k * SLAB + j * 256 + h * 128, k * SLAB + j * 256 + h * 128 + 128)
                        split(hi, lo, rows, span, jnp.concatenate([spec[0][k][j], spec[1][k][j]], axis=0))
            return carry

        lax.fori_loop(0, QX // 2, densities, 0)

    for k in (0, 1):
        if k == 0:
            rows_of = [[product(hi, lo, whi, wlo, 0, j)] for j in range(3)]
        else:
            both = [(product(hi, lo, whi, wlo, 1, j), product(hi, lo, whi, wlo, 2, j)) for j in range(3)]
            rows_of = [[c - s, c + s] for c, s in both]
        for n in range(len(rows_of[0])):
            a, c, s = (rows_of[j][n] for j in range(3))
            field[:, group(k + n, 0)] = a
            field[:, group(k + n, 1)] = c - s
            field[:, group(k + n, 2)] = c + s

    def along_x(i, carry):
        span = pl.ds(pl.multiple_of(128 * i, 128), 128)
        f = [field[8 * x : 8 * x + 8, span] for x in range(NG)]
        out = convolve_x(f, lambda k: kern[k : k + 1, span])
        for x in range(NG):
            field[8 * x : 8 * x + 8, span] = out[x]
        return carry

    lax.fori_loop(0, PLANE // 128, along_x, 0)


def terms_kernel(q_ref, right, left, field, third, whi, wlo, near0, near2, cross, low0, low2, hi, lo, back):
    q = q_ref[0]

    def unmix(i, carry):
        rows = pl.ds(pl.multiple_of(16 * i, 16), 16)
        mixed = [[field[rows, group(k, j)] for j in range(3)] for k in range(3)]
        mixed = [[a, u + v, v - u] for a, u, v in mixed]
        for j in range(3):
            a, u, v = (mixed[k][j] for k in range(3))
            for k, value in enumerate((a, u + v, v - u)):
                split(hi, lo, rows, group(k, j), value)
        return carry

    lax.fori_loop(0, NG // 2, unmix, 0)
    for k in range(3):
        for j in range(3):
            back[:, group(k, j)] = product(hi, lo, whi, wlo, k, j)

    sub = lax.broadcasted_iota(jnp.int32, (8, 128), 0)
    mine = (sub == q).astype(F32)
    place = lax.broadcasted_iota(jnp.int32, (8, 128), 1) // 16 % 3

    for delta in range(4):
        base = (q ^ delta) * QX

        def finish(i, carry):
            for half in range(X_STEP):
                x = base + X_STEP * i + half
                rows = pl.ds(pl.multiple_of(x * 8, 8), 8)
                for h in range(2):
                    thirds_h = third_rows(third, h, 8)

                    def spot(k, j):
                        return slice(k * SLAB + j * 256 + h * 128, k * SLAB + j * 256 + h * 128 + 128)

                    v = [from_thirds(*(back[rows, spot(k, j)] for j in range(3)), thirds_h, 6) for k in range(3)]
                    v = [from_thirds(*(v[k][j] for k in range(3)), thirds_h, 0) for j in range(3)]
                    for m in range(3):
                        parts = []
                        for j in range(3):
                            pr = v[j][m] * right[x, :, spot(m, j)]
                            pr = pr + swapped(pr, sub, 1)
                            pr = pr + swapped(pr, sub, 2)
                            po = swapped(v[j][m] * left[x, :, spot(m, j)], sub, 4) + mine * pr
                            parts.append(turn(jnp.where(sub < 4, po, pr), 16 * j))
                        for n in range(3):
                            out = jnp.where(place == n, parts[0], jnp.where(place == (n + 1) % 3, parts[1], parts[2]))
                            start = (X_STEP * i + half) * PLANE + (m * SLAB + h * 384 + n * 128)
                            at = pl.ds(pl.multiple_of(start, 128), 128)
                            if delta % 2:
                                cross[delta // 2 * 4 : delta // 2 * 4 + 4, at] = out[0:4, :]
                                cross[8 + delta // 2 : 9 + delta // 2, at] = out[4:5, :]
                            else:
                                (near0, near2)[delta // 2][:, at] = out[0:4, :]
                                (low0, low2)[delta // 2][:, at] = out[4:5, :]
            return carry

        lax.fori_loop(0, QX // X_STEP, finish, 0)


def swapped(value, sub, flip):
    return jnp.take_along_axis(value, sub ^ flip, axis=0)


X_STEP = 2
VMEM_SPEC = pl.BlockSpec(memory_space=pltpu.VMEM)
SMEM_SPEC = pl.BlockSpec(memory_space=pltpu.SMEM)
SPLIT = [pltpu.VMEM((NG * 8, PLANE), BF16)] * 2


def spectrum(q, bands, kern, third, tables):
    return pl.pallas_call(
        spectrum_kernel,
        out_shape=[jax.ShapeDtypeStruct((NG, 8, PLANE), F32)] * 2 + [jax.ShapeDtypeStruct((NG * 8, PLANE), F32)],
        in_specs=[SMEM_SPEC] + [VMEM_SPEC] * 12,
        out_specs=[VMEM_SPEC] * 3,
        scratch_shapes=SPLIT,
        name="spectrum",
        compiler_params=pltpu.CompilerParams(vmem_limit_bytes=24 << 20),
    )(q.reshape(1), *bands, kern, third, *tables)


def terms(q, right, left, field, third, tables):
    return pl.pallas_call(
        terms_kernel,
        out_shape=[jax.ShapeDtypeStruct(shape, F32) for shape in [(4, QCELL)] * 2 + [(10, QCELL)] + [(1, QCELL)] * 2],
        in_specs=[SMEM_SPEC] + [VMEM_SPEC] * 6,
        out_specs=[VMEM_SPEC] * 5,
        scratch_shapes=SPLIT + [pltpu.VMEM((NG * 8, PLANE), F32)],
        name="terms",
        compiler_params=pltpu.CompilerParams(vmem_limit_bytes=28 << 20),
    )(q.reshape(1), right, left, field, third, *tables)


BOTH = ("band", "grid")
CHUNK = QCELL // 4


def small_call(body, outs, scratch=(), limit=8):
    vmem = pl.BlockSpec(memory_space=pltpu.VMEM)

    def call(where, *arrays):
        return pl.pallas_call(
            body,
            out_shape=[jax.ShapeDtypeStruct(shape, F32) for shape in outs],
            in_specs=[pl.BlockSpec(memory_space=pltpu.SMEM)] + [vmem] * len(arrays),
            out_specs=[vmem] * len(outs),
            scratch_shapes=list(scratch),
            compiler_params=pltpu.CompilerParams(vmem_limit_bytes=limit << 20),
        )(where, *arrays)

    return call


def chunk_of(where, k):
    return pl.ds(pl.multiple_of((where[2] ^ k) * CHUNK, 128), CHUNK)


def rows_kernel(where, orbitals, sel_a, sel_b):
    lower = where[0] < 2
    a, b = orbitals[0:2, :], orbitals[2:4, :]
    sel_a[...] = jnp.where(lower, a, b)
    sel_b[...] = jnp.where(lower, b, a)


def chunks_kernel(where, orbitals, *chunks):
    for k in range(4):
        chunks[k][...] = orbitals[:, chunk_of(where, k)]


def merge_kernel(where, near0, near2, low0, low2, across, near, far, owed_a, owed_b):
    first = where[0] % 2 == 0
    near[...] = near0[...] + across[0:4, :]
    far[...] = near2[...] + across[4:8, :]
    for out, low, row in ((owed_a, low0, 8), (owed_b, low2, 9)):
        a, b = low[...], across[row : row + 1, :]
        out[0:1, :] = jnp.where(first, a, b)
        out[1:2, :] = jnp.where(first, b, a)


def total_of(where, near, far, owed_a, owed_b, span):
    lower = where[0] < 2
    a, b = owed_a[:, span], owed_b[:, span]
    owed = jnp.concatenate([jnp.where(lower, a, b), jnp.where(lower, b, a)], axis=0)
    return -(near[:, span] + far[:, span] + owed)


def finalize_kernel(where, near, far, owed_a, owed_b, *chunks):
    for k in (1, 2, 3, 0):
        chunks[k][...] = total_of(where, near, far, owed_a, owed_b, chunk_of(where, k))


def vectors_kernel(where, near, far, owed_a, owed_b, vectors):
    for c in range(4):
        span = pl.ds(c * CHUNK, CHUNK)
        vectors[:, span] = total_of(where, near, far, owed_a, owed_b, span)


def margin_kernel(where, own0, oth0, own1, oth1, own2, oth2, own3, oth3, v0, v1, v2, v3, pieces, block):
    z, y, h = where[1], where[2], where[3]

    def halves(a):
        top = a.astype(BF16)
        return top, (a - top.astype(F32)).astype(BF16)

    v = jnp.concatenate(halves(jnp.concatenate([v0[...], v1[...], v2[...], v3[...]], axis=0)), axis=0)
    parts = jnp.concatenate([r[...] for r in (own0, oth0, own1, oth1, own2, oth2, own3, oth3)], axis=0)
    f = jnp.concatenate(halves(parts), axis=0)
    both = lax.dot_general(f, v, (((1,), (1,)), ((), ())), preferred_element_type=F32)
    both = both[0:128, :] + both[128:256, :]
    got = both[:, 0:16] + both[:, 16:32]
    for dz in range(4):
        for dy in range(4):
            row = 32 * dz + 4 * dy
            pair = got[row : row + 4, :], got[row + 16 : row + 20, :]
            at = (z + 4 - dz) % 4 * 4 + (y ^ dy)
            block[at, 0:4, :] = jnp.where(h == 0, pair[0], pair[1])
            block[at, 4:8, :] = jnp.where(h == 0, pair[1], pair[0])
    out = block[...].reshape(128, 16).T * (1.0 / NCELL)
    turned = [out] + [pltpu.roll(out, 32 * r, 1) for r in (1, 2, 3)]
    third_of = lax.broadcasted_iota(jnp.int32, (16, 128), 1) // 32
    keep = third_of == lax.broadcasted_iota(jnp.int32, (16, 128), 0) % 4
    for q_to in range(4):
        picked = turned[(3 - q_to) % 4]
        for j in range(3):
            picked = jnp.where(third_of == j, turned[(j - q_to) % 4], picked)
        picked = jnp.where(keep, picked, 0.0)
        for dy in range(4):
            row = jnp.sum(picked[4 * dy : 4 * dy + 4, :], axis=0, keepdims=True)
            pieces[pl.ds((y ^ dy) * 4 + q_to, 1), :] = row


def move(value, target):
    nb, nq = lax.axis_size("band"), lax.axis_size("grid")
    pairs = []
    for b in range(nb):
        for q in range(nq):
            z, y, h, q_to = target(b // 8, b // 2 % 4, b % 2, q)
            pairs.append((b * nq + q, ((z % 4) * 8 + (y % 4) * 2 + h) * nq + q_to))
    return lax.ppermute(value, BOTH, pairs)


def along_y(value, flip):
    return move(value, lambda z, y, h, q: (z, y ^ flip, h, q))


def along_z(value, k):
    return move(value, lambda z, y, h, q: (z + k, y, h, q))


def within(value, flip):
    return move(value, lambda z, y, h, q: (z, y, h, q ^ flip))


def around(value, blocks, flip):
    def target(z, y, h, q):
        b = (z * 8 + y * 2 + h + blocks) % 32
        return b // 8, b // 2 % 4, b % 2, q ^ flip

    return move(value, target)


def step(orbitals):
    b = lax.axis_index("band").astype(jnp.int32)
    q = lax.axis_index("grid").astype(jnp.int32)
    where = jnp.stack([q, b // 8, b // 2 % 4, b % 2])
    rows = small_call(rows_kernel, [(2, QCELL)] * 2)
    sel_a, sel_b = rows(where, orbitals)
    low_a = around(sel_a, 1, 0)
    low_b = around(sel_b, 1, 2)
    two = within(orbitals, 2)
    one = within(orbitals, 1)
    pc = small_call(chunks_kernel, [(4, CHUNK)] * 4)(where, orbitals)
    pieces = [pc[0]] + [along_y(pc[k], k) for k in (1, 2, 3)]
    *tables, kern, third = plane_tables()
    together = jnp.concatenate(pieces, axis=0)
    core_a = within(low_a, 1)
    core_b = within(low_b, 1)
    three = within(two, 1)
    other = move(together, lambda z, y, h, q: (z, y, 1 - h, q))
    right, left, field = spectrum(q, (orbitals, one, two, three, low_a, core_a, low_b, core_b), kern, third, tables[:2])
    near0, near2, cross, low0, low2 = terms(q, right, left, field, third, tables[2:4])
    across = within(cross, 1)
    together, other, _ = lax.optimization_barrier((together, other, near0))
    own1 = along_z(together, 1)
    own3 = along_z(together, 3)
    merge = small_call(merge_kernel, [(4, QCELL)] * 2 + [(2, QCELL)] * 2)
    near, both, owe_a, owe_b = merge(where, near0, near2, low0, low2, across)
    far = within(both, 2)
    owed_a = around(owe_a, -1, 0)
    owed_b = around(owe_b, -1, 2)
    oth1 = along_z(other, 1)
    oth3 = along_z(other, 3)
    own2 = along_z(own1, 1)
    oth2 = along_z(oth3, 3)
    finalize = small_call(finalize_kernel, [(4, CHUNK)] * 4)
    vc = finalize(where, near, far, owed_a, owed_b)
    (vectors,) = small_call(vectors_kernel, [(4, QCELL)])(where, near, far, owed_a, owed_b)
    given = [vc[0]] + [along_y(vc[k], k) for k in (1, 2, 3)]
    margin_part = small_call(margin_kernel, [(16, 128)], [pltpu.VMEM((16, 8, 16), F32)], 20)
    (sums,) = margin_part(where, together, other, own1, oth1, own2, oth2, own3, oth3, *given)
    groups = [[(z * 8 + y * 2 + h) * 4 + p for y in range(4) for p in range(4)] for z in range(4) for h in range(2)]
    sums = lax.all_to_all(sums, BOTH, 0, 0, tiled=True, axis_index_groups=groups)
    margin = jnp.sum(sums, axis=0).reshape(4, 32).T
    return vectors, margin


def solution(mesh):
    return jax.shard_map(
        step,
        mesh=mesh,
        in_specs=(P("band", "grid"),),
        out_specs=(P("band", "grid"), P("grid", "band")),
        check_vma=False,
    )
```

```python
import math

import jax
import jax.numpy as jnp
import numpy as np
from jax import lax
from jax.experimental import pallas as pl
from jax.experimental.pallas import tpu as pltpu
from jax.sharding import PartitionSpec as P

NG = 48
NCELL = 110592
PLANE = NG * NG
SLAB = 768
QX = 12
QCELL = QX * PLANE
F32 = jnp.float32
BF16 = jnp.bfloat16
R2 = math.sqrt(0.5)
C1 = math.cos(math.pi / 8)
C3 = math.cos(3 * math.pi / 8)
S3 = math.sqrt(3.0) / 2

ORDER = [("C", b) for b in range(9)] + [("S", b) for b in range(1, 8)]
SWAPPED = [("C", 0)] + [("S", b) for b in range(1, 8)] + [("C", 8)] + [("C", b) for b in range(1, 8)]


def sixteen(order):
    u = np.arange(16)
    cols = []
    for kind, b in order:
        col = np.cos(2 * np.pi * b * u / 16) if kind == "C" else np.sin(2 * np.pi * b * u / 16)
        cols.append(col / np.linalg.norm(col))
    return np.stack(cols, 1)


def folded(g):
    return (g + 24) % 48 - 24


def x_basis():
    keys, freqs, norms = [], [], []
    for b in range(9):
        keys.append(("A", "C", b)); freqs.append(3 * b); norms.append(48 if b in (0, 8) else 24)
    for b in range(1, 8):
        keys.append(("A", "S", b)); freqs.append(3 * b); norms.append(24)
    for b in (0, 8):
        for t in "cs":
            keys.append((t, "C", b)); freqs.append(16 + 3 * b); norms.append(24)
    for b in range(1, 8):
        for sign in (1, -1):
            for kind in ("cos", "sin"):
                keys.append((kind, sign, b)); freqs.append(16 + 3 * sign * b); norms.append(24)
    return keys, np.array(freqs), np.array(norms)


def lane_freqs(group):
    out = []
    for kind, b in ORDER:
        if group == "A":
            out.append(3 * b)
        elif b in (0, 8):
            out.append(16 + 3 * b)
        else:
            out.append(16 + 3 * b if (group == "u") == (kind == "C") else 16 - 3 * b)
    return np.array(out)


def kernel_values():
    _, gx, nx = x_basis()
    g = np.stack([lane_freqs(group) for group in "Auv"])
    gy, gz = g[:, None, :, None], g[None, :, None, :]
    q = folded(gx)[:, None, None, None, None] ** 2 + (folded(gy) ** 2 + folded(gz) ** 2)[None]
    q = q.astype(np.float64)
    kern = np.where(q > 0, 40.0 * (1.0 - np.exp(-q / 16.0)) / np.where(q > 0, q, 1.0), 0.0)
    return (kern / (9.0 * nx[:, None, None, None, None])).reshape(NG, PLANE).astype(np.float32)


PLACES = np.array([0, 3, 6, 1, 4, 7, 2, 5])
LANE_Y = np.repeat(np.concatenate([PLACES, 8 + PLACES]), 16)
LANE_Z = np.tile(np.arange(16), 16)


def thirds():
    rows = []
    for lane in (LANE_Y, LANE_Z):
        rows += [np.cos(2 * np.pi * (m + lane) / 3) for m in range(3)]
        rows += [np.sin(2 * np.pi * (m + lane) / 3) for m in range(3)]
    return np.concatenate([np.stack(rows), np.zeros((4, 256))]).astype(np.float32)


def factor_tables():
    bases = sixteen(ORDER), sixteen(SWAPPED)
    slow = [np.repeat(t[LANE_Y[::16]], 16, 1) for t in bases] + [t.T[:, LANE_Y] for t in bases]
    fast = [np.tile(t, (1, 16)) for t in bases] + [np.tile(t.T, (1, 16)) for t in bases]
    return np.stack(slow).astype(np.float32), np.stack(fast).astype(np.float32)


def tables_kernel(slow, fast, kern_in, third_in, hi_there, lo_there, hi_back, lo_back, kern, third):
    kern[...] = kern_in[...]
    third[...] = third_in[...]
    for way, (hi, lo) in enumerate(((hi_there, lo_there), (hi_back, lo_back))):
        for k in range(4):
            for u in range(16):
                w = fast[2 * way + k % 2] * slow[2 * way + k // 2, u : u + 1, :]
                top = w.astype(BF16)
                hi[k, 16 * u : 16 * u + 16, :] = top
                lo[k, 16 * u : 16 * u + 16, :] = (w - top.astype(F32)).astype(BF16)


def plane_tables():
    out = [jax.ShapeDtypeStruct((4, 256, 256), BF16)] * 4
    out += [jax.ShapeDtypeStruct((NG, PLANE), F32), jax.ShapeDtypeStruct((16, 256), F32)]
    return pl.pallas_call(
        tables_kernel, out_shape=out, name="plane_tables",
        compiler_params=pltpu.CompilerParams(vmem_limit_bytes=8 << 20),
    )(*[jnp.asarray(a) for a in (*factor_tables(), kernel_values(), thirds())])


def t16(f):
    o = [f[u] - f[u + 8] for u in range(8)]
    e = [f[u] + f[u + 8] for u in range(8)]
    ee = [e[u] + e[u + 4] for u in range(4)]
    eo = [e[u] - e[u + 4] for u in range(4)]
    c, s = {}, {}
    p0, p1 = ee[0] + ee[2], ee[1] + ee[3]
    c[0], c[8], c[4], s[4] = p0 + p1, p0 - p1, ee[0] - ee[2], ee[1] - ee[3]
    d, a = R2 * (eo[1] - eo[3]), R2 * (eo[1] + eo[3])
    c[2], c[6], s[2], s[6] = eo[0] + d, eo[0] - d, a + eo[2], a - eo[2]
    d1, d2, d3 = (o[u] - o[8 - u] for u in (1, 2, 3))
    s1, s2, s3 = (o[u] + o[8 - u] for u in (1, 2, 3))
    d2, s2 = R2 * d2, R2 * s2
    e1, e3 = o[0] + d2, o[0] - d2
    o1, o3 = C1 * d1 + C3 * d3, C3 * d1 - C1 * d3
    c[1], c[7], c[3], c[5] = e1 + o1, e1 - o1, e3 + o3, e3 - o3
    x1, x3 = o[4] + s2, o[4] - s2
    y1, y3 = C3 * s1 + C1 * s3, C1 * s1 - C3 * s3
    s[1], s[7], s[3], s[5] = y1 + x1, y1 - x1, y3 - x3, y3 + x3
    return c, s


def t16_back(c, s):
    e1, o1, e3, o3 = c[1] + c[7], c[1] - c[7], c[3] + c[5], c[3] - c[5]
    o0, d2 = e1 + e3, R2 * (e1 - e3)
    d1, d3 = C1 * o1 + C3 * o3, C3 * o1 - C1 * o3
    y1, x1, y3, x3 = s[1] + s[7], s[1] - s[7], s[3] + s[5], s[5] - s[3]
    o4, s2 = x1 + x3, R2 * (x1 - x3)
    s1, s3 = C3 * y1 + C1 * y3, C1 * y1 - C3 * y3
    o = [o0, d1 + s1, d2 + s2, d3 + s3, o4, s3 - d3, s2 - d2, s1 - d1]
    d, a = R2 * (c[2] - c[6]), R2 * (s[2] + s[6])
    eo = [c[2] + c[6], d + a, s[2] - s[6], a - d]
    p0, p1 = c[0] + c[8], c[0] - c[8]
    ee = [p0 + c[4], p1 + s[4], p0 - c[4], p1 - s[4]]
    e = [ee[u] + eo[u] for u in range(4)] + [ee[u] - eo[u] for u in range(4)]
    return [e[u] + o[u] for u in range(8)] + [e[u] - o[u] for u in range(8)]


def convolve_x(f, table):
    keys, _, _ = x_basis()
    row = {key: k for k, key in enumerate(keys)}
    place = {(x % 3, x % 16): x for x in range(NG)}
    part = {"A": [], "c": [], "s": []}
    for u in range(16):
        f0, f1, f2 = (f[place[t, u]] for t in range(3))
        a = f1 + f2
        part["A"].append(f0 + a)
        part["c"].append(f0 - 0.5 * a)
        part["s"].append(S3 * (f1 - f2))
    c, s = t16(part["A"])
    c = {b: v * table(row["A", "C", b]) for b, v in c.items()}
    s = {b: v * table(row["A", "S", b]) for b, v in s.items()}
    back_a = t16_back(c, s)
    cc, cs = t16(part["c"])
    sc, ss = t16(part["s"])
    for b in (0, 8):
        cc[b] = cc[b] * table(row["c", "C", b])
        sc[b] = sc[b] * table(row["s", "C", b])
    for b in range(1, 8):
        p = (cc[b] - ss[b]) * table(row["cos", 1, b])
        m = (cc[b] + ss[b]) * table(row["cos", -1, b])
        cc[b], ss[b] = p + m, m - p
        p = (sc[b] + cs[b]) * table(row["sin", 1, b])
        m = (sc[b] - cs[b]) * table(row["sin", -1, b])
        sc[b], cs[b] = p + m, p - m
    back_c, back_s = t16_back(cc, cs), t16_back(sc, ss)
    out = [None] * NG
    for u in range(16):
        a, c_, s_ = back_a[u], back_c[u], S3 * back_s[u]
        h = a - 0.5 * c_
        out[place[0, u]] = a + c_
        out[place[1, u]] = h + s_
        out[place[2, u]] = h - s_
    return out


def group(k, j):
    return slice(k * SLAB + j * 256, k * SLAB + j * 256 + 256)


def split(hi, lo, rows, span, value):
    top = value.astype(BF16)
    hi[rows, span] = top
    lo[rows, span] = (value - top.astype(F32)).astype(BF16)


def product(hi, lo, whi, wlo, k, j):
    span = group(k, j)
    a, b = hi[:, span], lo[:, span]
    w = (k // 2) * 2 + j // 2
    lhs = jnp.concatenate([a, b, a], axis=1)
    rhs = jnp.concatenate([whi[w], whi[w], wlo[w]], axis=0)
    return jnp.dot(lhs, rhs, preferred_element_type=F32)


def turn(value, lanes):
    return pltpu.roll(value, lanes % 128, 1) if lanes % 128 else value


def to_thirds(f, third, first):
    c, s = third[first : first + 3], third[first + 3 : first + 6]
    return (
        f[0] + f[1] + f[2],
        f[0] * c[0] + f[1] * c[1] + f[2] * c[2],
        f[0] * s[0] + f[1] * s[1] + f[2] * s[2],
    )


def third_rows(third, h, rows):
    lanes = slice(128 * h, 128 * h + 128)
    return [jnp.broadcast_to(third[k : k + 1, lanes], (rows, 128)) for k in range(12)]


def from_thirds(a, c, s, third, first):
    return [a + c * third[first + m] + s * third[first + 3 + m] for m in range(3)]


def densities_of(q, sources, third, right, left, hi, lo):
    sub = lax.broadcasted_iota(jnp.int32, (8, 128), 0)
    to_right = sub % 4
    to_left = jnp.where(sub < 4, q, 4 + q % 2)
    place = lax.broadcasted_iota(jnp.int32, (8, 128), 1) // 16 % 3
    for delta, bands_ref, low_ref in sources:
        base = (q ^ delta) * QX

        def densities(i, carry):
            rows = pl.ds(pl.multiple_of(8 * base + 16 * i, 16), 16)
            for h in range(2):
                pairs = []
                for half in range(2):
                    x = base + 2 * i + half
                    f = [[None] * 3 for _ in range(3)]
                    for m in range(3):
                        v = []
                        for n in range(3):
                            at = pl.ds(pl.multiple_of((2 * i + half) * PLANE + (m * SLAB + h * 384 + n * 128), 128), 128)
                            low = low_ref[:, at]
                            v.append(jnp.concatenate([bands_ref[:, at], low, low], axis=0))
                        for j in range(3):
                            got = jnp.where(place == j, v[0], jnp.where(place == (j + 1) % 3, v[1], v[2]))
                            got = turn(got, -16 * j)
                            r = jnp.take_along_axis(got, to_right, axis=0)
                            l = jnp.take_along_axis(got, to_left, axis=0)
                            span = slice(m * SLAB + j * 256 + h * 128, m * SLAB + j * 256 + h * 128 + 128)
                            right[x, :, span] = r
                            left[x, :, span] = l
                            f[m][j] = r * l
                    pairs.append(f)
                thirds_h = third_rows(third, h, 8)
                spec = []
                for f in pairs:
                    f = [to_thirds([f[m][j] for m in range(3)], thirds_h, 0) for j in range(3)]
                    spec.append([to_thirds([f[n][k] for n in range(3)], thirds_h, 6) for k in range(3)])
                for k in range(3):
                    for j in range(3):
                        span = slice(k * SLAB + j * 256 + h * 128, k * SLAB + j * 256 + h * 128 + 128)
                        split(hi, lo, rows, span, jnp.concatenate([spec[0][k][j], spec[1][k][j]], axis=0))
            return carry

        lax.fori_loop(0, QX // 2, densities, 0)


def first_kernel(q_ref, own, one, low_a, core_a, third, right, left, hi, lo):
    densities_of(q_ref[0], ((0, own, low_a), (1, one, core_a)), third, right, left, hi, lo)


def spectrum_kernel(q_ref, two, three, low_b, core_b, kern, third, whi, wlo, right_in, left_in, hi_in, lo_in,
                    right, left, hi, lo, field):
    densities_of(q_ref[0], ((2, two, low_b), (3, three, core_b)), third, right, left, hi, lo)
    for k in (0, 1):
        if k == 0:
            rows_of = [[product(hi, lo, whi, wlo, 0, j)] for j in range(3)]
        else:
            both = [(product(hi, lo, whi, wlo, 1, j), product(hi, lo, whi, wlo, 2, j)) for j in range(3)]
            rows_of = [[c - s, c + s] for c, s in both]
        for n in range(len(rows_of[0])):
            a, c, s = (rows_of[j][n] for j in range(3))
            field[:, group(k + n, 0)] = a
            field[:, group(k + n, 1)] = c - s
            field[:, group(k + n, 2)] = c + s

    def along_x(i, carry):
        span = pl.ds(pl.multiple_of(128 * i, 128), 128)
        f = [field[8 * x : 8 * x + 8, span] for x in range(NG)]
        out = convolve_x(f, lambda k: kern[k : k + 1, span])
        for x in range(NG):
            field[8 * x : 8 * x + 8, span] = out[x]
        return carry

    lax.fori_loop(0, PLANE // 128, along_x, 0)


def terms_kernel(q_ref, right, left, field, third, whi, wlo, near0, near2, cross, low0, low2, hi, lo, back):
    q = q_ref[0]

    def unmix(i, carry):
        rows = pl.ds(pl.multiple_of(16 * i, 16), 16)
        mixed = [[field[rows, group(k, j)] for j in range(3)] for k in range(3)]
        mixed = [[a, u + v, v - u] for a, u, v in mixed]
        for j in range(3):
            a, u, v = (mixed[k][j] for k in range(3))
            for k, value in enumerate((a, u + v, v - u)):
                split(hi, lo, rows, group(k, j), value)
        return carry

    lax.fori_loop(0, NG // 2, unmix, 0)
    for k in range(3):
        for j in range(3):
            back[:, group(k, j)] = product(hi, lo, whi, wlo, k, j)

    sub = lax.broadcasted_iota(jnp.int32, (8, 128), 0)
    mine = (sub == q).astype(F32)
    place = lax.broadcasted_iota(jnp.int32, (8, 128), 1) // 16 % 3

    for delta in range(4):
        base = (q ^ delta) * QX

        def finish(i, carry):
            for half in range(X_STEP):
                x = base + X_STEP * i + half
                rows = pl.ds(pl.multiple_of(x * 8, 8), 8)
                for h in range(2):
                    thirds_h = third_rows(third, h, 8)

                    def spot(k, j):
                        return slice(k * SLAB + j * 256 + h * 128, k * SLAB + j * 256 + h * 128 + 128)

                    v = [from_thirds(*(back[rows, spot(k, j)] for j in range(3)), thirds_h, 6) for k in range(3)]
                    v = [from_thirds(*(v[k][j] for k in range(3)), thirds_h, 0) for j in range(3)]
                    for m in range(3):
                        parts = []
                        for j in range(3):
                            pr = v[j][m] * right[x, :, spot(m, j)]
                            pr = pr + swapped(pr, sub, 1)
                            pr = pr + swapped(pr, sub, 2)
                            po = swapped(v[j][m] * left[x, :, spot(m, j)], sub, 4) + mine * pr
                            parts.append(turn(jnp.where(sub < 4, po, pr), 16 * j))
                        for n in range(3):
                            out = jnp.where(place == n, parts[0], jnp.where(place == (n + 1) % 3, parts[1], parts[2]))
                            start = (X_STEP * i + half) * PLANE + (m * SLAB + h * 384 + n * 128)
                            at = pl.ds(pl.multiple_of(start, 128), 128)
                            if delta % 2:
                                cross[delta // 2 * 4 : delta // 2 * 4 + 4, at] = out[0:4, :]
                                cross[8 + delta // 2 : 9 + delta // 2, at] = out[4:5, :]
                            else:
                                (near0, near2)[delta // 2][:, at] = out[0:4, :]
                                (low0, low2)[delta // 2][:, at] = out[4:5, :]
            return carry

        lax.fori_loop(0, QX // X_STEP, finish, 0)


def swapped(value, sub, flip):
    return jnp.take_along_axis(value, sub ^ flip, axis=0)


X_STEP = 2
VMEM_SPEC = pl.BlockSpec(memory_space=pltpu.VMEM)
SMEM_SPEC = pl.BlockSpec(memory_space=pltpu.SMEM)
SPLIT = [pltpu.VMEM((NG * 8, PLANE), BF16)] * 2


STATE = [jax.ShapeDtypeStruct((NG, 8, PLANE), F32)] * 2 + [jax.ShapeDtypeStruct((NG * 8, PLANE), BF16)] * 2


def first_densities(q, bands, third):
    return pl.pallas_call(
        first_kernel,
        out_shape=STATE,
        in_specs=[SMEM_SPEC] + [VMEM_SPEC] * 5,
        out_specs=[VMEM_SPEC] * 4,
        name="first_densities",
        compiler_params=pltpu.CompilerParams(vmem_limit_bytes=16 << 20),
    )(q.reshape(1), *bands, third)


def spectrum(q, bands, kern, third, tables, state):
    return pl.pallas_call(
        spectrum_kernel,
        out_shape=STATE + [jax.ShapeDtypeStruct((NG * 8, PLANE), F32)],
        in_specs=[SMEM_SPEC] + [VMEM_SPEC] * 12,
        out_specs=[VMEM_SPEC] * 5,
        input_output_aliases={9: 0, 10: 1, 11: 2, 12: 3},
        name="spectrum",
        compiler_params=pltpu.CompilerParams(vmem_limit_bytes=28 << 20),
    )(q.reshape(1), *bands, kern, third, *tables, *state)


def terms(q, right, left, field, third, tables):
    return pl.pallas_call(
        terms_kernel,
        out_shape=[jax.ShapeDtypeStruct(shape, F32) for shape in [(4, QCELL)] * 2 + [(10, QCELL)] + [(1, QCELL)] * 2],
        in_specs=[SMEM_SPEC] + [VMEM_SPEC] * 6,
        out_specs=[VMEM_SPEC] * 5,
        scratch_shapes=SPLIT + [pltpu.VMEM((NG * 8, PLANE), F32)],
        name="terms",
        compiler_params=pltpu.CompilerParams(vmem_limit_bytes=28 << 20),
    )(q.reshape(1), right, left, field, third, *tables)


BOTH = ("band", "grid")
CHUNK = QCELL // 4


def small_call(body, outs, scratch=(), limit=8):
    vmem = pl.BlockSpec(memory_space=pltpu.VMEM)

    def call(where, *arrays):
        return pl.pallas_call(
            body,
            out_shape=[jax.ShapeDtypeStruct(shape, F32) for shape in outs],
            in_specs=[pl.BlockSpec(memory_space=pltpu.SMEM)] + [vmem] * len(arrays),
            out_specs=[vmem] * len(outs),
            scratch_shapes=list(scratch),
            compiler_params=pltpu.CompilerParams(vmem_limit_bytes=limit << 20),
        )(where, *arrays)

    return call


def chunk_of(where, k):
    return pl.ds(pl.multiple_of((where[2] ^ k) * CHUNK, 128), CHUNK)


def rows_kernel(where, orbitals, sel_a, sel_b):
    lower = where[0] < 2
    a, b = orbitals[0:2, :], orbitals[2:4, :]
    sel_a[...] = jnp.where(lower, a, b)
    sel_b[...] = jnp.where(lower, b, a)


def chunks_kernel(where, orbitals, *chunks):
    for k in range(4):
        chunks[k][...] = orbitals[:, chunk_of(where, k)]


def merge_kernel(where, near0, near2, low0, low2, across, near, far, owed_a, owed_b):
    first = where[0] % 2 == 0
    near[...] = near0[...] + across[0:4, :]
    far[...] = near2[...] + across[4:8, :]
    for out, low, row in ((owed_a, low0, 8), (owed_b, low2, 9)):
        a, b = low[...], across[row : row + 1, :]
        out[0:1, :] = jnp.where(first, a, b)
        out[1:2, :] = jnp.where(first, b, a)


def total_of(where, near, far, owed_a, owed_b, span):
    lower = where[0] < 2
    a, b = owed_a[:, span], owed_b[:, span]
    owed = jnp.concatenate([jnp.where(lower, a, b), jnp.where(lower, b, a)], axis=0)
    return -(near[:, span] + far[:, span] + owed)


def finalize_kernel(where, near, far, owed_a, owed_b, *chunks):
    for k in (1, 2, 3, 0):
        chunks[k][...] = total_of(where, near, far, owed_a, owed_b, chunk_of(where, k))


def vectors_kernel(where, near, far, owed_a, owed_b, vectors):
    for c in range(4):
        span = pl.ds(c * CHUNK, CHUNK)
        vectors[:, span] = total_of(where, near, far, owed_a, owed_b, span)


def margin_kernel(where, own0, oth0, own1, oth1, own2, oth2, own3, oth3, v0, v1, v2, v3, pieces, block):
    z, y, h = where[1], where[2], where[3]

    def halves(a):
        top = a.astype(BF16)
        return top, (a - top.astype(F32)).astype(BF16)

    v = jnp.concatenate(halves(jnp.concatenate([v0[...], v1[...], v2[...], v3[...]], axis=0)), axis=0)
    parts = jnp.concatenate([r[...] for r in (own0, oth0, own1, oth1, own2, oth2, own3, oth3)], axis=0)
    f = jnp.concatenate(halves(parts), axis=0)
    both = lax.dot_general(f, v, (((1,), (1,)), ((), ())), preferred_element_type=F32)
    both = both[0:128, :] + both[128:256, :]
    got = both[:, 0:16] + both[:, 16:32]
    for dz in range(4):
        for dy in range(4):
            row = 32 * dz + 4 * dy
            pair = got[row : row + 4, :], got[row + 16 : row + 20, :]
            at = (z + 4 - dz) % 4 * 4 + (y ^ dy)
            block[at, 0:4, :] = jnp.where(h == 0, pair[0], pair[1])
            block[at, 4:8, :] = jnp.where(h == 0, pair[1], pair[0])
    out = block[...].reshape(128, 16).T * (1.0 / NCELL)
    turned = [out] + [pltpu.roll(out, 32 * r, 1) for r in (1, 2, 3)]
    third_of = lax.broadcasted_iota(jnp.int32, (16, 128), 1) // 32
    keep = third_of == lax.broadcasted_iota(jnp.int32, (16, 128), 0) % 4
    for q_to in range(4):
        picked = turned[(3 - q_to) % 4]
        for j in range(3):
            picked = jnp.where(third_of == j, turned[(j - q_to) % 4], picked)
        picked = jnp.where(keep, picked, 0.0)
        for dy in range(4):
            row = jnp.sum(picked[4 * dy : 4 * dy + 4, :], axis=0, keepdims=True)
            pieces[pl.ds((y ^ dy) * 4 + q_to, 1), :] = row


def move(value, target):
    nb, nq = lax.axis_size("band"), lax.axis_size("grid")
    pairs = []
    for b in range(nb):
        for q in range(nq):
            z, y, h, q_to = target(b // 8, b // 2 % 4, b % 2, q)
            pairs.append((b * nq + q, ((z % 4) * 8 + (y % 4) * 2 + h) * nq + q_to))
    return lax.ppermute(value, BOTH, pairs)


def along_y(value, flip):
    return move(value, lambda z, y, h, q: (z, y ^ flip, h, q))


def along_z(value, k):
    return move(value, lambda z, y, h, q: (z + k, y, h, q))


def within(value, flip):
    return move(value, lambda z, y, h, q: (z, y, h, q ^ flip))


def around(value, blocks, flip):
    def target(z, y, h, q):
        b = (z * 8 + y * 2 + h + blocks) % 32
        return b // 8, b // 2 % 4, b % 2, q ^ flip

    return move(value, target)


def step(orbitals):
    b = lax.axis_index("band").astype(jnp.int32)
    q = lax.axis_index("grid").astype(jnp.int32)
    where = jnp.stack([q, b // 8, b // 2 % 4, b % 2])
    rows = small_call(rows_kernel, [(2, QCELL)] * 2)
    sel_a, sel_b = rows(where, orbitals)
    low_a = around(sel_a, 1, 0)
    low_b = around(sel_b, 1, 2)
    two = within(orbitals, 2)
    one = within(orbitals, 1)
    pc = small_call(chunks_kernel, [(4, CHUNK)] * 4)(where, orbitals)
    pieces = [pc[0]] + [along_y(pc[k], k) for k in (1, 2, 3)]
    *tables, kern, third = plane_tables()
    together = jnp.concatenate(pieces, axis=0)
    core_a = within(low_a, 1)
    core_b = within(low_b, 1)
    three = within(two, 1)
    other = move(together, lambda z, y, h, q: (z, y, 1 - h, q))
    own1 = along_z(together, 1)
    own3 = along_z(together, 3)
    state = first_densities(q, (orbitals, one, low_a, core_a), third)
    right, left, _, _, field = spectrum(q, (two, three, low_b, core_b), kern, third, tables[:2], state)
    near0, near2, cross, low0, low2 = terms(q, right, left, field, third, tables[2:4])
    across = within(cross, 1)
    other, _ = lax.optimization_barrier((other, near0))
    oth1 = along_z(other, 1)
    oth3 = along_z(other, 3)
    own2 = along_z(own1, 1)
    merge = small_call(merge_kernel, [(4, QCELL)] * 2 + [(2, QCELL)] * 2)
    near, both, owe_a, owe_b = merge(where, near0, near2, low0, low2, across)
    far = within(both, 2)
    owed_a = around(owe_a, -1, 0)
    owed_b = around(owe_b, -1, 2)
    oth2 = along_z(oth1, 1)
    finalize = small_call(finalize_kernel, [(4, CHUNK)] * 4)
    vc = finalize(where, near, far, owed_a, owed_b)
    (vectors,) = small_call(vectors_kernel, [(4, QCELL)])(where, near, far, owed_a, owed_b)
    given = [vc[0]] + [along_y(vc[k], k) for k in (1, 2, 3)]
    margin_part = small_call(margin_kernel, [(16, 128)], [pltpu.VMEM((16, 8, 16), F32)], 20)
    (sums,) = margin_part(where, together, other, own1, oth1, own2, oth2, own3, oth3, *given)
    groups = [[(z * 8 + y * 2 + h) * 4 + p for y in range(4) for p in range(4)] for z in range(4) for h in range(2)]
    sums = lax.all_to_all(sums, BOTH, 0, 0, tiled=True, axis_index_groups=groups)
    margin = jnp.sum(sums, axis=0).reshape(4, 32).T
    return vectors, margin


def solution(mesh):
    return jax.shard_map(
        step,
        mesh=mesh,
        in_specs=(P("band", "grid"),),
        out_specs=(P("band", "grid"), P("grid", "band")),
        check_vma=False,
    )
```

```python
import math

import jax
import jax.numpy as jnp
import numpy as np
from jax import lax
from jax.experimental import pallas as pl
from jax.experimental.pallas import tpu as pltpu
from jax.sharding import PartitionSpec as P

NG = 48
NCELL = 110592
PLANE = NG * NG
SLAB = 768
QX = 12
QCELL = QX * PLANE
F32 = jnp.float32
BF16 = jnp.bfloat16
R2 = math.sqrt(0.5)
C1 = math.cos(math.pi / 8)
C3 = math.cos(3 * math.pi / 8)
S3 = math.sqrt(3.0) / 2

ORDER = [("C", b) for b in range(9)] + [("S", b) for b in range(1, 8)]
SWAPPED = [("C", 0)] + [("S", b) for b in range(1, 8)] + [("C", 8)] + [("C", b) for b in range(1, 8)]


def sixteen(order):
    u = np.arange(16)
    cols = []
    for kind, b in order:
        col = np.cos(2 * np.pi * b * u / 16) if kind == "C" else np.sin(2 * np.pi * b * u / 16)
        cols.append(col / np.linalg.norm(col))
    return np.stack(cols, 1)


def folded(g):
    return (g + 24) % 48 - 24


def x_basis():
    keys, freqs, norms = [], [], []
    for b in range(9):
        keys.append(("A", "C", b)); freqs.append(3 * b); norms.append(48 if b in (0, 8) else 24)
    for b in range(1, 8):
        keys.append(("A", "S", b)); freqs.append(3 * b); norms.append(24)
    for b in (0, 8):
        for t in "cs":
            keys.append((t, "C", b)); freqs.append(16 + 3 * b); norms.append(24)
    for b in range(1, 8):
        for sign in (1, -1):
            for kind in ("cos", "sin"):
                keys.append((kind, sign, b)); freqs.append(16 + 3 * sign * b); norms.append(24)
    return keys, np.array(freqs), np.array(norms)


def lane_freqs(group):
    out = []
    for kind, b in ORDER:
        if group == "A":
            out.append(3 * b)
        elif b in (0, 8):
            out.append(16 + 3 * b)
        else:
            out.append(16 + 3 * b if (group == "u") == (kind == "C") else 16 - 3 * b)
    return np.array(out)


def kernel_values():
    _, gx, nx = x_basis()
    g = np.stack([lane_freqs(group) for group in "Auv"])
    gy, gz = g[:, None, :, None], g[None, :, None, :]
    q = folded(gx)[:, None, None, None, None] ** 2 + (folded(gy) ** 2 + folded(gz) ** 2)[None]
    q = q.astype(np.float64)
    kern = np.where(q > 0, 40.0 * (1.0 - np.exp(-q / 16.0)) / np.where(q > 0, q, 1.0), 0.0)
    return (kern / (9.0 * nx[:, None, None, None, None])).reshape(NG, PLANE).astype(np.float32)


PLACES = np.array([0, 3, 6, 1, 4, 7, 2, 5])
LANE_Y = np.repeat(np.concatenate([PLACES, 8 + PLACES]), 16)
LANE_Z = np.tile(np.arange(16), 16)


def thirds():
    rows = []
    for lane in (LANE_Y, LANE_Z):
        rows += [np.cos(2 * np.pi * (m + lane) / 3) for m in range(3)]
        rows += [np.sin(2 * np.pi * (m + lane) / 3) for m in range(3)]
    return np.concatenate([np.stack(rows), np.zeros((4, 256))]).astype(np.float32)


def factor_tables():
    bases = sixteen(ORDER), sixteen(SWAPPED)
    slow = [np.repeat(t[LANE_Y[::16]], 16, 1) for t in bases] + [t.T[:, LANE_Y] for t in bases]
    fast = [np.tile(t, (1, 16)) for t in bases] + [np.tile(t.T, (1, 16)) for t in bases]
    return np.stack(slow).astype(np.float32), np.stack(fast).astype(np.float32)


def tables_kernel(slow, fast, kern_in, third_in, hi_there, lo_there, hi_back, lo_back, kern, third):
    kern[...] = kern_in[...]
    third[...] = third_in[...]
    for way, (hi, lo) in enumerate(((hi_there, lo_there), (hi_back, lo_back))):
        for k in range(4):
            for u in range(16):
                w = fast[2 * way + k % 2] * slow[2 * way + k // 2, u : u + 1, :]
                top = w.astype(BF16)
                hi[k, 16 * u : 16 * u + 16, :] = top
                lo[k, 16 * u : 16 * u + 16, :] = (w - top.astype(F32)).astype(BF16)


def plane_tables():
    out = [jax.ShapeDtypeStruct((4, 256, 256), BF16)] * 4
    out += [jax.ShapeDtypeStruct((NG, PLANE), F32), jax.ShapeDtypeStruct((16, 256), F32)]
    return pl.pallas_call(
        tables_kernel, out_shape=out, name="plane_tables",
        compiler_params=pltpu.CompilerParams(vmem_limit_bytes=8 << 20),
    )(*[jnp.asarray(a) for a in (*factor_tables(), kernel_values(), thirds())])


def t16(f):
    o = [f[u] - f[u + 8] for u in range(8)]
    e = [f[u] + f[u + 8] for u in range(8)]
    ee = [e[u] + e[u + 4] for u in range(4)]
    eo = [e[u] - e[u + 4] for u in range(4)]
    c, s = {}, {}
    p0, p1 = ee[0] + ee[2], ee[1] + ee[3]
    c[0], c[8], c[4], s[4] = p0 + p1, p0 - p1, ee[0] - ee[2], ee[1] - ee[3]
    d, a = R2 * (eo[1] - eo[3]), R2 * (eo[1] + eo[3])
    c[2], c[6], s[2], s[6] = eo[0] + d, eo[0] - d, a + eo[2], a - eo[2]
    d1, d2, d3 = (o[u] - o[8 - u] for u in (1, 2, 3))
    s1, s2, s3 = (o[u] + o[8 - u] for u in (1, 2, 3))
    d2, s2 = R2 * d2, R2 * s2
    e1, e3 = o[0] + d2, o[0] - d2
    o1, o3 = C1 * d1 + C3 * d3, C3 * d1 - C1 * d3
    c[1], c[7], c[3], c[5] = e1 + o1, e1 - o1, e3 + o3, e3 - o3
    x1, x3 = o[4] + s2, o[4] - s2
    y1, y3 = C3 * s1 + C1 * s3, C1 * s1 - C3 * s3
    s[1], s[7], s[3], s[5] = y1 + x1, y1 - x1, y3 - x3, y3 + x3
    return c, s


def t16_back(c, s):
    e1, o1, e3, o3 = c[1] + c[7], c[1] - c[7], c[3] + c[5], c[3] - c[5]
    o0, d2 = e1 + e3, R2 * (e1 - e3)
    d1, d3 = C1 * o1 + C3 * o3, C3 * o1 - C1 * o3
    y1, x1, y3, x3 = s[1] + s[7], s[1] - s[7], s[3] + s[5], s[5] - s[3]
    o4, s2 = x1 + x3, R2 * (x1 - x3)
    s1, s3 = C3 * y1 + C1 * y3, C1 * y1 - C3 * y3
    o = [o0, d1 + s1, d2 + s2, d3 + s3, o4, s3 - d3, s2 - d2, s1 - d1]
    d, a = R2 * (c[2] - c[6]), R2 * (s[2] + s[6])
    eo = [c[2] + c[6], d + a, s[2] - s[6], a - d]
    p0, p1 = c[0] + c[8], c[0] - c[8]
    ee = [p0 + c[4], p1 + s[4], p0 - c[4], p1 - s[4]]
    e = [ee[u] + eo[u] for u in range(4)] + [ee[u] - eo[u] for u in range(4)]
    return [e[u] + o[u] for u in range(8)] + [e[u] - o[u] for u in range(8)]


def convolve_x(f, table):
    keys, _, _ = x_basis()
    row = {key: k for k, key in enumerate(keys)}
    place = {(x % 3, x % 16): x for x in range(NG)}
    part = {"A": [], "c": [], "s": []}
    for u in range(16):
        f0, f1, f2 = (f[place[t, u]] for t in range(3))
        a = f1 + f2
        part["A"].append(f0 + a)
        part["c"].append(f0 - 0.5 * a)
        part["s"].append(S3 * (f1 - f2))
    c, s = t16(part["A"])
    c = {b: v * table(row["A", "C", b]) for b, v in c.items()}
    s = {b: v * table(row["A", "S", b]) for b, v in s.items()}
    back_a = t16_back(c, s)
    cc, cs = t16(part["c"])
    sc, ss = t16(part["s"])
    for b in (0, 8):
        cc[b] = cc[b] * table(row["c", "C", b])
        sc[b] = sc[b] * table(row["s", "C", b])
    for b in range(1, 8):
        p = (cc[b] - ss[b]) * table(row["cos", 1, b])
        m = (cc[b] + ss[b]) * table(row["cos", -1, b])
        cc[b], ss[b] = p + m, m - p
        p = (sc[b] + cs[b]) * table(row["sin", 1, b])
        m = (sc[b] - cs[b]) * table(row["sin", -1, b])
        sc[b], cs[b] = p + m, p - m
    back_c, back_s = t16_back(cc, cs), t16_back(sc, ss)
    out = [None] * NG
    for u in range(16):
        a, c_, s_ = back_a[u], back_c[u], S3 * back_s[u]
        h = a - 0.5 * c_
        out[place[0, u]] = a + c_
        out[place[1, u]] = h + s_
        out[place[2, u]] = h - s_
    return out


def group(k, j):
    return slice(k * SLAB + j * 256, k * SLAB + j * 256 + 256)


def split(hi, lo, rows, span, value):
    top = value.astype(BF16)
    hi[rows, span] = top
    lo[rows, span] = (value - top.astype(F32)).astype(BF16)


def product(hi, lo, whi, wlo, k, j):
    span = group(k, j)
    a, b = hi[:, span], lo[:, span]
    w = (k // 2) * 2 + j // 2
    lhs = jnp.concatenate([a, b, a], axis=1)
    rhs = jnp.concatenate([whi[w], whi[w], wlo[w]], axis=0)
    return jnp.dot(lhs, rhs, preferred_element_type=F32)


def turn(value, lanes):
    return pltpu.roll(value, lanes % 128, 1) if lanes % 128 else value


def to_thirds(f, third, first):
    c, s = third[first : first + 3], third[first + 3 : first + 6]
    return (
        f[0] + f[1] + f[2],
        f[0] * c[0] + f[1] * c[1] + f[2] * c[2],
        f[0] * s[0] + f[1] * s[1] + f[2] * s[2],
    )


def third_rows(third, h, rows):
    lanes = slice(128 * h, 128 * h + 128)
    return [jnp.broadcast_to(third[k : k + 1, lanes], (rows, 128)) for k in range(12)]


def from_thirds(a, c, s, third, first):
    return [a + c * third[first + m] + s * third[first + 3 + m] for m in range(3)]


def densities_of(q, sources, third, right, left, hi, lo):
    sub = lax.broadcasted_iota(jnp.int32, (8, 128), 0)
    to_right = sub % 4
    to_left = jnp.where(sub < 4, q, 4 + q % 2)
    place = lax.broadcasted_iota(jnp.int32, (8, 128), 1) // 16 % 3
    for delta, bands_ref, low_ref in sources:
        base = (q ^ delta) * QX

        def densities(i, carry):
            rows = pl.ds(pl.multiple_of(8 * base + 16 * i, 16), 16)
            for h in range(2):
                pairs = []
                for half in range(2):
                    x = base + 2 * i + half
                    f = [[None] * 3 for _ in range(3)]
                    for m in range(3):
                        v = []
                        for n in range(3):
                            at = pl.ds(pl.multiple_of((2 * i + half) * PLANE + (m * SLAB + h * 384 + n * 128), 128), 128)
                            low = low_ref[:, at]
                            v.append(jnp.concatenate([bands_ref[:, at], low, low], axis=0))
                        for j in range(3):
                            got = jnp.where(place == j, v[0], jnp.where(place == (j + 1) % 3, v[1], v[2]))
                            got = turn(got, -16 * j)
                            r = jnp.take_along_axis(got, to_right, axis=0)
                            l = jnp.take_along_axis(got, to_left, axis=0)
                            span = slice(m * SLAB + j * 256 + h * 128, m * SLAB + j * 256 + h * 128 + 128)
                            right[x, :, span] = r
                            left[x, :, span] = l
                            f[m][j] = r * l
                    pairs.append(f)
                thirds_h = third_rows(third, h, 8)
                spec = []
                for f in pairs:
                    f = [to_thirds([f[m][j] for m in range(3)], thirds_h, 0) for j in range(3)]
                    spec.append([to_thirds([f[n][k] for n in range(3)], thirds_h, 6) for k in range(3)])
                for k in range(3):
                    for j in range(3):
                        span = slice(k * SLAB + j * 256 + h * 128, k * SLAB + j * 256 + h * 128 + 128)
                        split(hi, lo, rows, span, jnp.concatenate([spec[0][k][j], spec[1][k][j]], axis=0))
            return carry

        lax.fori_loop(0, QX // 2, densities, 0)


def first_kernel(q_ref, own, one, low_a, core_a, third, right, left, hi, lo):
    densities_of(q_ref[0], ((0, own, low_a), (1, one, core_a)), third, right, left, hi, lo)


def spectrum_kernel(q_ref, two, three, low_b, core_b, kern, third, whi, wlo, right_in, left_in, hi_in, lo_in,
                    right, left, hi, lo, field):
    densities_of(q_ref[0], ((2, two, low_b), (3, three, core_b)), third, right, left, hi, lo)
    for k in (0, 1):
        if k == 0:
            rows_of = [[product(hi, lo, whi, wlo, 0, j)] for j in range(3)]
        else:
            both = [(product(hi, lo, whi, wlo, 1, j), product(hi, lo, whi, wlo, 2, j)) for j in range(3)]
            rows_of = [[c - s, c + s] for c, s in both]
        for n in range(len(rows_of[0])):
            a, c, s = (rows_of[j][n] for j in range(3))
            field[:, group(k + n, 0)] = a
            field[:, group(k + n, 1)] = c - s
            field[:, group(k + n, 2)] = c + s

    def along_x(i, carry):
        span = pl.ds(pl.multiple_of(128 * i, 128), 128)
        f = [field[8 * x : 8 * x + 8, span] for x in range(NG)]
        out = convolve_x(f, lambda k: kern[k : k + 1, span])
        for x in range(NG):
            field[8 * x : 8 * x + 8, span] = out[x]
        return carry

    lax.fori_loop(0, PLANE // 128, along_x, 0)


def terms_kernel(q_ref, right, left, field, third, whi, wlo, near0, near2, cross, low0, low2, hi, lo, back):
    q = q_ref[0]

    def unmix(i, carry):
        rows = pl.ds(pl.multiple_of(16 * i, 16), 16)
        mixed = [[field[rows, group(k, j)] for j in range(3)] for k in range(3)]
        mixed = [[a, u + v, v - u] for a, u, v in mixed]
        for j in range(3):
            a, u, v = (mixed[k][j] for k in range(3))
            for k, value in enumerate((a, u + v, v - u)):
                split(hi, lo, rows, group(k, j), value)
        return carry

    lax.fori_loop(0, NG // 2, unmix, 0)
    for k in range(3):
        for j in range(3):
            back[:, group(k, j)] = product(hi, lo, whi, wlo, k, j)

    sub = lax.broadcasted_iota(jnp.int32, (8, 128), 0)
    mine = (sub == q).astype(F32)
    place = lax.broadcasted_iota(jnp.int32, (8, 128), 1) // 16 % 3

    for delta in range(4):
        base = (q ^ delta) * QX

        def finish(i, carry):
            for half in range(X_STEP):
                x = base + X_STEP * i + half
                rows = pl.ds(pl.multiple_of(x * 8, 8), 8)
                for h in range(2):
                    thirds_h = third_rows(third, h, 8)

                    def spot(k, j):
                        return slice(k * SLAB + j * 256 + h * 128, k * SLAB + j * 256 + h * 128 + 128)

                    v = [from_thirds(*(back[rows, spot(k, j)] for j in range(3)), thirds_h, 6) for k in range(3)]
                    v = [from_thirds(*(v[k][j] for k in range(3)), thirds_h, 0) for j in range(3)]
                    for m in range(3):
                        parts = []
                        for j in range(3):
                            pr = v[j][m] * right[x, :, spot(m, j)]
                            pr = pr + swapped(pr, sub, 1)
                            pr = pr + swapped(pr, sub, 2)
                            po = swapped(v[j][m] * left[x, :, spot(m, j)], sub, 4) + mine * pr
                            parts.append(turn(jnp.where(sub < 4, po, pr), 16 * j))
                        for n in range(3):
                            out = jnp.where(place == n, parts[0], jnp.where(place == (n + 1) % 3, parts[1], parts[2]))
                            start = (X_STEP * i + half) * PLANE + (m * SLAB + h * 384 + n * 128)
                            at = pl.ds(pl.multiple_of(start, 128), 128)
                            if delta % 2:
                                cross[delta // 2 * 4 : delta // 2 * 4 + 4, at] = out[0:4, :]
                                cross[8 + delta // 2 : 9 + delta // 2, at] = out[4:5, :]
                            else:
                                (near0, near2)[delta // 2][:, at] = out[0:4, :]
                                (low0, low2)[delta // 2][:, at] = out[4:5, :]
            return carry

        lax.fori_loop(0, QX // X_STEP, finish, 0)


def swapped(value, sub, flip):
    return jnp.take_along_axis(value, sub ^ flip, axis=0)


X_STEP = 6
VMEM_SPEC = pl.BlockSpec(memory_space=pltpu.VMEM)
SMEM_SPEC = pl.BlockSpec(memory_space=pltpu.SMEM)
SPLIT = [pltpu.VMEM((NG * 8, PLANE), BF16)] * 2


STATE = [jax.ShapeDtypeStruct((NG, 8, PLANE), F32)] * 2 + [jax.ShapeDtypeStruct((NG * 8, PLANE), BF16)] * 2


def first_densities(q, bands, third):
    return pl.pallas_call(
        first_kernel,
        out_shape=STATE,
        in_specs=[SMEM_SPEC] + [VMEM_SPEC] * 5,
        out_specs=[VMEM_SPEC] * 4,
        name="first_densities",
        compiler_params=pltpu.CompilerParams(vmem_limit_bytes=16 << 20),
    )(q.reshape(1), *bands, third)


def spectrum(q, bands, kern, third, tables, state):
    return pl.pallas_call(
        spectrum_kernel,
        out_shape=STATE + [jax.ShapeDtypeStruct((NG * 8, PLANE), F32)],
        in_specs=[SMEM_SPEC] + [VMEM_SPEC] * 12,
        out_specs=[VMEM_SPEC] * 5,
        input_output_aliases={9: 0, 10: 1, 11: 2, 12: 3},
        name="spectrum",
        compiler_params=pltpu.CompilerParams(vmem_limit_bytes=28 << 20),
    )(q.reshape(1), *bands, kern, third, *tables, *state)


def terms(q, right, left, field, third, tables):
    return pl.pallas_call(
        terms_kernel,
        out_shape=[jax.ShapeDtypeStruct(shape, F32) for shape in [(4, QCELL)] * 2 + [(10, QCELL)] + [(1, QCELL)] * 2],
        in_specs=[SMEM_SPEC] + [VMEM_SPEC] * 6,
        out_specs=[VMEM_SPEC] * 5,
        scratch_shapes=SPLIT + [pltpu.VMEM((NG * 8, PLANE), F32)],
        name="terms",
        compiler_params=pltpu.CompilerParams(vmem_limit_bytes=28 << 20),
    )(q.reshape(1), right, left, field, third, *tables)


BOTH = ("band", "grid")
CHUNK = QCELL // 4


def small_call(body, outs, scratch=(), limit=8):
    vmem = pl.BlockSpec(memory_space=pltpu.VMEM)

    def call(where, *arrays):
        return pl.pallas_call(
            body,
            out_shape=[jax.ShapeDtypeStruct(shape, F32) for shape in outs],
            in_specs=[pl.BlockSpec(memory_space=pltpu.SMEM)] + [vmem] * len(arrays),
            out_specs=[vmem] * len(outs),
            scratch_shapes=list(scratch),
            compiler_params=pltpu.CompilerParams(vmem_limit_bytes=limit << 20),
        )(where, *arrays)

    return call


def chunk_of(where, k):
    return pl.ds(pl.multiple_of((where[2] ^ k) * CHUNK, 128), CHUNK)


def rows_kernel(where, orbitals, sel_a, sel_b):
    lower = where[0] < 2
    a, b = orbitals[0:2, :], orbitals[2:4, :]
    sel_a[...] = jnp.where(lower, a, b)
    sel_b[...] = jnp.where(lower, b, a)


def chunks_kernel(where, orbitals, copy, *chunks):
    copy[...] = orbitals[...]
    for k in range(4):
        chunks[k][...] = orbitals[:, chunk_of(where, k)]


def merge_kernel(where, near0, near2, low0, low2, across, near, far, owed_a, owed_b):
    first = where[0] % 2 == 0
    near[...] = near0[...] + across[0:4, :]
    far[...] = near2[...] + across[4:8, :]
    for out, low, row in ((owed_a, low0, 8), (owed_b, low2, 9)):
        a, b = low[...], across[row : row + 1, :]
        out[0:1, :] = jnp.where(first, a, b)
        out[1:2, :] = jnp.where(first, b, a)


def total_of(where, near, far, owed_a, owed_b, span):
    lower = where[0] < 2
    a, b = owed_a[:, span], owed_b[:, span]
    owed = jnp.concatenate([jnp.where(lower, a, b), jnp.where(lower, b, a)], axis=0)
    return -(near[:, span] + far[:, span] + owed)


def finalize_kernel(where, near, far, owed_a, owed_b, *chunks):
    for k in (1, 2, 3, 0):
        chunks[k][...] = total_of(where, near, far, owed_a, owed_b, chunk_of(where, k))


def vectors_kernel(where, near, far, owed_a, owed_b, vectors):
    for c in range(4):
        span = pl.ds(c * CHUNK, CHUNK)
        vectors[:, span] = total_of(where, near, far, owed_a, owed_b, span)


def margin_kernel(where, own0, oth0, own1, oth1, own2, oth2, own3, oth3, v0, v1, v2, v3, pieces, block):
    z, y, h = where[1], where[2], where[3]

    def halves(a):
        top = a.astype(BF16)
        return top, (a - top.astype(F32)).astype(BF16)

    v = jnp.concatenate(halves(jnp.concatenate([v0[...], v1[...], v2[...], v3[...]], axis=0)), axis=0)
    parts = jnp.concatenate([r[...] for r in (own0, oth0, own1, oth1, own2, oth2, own3, oth3)], axis=0)
    f = jnp.concatenate(halves(parts), axis=0)
    both = lax.dot_general(f, v, (((1,), (1,)), ((), ())), preferred_element_type=F32)
    both = both[0:128, :] + both[128:256, :]
    got = both[:, 0:16] + both[:, 16:32]
    for dz in range(4):
        for dy in range(4):
            row = 32 * dz + 4 * dy
            pair = got[row : row + 4, :], got[row + 16 : row + 20, :]
            at = (z + 4 - dz) % 4 * 4 + (y ^ dy)
            block[at, 0:4, :] = jnp.where(h == 0, pair[0], pair[1])
            block[at, 4:8, :] = jnp.where(h == 0, pair[1], pair[0])
    out = block[...].reshape(128, 16).T * (1.0 / NCELL)
    turned = [out] + [pltpu.roll(out, 32 * r, 1) for r in (1, 2, 3)]
    third_of = lax.broadcasted_iota(jnp.int32, (16, 128), 1) // 32
    keep = third_of == lax.broadcasted_iota(jnp.int32, (16, 128), 0) % 4
    for q_to in range(4):
        picked = turned[(3 - q_to) % 4]
        for j in range(3):
            picked = jnp.where(third_of == j, turned[(j - q_to) % 4], picked)
        picked = jnp.where(keep, picked, 0.0)
        for dy in range(4):
            row = jnp.sum(picked[4 * dy : 4 * dy + 4, :], axis=0, keepdims=True)
            pieces[pl.ds((y ^ dy) * 4 + q_to, 1), :] = row


def move(value, target):
    nb, nq = lax.axis_size("band"), lax.axis_size("grid")
    pairs = []
    for b in range(nb):
        for q in range(nq):
            z, y, h, q_to = target(b // 8, b // 2 % 4, b % 2, q)
            pairs.append((b * nq + q, ((z % 4) * 8 + (y % 4) * 2 + h) * nq + q_to))
    return lax.ppermute(value, BOTH, pairs)


def along_y(value, flip):
    return move(value, lambda z, y, h, q: (z, y ^ flip, h, q))


def along_z(value, k):
    return move(value, lambda z, y, h, q: (z + k, y, h, q))


def within(value, flip):
    return move(value, lambda z, y, h, q: (z, y, h, q ^ flip))


def around(value, blocks, flip):
    def target(z, y, h, q):
        b = (z * 8 + y * 2 + h + blocks) % 32
        return b // 8, b // 2 % 4, b % 2, q ^ flip

    return move(value, target)


def step(orbitals):
    b = lax.axis_index("band").astype(jnp.int32)
    q = lax.axis_index("grid").astype(jnp.int32)
    where = jnp.stack([q, b // 8, b // 2 % 4, b % 2])
    rows = small_call(rows_kernel, [(2, QCELL)] * 2)
    sel_a, sel_b = rows(where, orbitals)
    low_a = around(sel_a, 1, 0)
    low_b = around(sel_b, 1, 2)
    two = within(orbitals, 2)
    one = within(orbitals, 1)
    chunks = small_call(chunks_kernel, [(4, QCELL)] + [(4, CHUNK)] * 4)
    own, *pc = chunks(where, orbitals)
    pieces = [pc[0]] + [along_y(pc[k], k) for k in (1, 2, 3)]
    *tables, kern, third = plane_tables()
    together = jnp.concatenate(pieces, axis=0)
    core_a = within(low_a, 1)
    core_b = within(low_b, 1)
    three = within(two, 1)
    other = move(together, lambda z, y, h, q: (z, y, 1 - h, q))
    own1 = along_z(together, 1)
    own3 = along_z(together, 3)
    state = first_densities(q, (own, one, low_a, core_a), third)
    right, left, _, _, field = spectrum(q, (two, three, low_b, core_b), kern, third, tables[:2], state)
    near0, near2, cross, low0, low2 = terms(q, right, left, field, third, tables[2:4])
    across = within(cross, 1)
    other, _ = lax.optimization_barrier((other, near0))
    oth1 = along_z(other, 1)
    oth3 = along_z(other, 3)
    own2 = along_z(own1, 1)
    merge = small_call(merge_kernel, [(4, QCELL)] * 2 + [(2, QCELL)] * 2)
    near, both, owe_a, owe_b = merge(where, near0, near2, low0, low2, across)
    far = within(both, 2)
    owed_a = around(owe_a, -1, 0)
    owed_b = around(owe_b, -1, 2)
    oth2 = along_z(oth1, 1)
    finalize = small_call(finalize_kernel, [(4, CHUNK)] * 4)
    vc = finalize(where, near, far, owed_a, owed_b)
    (vectors,) = small_call(vectors_kernel, [(4, QCELL)])(where, near, far, owed_a, owed_b)
    given = [vc[0]] + [along_y(vc[k], k) for k in (1, 2, 3)]
    margin_part = small_call(margin_kernel, [(16, 128)], [pltpu.VMEM((16, 8, 16), F32)], 20)
    (sums,) = margin_part(where, together, other, own1, oth1, own2, oth2, own3, oth3, *given)
    groups = [[(z * 8 + y * 2 + h) * 4 + p for y in range(4) for p in range(4)] for z in range(4) for h in range(2)]
    sums = lax.all_to_all(sums, BOTH, 0, 0, tiled=True, axis_index_groups=groups)
    margin = jnp.sum(sums, axis=0).reshape(4, 32).T
    return vectors, margin


def solution(mesh):
    return jax.shard_map(
        step,
        mesh=mesh,
        in_specs=(P("band", "grid"),),
        out_specs=(P("band", "grid"), P("grid", "band")),
        check_vma=False,
    )
```

```python
import math

import jax
import jax.numpy as jnp
import numpy as np
from jax import lax
from jax.experimental import pallas as pl
from jax.experimental.pallas import tpu as pltpu
from jax.sharding import PartitionSpec as P

NG = 48
NCELL = 110592
PLANE = NG * NG
SLAB = 768
QX = 12
QCELL = QX * PLANE
F32 = jnp.float32
BF16 = jnp.bfloat16
R2 = math.sqrt(0.5)
C1 = math.cos(math.pi / 8)
C3 = math.cos(3 * math.pi / 8)
S3 = math.sqrt(3.0) / 2

ORDER = [("C", b) for b in range(9)] + [("S", b) for b in range(1, 8)]
SWAPPED = [("C", 0)] + [("S", b) for b in range(1, 8)] + [("C", 8)] + [("C", b) for b in range(1, 8)]


def sixteen(order):
    u = np.arange(16)
    cols = []
    for kind, b in order:
        col = np.cos(2 * np.pi * b * u / 16) if kind == "C" else np.sin(2 * np.pi * b * u / 16)
        cols.append(col / np.linalg.norm(col))
    return np.stack(cols, 1)


def folded(g):
    return (g + 24) % 48 - 24


def x_basis():
    keys, freqs, norms = [], [], []
    for b in range(9):
        keys.append(("A", "C", b)); freqs.append(3 * b); norms.append(48 if b in (0, 8) else 24)
    for b in range(1, 8):
        keys.append(("A", "S", b)); freqs.append(3 * b); norms.append(24)
    for b in (0, 8):
        for t in "cs":
            keys.append((t, "C", b)); freqs.append(16 + 3 * b); norms.append(24)
    for b in range(1, 8):
        for sign in (1, -1):
            for kind in ("cos", "sin"):
                keys.append((kind, sign, b)); freqs.append(16 + 3 * sign * b); norms.append(24)
    return keys, np.array(freqs), np.array(norms)


def lane_freqs(group):
    out = []
    for kind, b in ORDER:
        if group == "A":
            out.append(3 * b)
        elif b in (0, 8):
            out.append(16 + 3 * b)
        else:
            out.append(16 + 3 * b if (group == "u") == (kind == "C") else 16 - 3 * b)
    return np.array(out)


def kernel_values():
    _, gx, nx = x_basis()
    g = np.stack([lane_freqs(group) for group in "Auv"])
    gy, gz = g[:, None, :, None], g[None, :, None, :]
    q = folded(gx)[:, None, None, None, None] ** 2 + (folded(gy) ** 2 + folded(gz) ** 2)[None]
    q = q.astype(np.float64)
    kern = np.where(q > 0, 40.0 * (1.0 - np.exp(-q / 16.0)) / np.where(q > 0, q, 1.0), 0.0)
    return (kern / (9.0 * nx[:, None, None, None, None])).reshape(NG, PLANE).astype(np.float32)


PLACES = np.array([0, 3, 6, 1, 4, 7, 2, 5])
LANE_Y = np.repeat(np.concatenate([PLACES, 8 + PLACES]), 16)
LANE_Z = np.tile(np.arange(16), 16)


def thirds():
    rows = []
    for lane in (LANE_Y, LANE_Z):
        rows += [np.cos(2 * np.pi * (m + lane) / 3) for m in range(3)]
        rows += [np.sin(2 * np.pi * (m + lane) / 3) for m in range(3)]
    return np.concatenate([np.stack(rows), np.zeros((4, 256))]).astype(np.float32)


def factor_tables():
    bases = sixteen(ORDER), sixteen(SWAPPED)
    slow = [np.repeat(t[LANE_Y[::16]], 16, 1) for t in bases] + [t.T[:, LANE_Y] for t in bases]
    fast = [np.tile(t, (1, 16)) for t in bases] + [np.tile(t.T, (1, 16)) for t in bases]
    return np.stack(slow).astype(np.float32), np.stack(fast).astype(np.float32)


def tables_kernel(slow, fast, kern_in, third_in, hi_there, lo_there, hi_back, lo_back, kern, third):
    kern[...] = kern_in[...]
    third[...] = third_in[...]
    for way, (hi, lo) in enumerate(((hi_there, lo_there), (hi_back, lo_back))):
        for k in range(4):
            for u in range(16):
                w = fast[2 * way + k % 2] * slow[2 * way + k // 2, u : u + 1, :]
                top = w.astype(BF16)
                hi[k, 16 * u : 16 * u + 16, :] = top
                lo[k, 16 * u : 16 * u + 16, :] = (w - top.astype(F32)).astype(BF16)


def plane_tables():
    out = [jax.ShapeDtypeStruct((4, 256, 256), BF16)] * 4
    out += [jax.ShapeDtypeStruct((NG, PLANE), F32), jax.ShapeDtypeStruct((16, 256), F32)]
    return pl.pallas_call(
        tables_kernel, out_shape=out, name="plane_tables",
        compiler_params=pltpu.CompilerParams(vmem_limit_bytes=8 << 20),
    )(*[jnp.asarray(a) for a in (*factor_tables(), kernel_values(), thirds())])


def t16(f):
    o = [f[u] - f[u + 8] for u in range(8)]
    e = [f[u] + f[u + 8] for u in range(8)]
    ee = [e[u] + e[u + 4] for u in range(4)]
    eo = [e[u] - e[u + 4] for u in range(4)]
    c, s = {}, {}
    p0, p1 = ee[0] + ee[2], ee[1] + ee[3]
    c[0], c[8], c[4], s[4] = p0 + p1, p0 - p1, ee[0] - ee[2], ee[1] - ee[3]
    d, a = R2 * (eo[1] - eo[3]), R2 * (eo[1] + eo[3])
    c[2], c[6], s[2], s[6] = eo[0] + d, eo[0] - d, a + eo[2], a - eo[2]
    d1, d2, d3 = (o[u] - o[8 - u] for u in (1, 2, 3))
    s1, s2, s3 = (o[u] + o[8 - u] for u in (1, 2, 3))
    d2, s2 = R2 * d2, R2 * s2
    e1, e3 = o[0] + d2, o[0] - d2
    o1, o3 = C1 * d1 + C3 * d3, C3 * d1 - C1 * d3
    c[1], c[7], c[3], c[5] = e1 + o1, e1 - o1, e3 + o3, e3 - o3
    x1, x3 = o[4] + s2, o[4] - s2
    y1, y3 = C3 * s1 + C1 * s3, C1 * s1 - C3 * s3
    s[1], s[7], s[3], s[5] = y1 + x1, y1 - x1, y3 - x3, y3 + x3
    return c, s


def t16_back(c, s):
    e1, o1, e3, o3 = c[1] + c[7], c[1] - c[7], c[3] + c[5], c[3] - c[5]
    o0, d2 = e1 + e3, R2 * (e1 - e3)
    d1, d3 = C1 * o1 + C3 * o3, C3 * o1 - C1 * o3
    y1, x1, y3, x3 = s[1] + s[7], s[1] - s[7], s[3] + s[5], s[5] - s[3]
    o4, s2 = x1 + x3, R2 * (x1 - x3)
    s1, s3 = C3 * y1 + C1 * y3, C1 * y1 - C3 * y3
    o = [o0, d1 + s1, d2 + s2, d3 + s3, o4, s3 - d3, s2 - d2, s1 - d1]
    d, a = R2 * (c[2] - c[6]), R2 * (s[2] + s[6])
    eo = [c[2] + c[6], d + a, s[2] - s[6], a - d]
    p0, p1 = c[0] + c[8], c[0] - c[8]
    ee = [p0 + c[4], p1 + s[4], p0 - c[4], p1 - s[4]]
    e = [ee[u] + eo[u] for u in range(4)] + [ee[u] - eo[u] for u in range(4)]
    return [e[u] + o[u] for u in range(8)] + [e[u] - o[u] for u in range(8)]


def convolve_x(f, table):
    keys, _, _ = x_basis()
    row = {key: k for k, key in enumerate(keys)}
    place = {(x % 3, x % 16): x for x in range(NG)}
    part = {"A": [], "c": [], "s": []}
    for u in range(16):
        f0, f1, f2 = (f[place[t, u]] for t in range(3))
        a = f1 + f2
        part["A"].append(f0 + a)
        part["c"].append(f0 - 0.5 * a)
        part["s"].append(S3 * (f1 - f2))
    c, s = t16(part["A"])
    c = {b: v * table(row["A", "C", b]) for b, v in c.items()}
    s = {b: v * table(row["A", "S", b]) for b, v in s.items()}
    back_a = t16_back(c, s)
    cc, cs = t16(part["c"])
    sc, ss = t16(part["s"])
    for b in (0, 8):
        cc[b] = cc[b] * table(row["c", "C", b])
        sc[b] = sc[b] * table(row["s", "C", b])
    for b in range(1, 8):
        p = (cc[b] - ss[b]) * table(row["cos", 1, b])
        m = (cc[b] + ss[b]) * table(row["cos", -1, b])
        cc[b], ss[b] = p + m, m - p
        p = (sc[b] + cs[b]) * table(row["sin", 1, b])
        m = (sc[b] - cs[b]) * table(row["sin", -1, b])
        sc[b], cs[b] = p + m, p - m
    back_c, back_s = t16_back(cc, cs), t16_back(sc, ss)
    out = [None] * NG
    for u in range(16):
        a, c_, s_ = back_a[u], back_c[u], S3 * back_s[u]
        h = a - 0.5 * c_
        out[place[0, u]] = a + c_
        out[place[1, u]] = h + s_
        out[place[2, u]] = h - s_
    return out


def group(k, j):
    return slice(k * SLAB + j * 256, k * SLAB + j * 256 + 256)


def split(hi, lo, rows, span, value):
    top = value.astype(BF16)
    hi[rows, span] = top
    lo[rows, span] = (value - top.astype(F32)).astype(BF16)


def product(hi, lo, whi, wlo, k, j):
    span = group(k, j)
    a, b = hi[:, span], lo[:, span]
    w = (k // 2) * 2 + j // 2
    lhs = jnp.concatenate([a, b, a], axis=1)
    rhs = jnp.concatenate([whi[w], whi[w], wlo[w]], axis=0)
    return jnp.dot(lhs, rhs, preferred_element_type=F32)


def turn(value, lanes):
    return pltpu.roll(value, lanes % 128, 1) if lanes % 128 else value


def to_thirds(f, third, first):
    c, s = third[first : first + 3], third[first + 3 : first + 6]
    return (
        f[0] + f[1] + f[2],
        f[0] * c[0] + f[1] * c[1] + f[2] * c[2],
        f[0] * s[0] + f[1] * s[1] + f[2] * s[2],
    )


def third_rows(third, h, rows):
    lanes = slice(128 * h, 128 * h + 128)
    return [jnp.broadcast_to(third[k : k + 1, lanes], (rows, 128)) for k in range(12)]


def from_thirds(a, c, s, third, first):
    return [a + c * third[first + m] + s * third[first + 3 + m] for m in range(3)]


def densities_of(q, sources, third, right, left, hi, lo):
    sub = lax.broadcasted_iota(jnp.int32, (8, 128), 0)
    to_right = sub % 4
    to_left = jnp.where(sub < 4, q, 4 + q % 2)
    place = lax.broadcasted_iota(jnp.int32, (8, 128), 1) // 16 % 3
    for delta, bands_ref, low_ref in sources:
        base = (q ^ delta) * QX

        def densities(i, carry):
            rows = pl.ds(pl.multiple_of(8 * base + 16 * i, 16), 16)
            for h in range(2):
                pairs = []
                for half in range(2):
                    x = base + 2 * i + half
                    f = [[None] * 3 for _ in range(3)]
                    for m in range(3):
                        v = []
                        for n in range(3):
                            at = pl.ds(pl.multiple_of((2 * i + half) * PLANE + (m * SLAB + h * 384 + n * 128), 128), 128)
                            low = low_ref[:, at]
                            v.append(jnp.concatenate([bands_ref[:, at], low, low], axis=0))
                        for j in range(3):
                            got = jnp.where(place == j, v[0], jnp.where(place == (j + 1) % 3, v[1], v[2]))
                            got = turn(got, -16 * j)
                            r = jnp.take_along_axis(got, to_right, axis=0)
                            l = jnp.take_along_axis(got, to_left, axis=0)
                            span = slice(m * SLAB + j * 256 + h * 128, m * SLAB + j * 256 + h * 128 + 128)
                            right[x, :, span] = r
                            left[x, :, span] = l
                            f[m][j] = r * l
                    pairs.append(f)
                thirds_h = third_rows(third, h, 8)
                spec = []
                for f in pairs:
                    f = [to_thirds([f[m][j] for m in range(3)], thirds_h, 0) for j in range(3)]
                    spec.append([to_thirds([f[n][k] for n in range(3)], thirds_h, 6) for k in range(3)])
                for k in range(3):
                    for j in range(3):
                        span = slice(k * SLAB + j * 256 + h * 128, k * SLAB + j * 256 + h * 128 + 128)
                        split(hi, lo, rows, span, jnp.concatenate([spec[0][k][j], spec[1][k][j]], axis=0))
            return carry

        lax.fori_loop(0, QX // 2, densities, 0)


def first_kernel(q_ref, own, one, low_a, core_a, third, right, left, hi, lo):
    densities_of(q_ref[0], ((0, own, low_a), (1, one, core_a)), third, right, left, hi, lo)


def spectrum_kernel(q_ref, two, three, low_b, core_b, kern, third, whi, wlo, right_in, left_in, hi_in, lo_in,
                    right, left, hi, lo, field):
    densities_of(q_ref[0], ((2, two, low_b), (3, three, core_b)), third, right, left, hi, lo)
    for k in (0, 1):
        if k == 0:
            rows_of = [[product(hi, lo, whi, wlo, 0, j)] for j in range(3)]
        else:
            both = [(product(hi, lo, whi, wlo, 1, j), product(hi, lo, whi, wlo, 2, j)) for j in range(3)]
            rows_of = [[c - s, c + s] for c, s in both]
        for n in range(len(rows_of[0])):
            a, c, s = (rows_of[j][n] for j in range(3))
            field[:, group(k + n, 0)] = a
            field[:, group(k + n, 1)] = c - s
            field[:, group(k + n, 2)] = c + s

    def along_x(i, carry):
        span = pl.ds(pl.multiple_of(128 * i, 128), 128)
        f = [field[8 * x : 8 * x + 8, span] for x in range(NG)]
        out = convolve_x(f, lambda k: kern[k : k + 1, span])
        for x in range(NG):
            field[8 * x : 8 * x + 8, span] = out[x]
        return carry

    lax.fori_loop(0, PLANE // 128, along_x, 0)


def terms_kernel(q_ref, right, left, field, third, whi, wlo, near0, near2, cross, low0, low2, hi, lo, back):
    q = q_ref[0]

    def unmix(i, carry):
        rows = pl.ds(pl.multiple_of(16 * i, 16), 16)
        mixed = [[field[rows, group(k, j)] for j in range(3)] for k in range(3)]
        mixed = [[a, u + v, v - u] for a, u, v in mixed]
        for j in range(3):
            a, u, v = (mixed[k][j] for k in range(3))
            for k, value in enumerate((a, u + v, v - u)):
                split(hi, lo, rows, group(k, j), value)
        return carry

    lax.fori_loop(0, NG // 2, unmix, 0)
    for k in range(3):
        for j in range(3):
            back[:, group(k, j)] = product(hi, lo, whi, wlo, k, j)

    sub = lax.broadcasted_iota(jnp.int32, (8, 128), 0)
    mine = (sub == q).astype(F32)
    place = lax.broadcasted_iota(jnp.int32, (8, 128), 1) // 16 % 3

    for delta in range(4):
        base = (q ^ delta) * QX

        def finish(i, carry):
            for half in range(X_STEP):
                x = base + X_STEP * i + half
                rows = pl.ds(pl.multiple_of(x * 8, 8), 8)
                for h in range(2):
                    thirds_h = third_rows(third, h, 8)

                    def spot(k, j):
                        return slice(k * SLAB + j * 256 + h * 128, k * SLAB + j * 256 + h * 128 + 128)

                    v = [from_thirds(*(back[rows, spot(k, j)] for j in range(3)), thirds_h, 6) for k in range(3)]
                    v = [from_thirds(*(v[k][j] for k in range(3)), thirds_h, 0) for j in range(3)]
                    for m in range(3):
                        parts = []
                        for j in range(3):
                            pr = v[j][m] * right[x, :, spot(m, j)]
                            pr = pr + swapped(pr, sub, 1)
                            pr = pr + swapped(pr, sub, 2)
                            po = swapped(v[j][m] * left[x, :, spot(m, j)], sub, 4) + mine * pr
                            parts.append(turn(jnp.where(sub < 4, po, pr), 16 * j))
                        for n in range(3):
                            out = jnp.where(place == n, parts[0], jnp.where(place == (n + 1) % 3, parts[1], parts[2]))
                            start = (X_STEP * i + half) * PLANE + (m * SLAB + h * 384 + n * 128)
                            at = pl.ds(pl.multiple_of(start, 128), 128)
                            if delta % 2:
                                cross[delta // 2 * 4 : delta // 2 * 4 + 4, at] = out[0:4, :]
                                cross[8 + delta // 2 : 9 + delta // 2, at] = out[4:5, :]
                            else:
                                (near0, near2)[delta // 2][:, at] = out[0:4, :]
                                (low0, low2)[delta // 2][:, at] = out[4:5, :]
            return carry

        lax.fori_loop(0, QX // X_STEP, finish, 0)


def swapped(value, sub, flip):
    return jnp.take_along_axis(value, sub ^ flip, axis=0)


X_STEP = 6
VMEM_SPEC = pl.BlockSpec(memory_space=pltpu.VMEM)
SMEM_SPEC = pl.BlockSpec(memory_space=pltpu.SMEM)
SPLIT = [pltpu.VMEM((NG * 8, PLANE), BF16)] * 2


STATE = [jax.ShapeDtypeStruct((NG, 8, PLANE), F32)] * 2 + [jax.ShapeDtypeStruct((NG * 8, PLANE), BF16)] * 2


def first_densities(q, bands, third):
    return pl.pallas_call(
        first_kernel,
        out_shape=STATE,
        in_specs=[SMEM_SPEC] + [VMEM_SPEC] * 5,
        out_specs=[VMEM_SPEC] * 4,
        name="first_densities",
        compiler_params=pltpu.CompilerParams(vmem_limit_bytes=16 << 20),
    )(q.reshape(1), *bands, third)


def spectrum(q, bands, kern, third, tables, state):
    return pl.pallas_call(
        spectrum_kernel,
        out_shape=STATE + [jax.ShapeDtypeStruct((NG * 8, PLANE), F32)],
        in_specs=[SMEM_SPEC] + [VMEM_SPEC] * 12,
        out_specs=[VMEM_SPEC] * 5,
        input_output_aliases={9: 0, 10: 1, 11: 2, 12: 3},
        name="spectrum",
        compiler_params=pltpu.CompilerParams(vmem_limit_bytes=28 << 20),
    )(q.reshape(1), *bands, kern, third, *tables, *state)


def terms(q, right, left, field, third, tables):
    return pl.pallas_call(
        terms_kernel,
        out_shape=[jax.ShapeDtypeStruct(shape, F32) for shape in [(4, QCELL)] * 2 + [(10, QCELL)] + [(1, QCELL)] * 2],
        in_specs=[SMEM_SPEC] + [VMEM_SPEC] * 6,
        out_specs=[VMEM_SPEC] * 5,
        scratch_shapes=SPLIT + [pltpu.VMEM((NG * 8, PLANE), F32)],
        name="terms",
        compiler_params=pltpu.CompilerParams(vmem_limit_bytes=28 << 20),
    )(q.reshape(1), right, left, field, third, *tables)


BOTH = ("band", "grid")
CHUNK = QCELL // 4


def small_call(body, outs, scratch=(), limit=8):
    vmem = pl.BlockSpec(memory_space=pltpu.VMEM)

    def call(where, *arrays):
        return pl.pallas_call(
            body,
            out_shape=[jax.ShapeDtypeStruct(shape, F32) for shape in outs],
            in_specs=[pl.BlockSpec(memory_space=pltpu.SMEM)] + [vmem] * len(arrays),
            out_specs=[vmem] * len(outs),
            scratch_shapes=list(scratch),
            compiler_params=pltpu.CompilerParams(vmem_limit_bytes=limit << 20),
        )(where, *arrays)

    return call


def chunk_of(where, k):
    return pl.ds(pl.multiple_of((where[2] ^ k) * CHUNK, 128), CHUNK)


def rows_kernel(where, orbitals, sel_a, sel_b):
    lower = where[0] < 2
    a, b = orbitals[0:2, :], orbitals[2:4, :]
    sel_a[...] = jnp.where(lower, a, b)
    sel_b[...] = jnp.where(lower, b, a)


def chunks_kernel(where, orbitals, copy, *chunks):
    copy[...] = orbitals[...]
    for k in range(4):
        chunks[k][...] = orbitals[:, chunk_of(where, k)]


def merge_kernel(where, near0, near2, low0, low2, across, near, far, owed_a, owed_b):
    first = where[0] % 2 == 0
    near[...] = near0[...] + across[0:4, :]
    far[...] = near2[...] + across[4:8, :]
    for out, low, row in ((owed_a, low0, 8), (owed_b, low2, 9)):
        a, b = low[...], across[row : row + 1, :]
        out[0:1, :] = jnp.where(first, a, b)
        out[1:2, :] = jnp.where(first, b, a)


def total_of(where, near, far, owed_a, owed_b, span):
    lower = where[0] < 2
    a, b = owed_a[:, span], owed_b[:, span]
    owed = jnp.concatenate([jnp.where(lower, a, b), jnp.where(lower, b, a)], axis=0)
    return -(near[:, span] + far[:, span] + owed)


def finalize_kernel(where, near, far, owed_a, owed_b, *chunks):
    for k in (1, 2, 3, 0):
        chunks[k][...] = total_of(where, near, far, owed_a, owed_b, chunk_of(where, k))


def vectors_kernel(where, near, far, owed_a, owed_b, vectors):
    for c in range(4):
        span = pl.ds(c * CHUNK, CHUNK)
        vectors[:, span] = total_of(where, near, far, owed_a, owed_b, span)


def margin_kernel(where, own0, oth0, own1, oth1, own2, oth2a, oth2b, own3, oth3, v0, v1, v2, v3, pieces, block):
    z, y, h = where[1], where[2], where[3]

    def halves(a):
        top = a.astype(BF16)
        return top, (a - top.astype(F32)).astype(BF16)

    v = jnp.concatenate(halves(jnp.concatenate([v0[...], v1[...], v2[...], v3[...]], axis=0)), axis=0)
    parts = jnp.concatenate([r[...] for r in (own0, oth0, own1, oth1, own2, oth2a, oth2b, own3, oth3)], axis=0)
    f = jnp.concatenate(halves(parts), axis=0)
    both = lax.dot_general(f, v, (((1,), (1,)), ((), ())), preferred_element_type=F32)
    both = both[0:128, :] + both[128:256, :]
    got = both[:, 0:16] + both[:, 16:32]
    for dz in range(4):
        for dy in range(4):
            row = 32 * dz + 4 * dy
            pair = got[row : row + 4, :], got[row + 16 : row + 20, :]
            at = (z + 4 - dz) % 4 * 4 + (y ^ dy)
            block[at, 0:4, :] = jnp.where(h == 0, pair[0], pair[1])
            block[at, 4:8, :] = jnp.where(h == 0, pair[1], pair[0])
    out = block[...].reshape(128, 16).T * (1.0 / NCELL)
    turned = [out] + [pltpu.roll(out, 32 * r, 1) for r in (1, 2, 3)]
    third_of = lax.broadcasted_iota(jnp.int32, (16, 128), 1) // 32
    keep = third_of == lax.broadcasted_iota(jnp.int32, (16, 128), 0) % 4
    for q_to in range(4):
        picked = turned[(3 - q_to) % 4]
        for j in range(3):
            picked = jnp.where(third_of == j, turned[(j - q_to) % 4], picked)
        picked = jnp.where(keep, picked, 0.0)
        for dy in range(4):
            row = jnp.sum(picked[4 * dy : 4 * dy + 4, :], axis=0, keepdims=True)
            pieces[pl.ds((y ^ dy) * 4 + q_to, 1), :] = row


def move(value, target):
    nb, nq = lax.axis_size("band"), lax.axis_size("grid")
    pairs = []
    for b in range(nb):
        for q in range(nq):
            z, y, h, q_to = target(b // 8, b // 2 % 4, b % 2, q)
            pairs.append((b * nq + q, ((z % 4) * 8 + (y % 4) * 2 + h) * nq + q_to))
    return lax.ppermute(value, BOTH, pairs)


def along_y(value, flip):
    return move(value, lambda z, y, h, q: (z, y ^ flip, h, q))


def along_z(value, k):
    return move(value, lambda z, y, h, q: (z + k, y, h, q))


def within(value, flip):
    return move(value, lambda z, y, h, q: (z, y, h, q ^ flip))


def around(value, blocks, flip):
    def target(z, y, h, q):
        b = (z * 8 + y * 2 + h + blocks) % 32
        return b // 8, b // 2 % 4, b % 2, q ^ flip

    return move(value, target)


def step(orbitals):
    b = lax.axis_index("band").astype(jnp.int32)
    q = lax.axis_index("grid").astype(jnp.int32)
    where = jnp.stack([q, b // 8, b // 2 % 4, b % 2])
    rows = small_call(rows_kernel, [(2, QCELL)] * 2)
    sel_a, sel_b = rows(where, orbitals)
    low_a = around(sel_a, 1, 0)
    low_b = around(sel_b, 1, 2)
    two = within(orbitals, 2)
    one = within(orbitals, 1)
    chunks = small_call(chunks_kernel, [(4, QCELL)] + [(4, CHUNK)] * 4)
    own, *pc = chunks(where, orbitals)
    pieces = [pc[0]] + [along_y(pc[k], k) for k in (1, 2, 3)]
    *tables, kern, third = plane_tables()
    together = jnp.concatenate(pieces, axis=0)
    core_a = within(low_a, 1)
    core_b = within(low_b, 1)
    three = within(two, 1)
    other = move(together, lambda z, y, h, q: (z, y, 1 - h, q))
    own1 = along_z(together, 1)
    own3 = along_z(together, 3)
    state = first_densities(q, (own, one, low_a, core_a), third)
    right, left, _, _, field = spectrum(q, (two, three, low_b, core_b), kern, third, tables[:2], state)
    near0, near2, cross, low0, low2 = terms(q, right, left, field, third, tables[2:4])
    across = within(cross, 1)
    other, _ = lax.optimization_barrier((other, near0))
    oth1 = along_z(other, 1)
    oth3 = along_z(other, 3)
    merge = small_call(merge_kernel, [(4, QCELL)] * 2 + [(2, QCELL)] * 2)
    near, both, owe_a, owe_b = merge(where, near0, near2, low0, low2, across)
    far = within(both, 2)
    owed_a = around(owe_a, -1, 0)
    owed_b = around(owe_b, -1, 2)
    own2 = along_z(own1, 1)
    oth2 = [along_z(oth1[:8], 1), along_z(oth3[8:], 3)]
    finalize = small_call(finalize_kernel, [(4, CHUNK)] * 4)
    vc = finalize(where, near, far, owed_a, owed_b)
    (vectors,) = small_call(vectors_kernel, [(4, QCELL)])(where, near, far, owed_a, owed_b)
    given = [vc[0]] + [along_y(vc[k], k) for k in (1, 2, 3)]
    margin_part = small_call(margin_kernel, [(16, 128)], [pltpu.VMEM((16, 8, 16), F32)], 20)
    (sums,) = margin_part(where, together, other, own1, oth1, own2, *oth2, own3, oth3, *given)
    groups = [[(z * 8 + y * 2 + h) * 4 + p for y in range(4) for p in range(4)] for z in range(4) for h in range(2)]
    sums = lax.all_to_all(sums, BOTH, 0, 0, tiled=True, axis_index_groups=groups)
    margin = jnp.sum(sums, axis=0).reshape(4, 32).T
    return vectors, margin


def solution(mesh):
    return jax.shard_map(
        step,
        mesh=mesh,
        in_specs=(P("band", "grid"),),
        out_specs=(P("band", "grid"), P("grid", "band")),
        check_vma=False,
    )
```

```python
import math

import jax
import jax.numpy as jnp
import numpy as np
from jax import lax
from jax.experimental import pallas as pl
from jax.experimental.pallas import tpu as pltpu
from jax.sharding import PartitionSpec as P

NG = 48
NCELL = 110592
PLANE = NG * NG
SLAB = 768
QX = 12
QCELL = QX * PLANE
F32 = jnp.float32
BF16 = jnp.bfloat16
R2 = math.sqrt(0.5)
C1 = math.cos(math.pi / 8)
C3 = math.cos(3 * math.pi / 8)
S3 = math.sqrt(3.0) / 2

ORDER = [("C", b) for b in range(9)] + [("S", b) for b in range(1, 8)]
SWAPPED = [("C", 0)] + [("S", b) for b in range(1, 8)] + [("C", 8)] + [("C", b) for b in range(1, 8)]


def sixteen(order):
    u = np.arange(16)
    cols = []
    for kind, b in order:
        col = np.cos(2 * np.pi * b * u / 16) if kind == "C" else np.sin(2 * np.pi * b * u / 16)
        cols.append(col / np.linalg.norm(col))
    return np.stack(cols, 1)


def folded(g):
    return (g + 24) % 48 - 24


def x_basis():
    keys, freqs, norms = [], [], []
    for b in range(9):
        keys.append(("A", "C", b)); freqs.append(3 * b); norms.append(48 if b in (0, 8) else 24)
    for b in range(1, 8):
        keys.append(("A", "S", b)); freqs.append(3 * b); norms.append(24)
    for b in (0, 8):
        for t in "cs":
            keys.append((t, "C", b)); freqs.append(16 + 3 * b); norms.append(24)
    for b in range(1, 8):
        for sign in (1, -1):
            for kind in ("cos", "sin"):
                keys.append((kind, sign, b)); freqs.append(16 + 3 * sign * b); norms.append(24)
    return keys, np.array(freqs), np.array(norms)


def lane_freqs(group):
    out = []
    for kind, b in ORDER:
        if group == "A":
            out.append(3 * b)
        elif b in (0, 8):
            out.append(16 + 3 * b)
        else:
            out.append(16 + 3 * b if (group == "u") == (kind == "C") else 16 - 3 * b)
    return np.array(out)


def kernel_values():
    _, gx, nx = x_basis()
    g = np.stack([lane_freqs(group) for group in "Auv"])
    gy, gz = g[:, None, :, None], g[None, :, None, :]
    q = folded(gx)[:, None, None, None, None] ** 2 + (folded(gy) ** 2 + folded(gz) ** 2)[None]
    q = q.astype(np.float64)
    kern = np.where(q > 0, 40.0 * (1.0 - np.exp(-q / 16.0)) / np.where(q > 0, q, 1.0), 0.0)
    return (kern / (9.0 * nx[:, None, None, None, None])).reshape(NG, PLANE).astype(np.float32)


PLACES = np.array([0, 3, 6, 1, 4, 7, 2, 5])
LANE_Y = np.repeat(np.concatenate([PLACES, 8 + PLACES]), 16)
LANE_Z = np.tile(np.arange(16), 16)


def thirds():
    rows = []
    for lane in (LANE_Y, LANE_Z):
        rows += [np.cos(2 * np.pi * (m + lane) / 3) for m in range(3)]
        rows += [np.sin(2 * np.pi * (m + lane) / 3) for m in range(3)]
    return np.concatenate([np.stack(rows), np.zeros((4, 256))]).astype(np.float32)


def factor_tables():
    bases = sixteen(ORDER), sixteen(SWAPPED)
    slow = [np.repeat(t[LANE_Y[::16]], 16, 1) for t in bases] + [t.T[:, LANE_Y] for t in bases]
    fast = [np.tile(t, (1, 16)) for t in bases] + [np.tile(t.T, (1, 16)) for t in bases]
    return np.stack(slow).astype(np.float32), np.stack(fast).astype(np.float32)


def packed_tables():
    slow, fast = factor_tables()
    kern = kernel_values().reshape(3, 16, 9, 256).transpose(2, 0, 1, 3).reshape(27, 16, 256)
    return np.concatenate([slow, fast, thirds()[None], kern])


def tables_kernel(packed, hi_there, lo_there, hi_back, lo_back, kern, third):
    third[...] = packed[8]
    for g in range(9):
        for r in range(3):
            kern[16 * r : 16 * r + 16, 256 * g : 256 * g + 256] = packed[9 + 3 * g + r]
    for way, (hi, lo) in enumerate(((hi_there, lo_there), (hi_back, lo_back))):
        for k in range(4):
            for u in range(16):
                w = packed[4 + 2 * way + k % 2] * packed[2 * way + k // 2, u : u + 1, :]
                top = w.astype(BF16)
                hi[k, 16 * u : 16 * u + 16, :] = top
                lo[k, 16 * u : 16 * u + 16, :] = (w - top.astype(F32)).astype(BF16)


def plane_tables():
    out = [jax.ShapeDtypeStruct((4, 256, 256), BF16)] * 4
    out += [jax.ShapeDtypeStruct((NG, PLANE), F32), jax.ShapeDtypeStruct((16, 256), F32)]
    return pl.pallas_call(
        tables_kernel, out_shape=out, name="plane_tables",
        compiler_params=pltpu.CompilerParams(vmem_limit_bytes=8 << 20),
    )(jnp.asarray(packed_tables()))


def t16(f):
    o = [f[u] - f[u + 8] for u in range(8)]
    e = [f[u] + f[u + 8] for u in range(8)]
    ee = [e[u] + e[u + 4] for u in range(4)]
    eo = [e[u] - e[u + 4] for u in range(4)]
    c, s = {}, {}
    p0, p1 = ee[0] + ee[2], ee[1] + ee[3]
    c[0], c[8], c[4], s[4] = p0 + p1, p0 - p1, ee[0] - ee[2], ee[1] - ee[3]
    d, a = R2 * (eo[1] - eo[3]), R2 * (eo[1] + eo[3])
    c[2], c[6], s[2], s[6] = eo[0] + d, eo[0] - d, a + eo[2], a - eo[2]
    d1, d2, d3 = (o[u] - o[8 - u] for u in (1, 2, 3))
    s1, s2, s3 = (o[u] + o[8 - u] for u in (1, 2, 3))
    d2, s2 = R2 * d2, R2 * s2
    e1, e3 = o[0] + d2, o[0] - d2
    o1, o3 = C1 * d1 + C3 * d3, C3 * d1 - C1 * d3
    c[1], c[7], c[3], c[5] = e1 + o1, e1 - o1, e3 + o3, e3 - o3
    x1, x3 = o[4] + s2, o[4] - s2
    y1, y3 = C3 * s1 + C1 * s3, C1 * s1 - C3 * s3
    s[1], s[7], s[3], s[5] = y1 + x1, y1 - x1, y3 - x3, y3 + x3
    return c, s


def t16_back(c, s):
    e1, o1, e3, o3 = c[1] + c[7], c[1] - c[7], c[3] + c[5], c[3] - c[5]
    o0, d2 = e1 + e3, R2 * (e1 - e3)
    d1, d3 = C1 * o1 + C3 * o3, C3 * o1 - C1 * o3
    y1, x1, y3, x3 = s[1] + s[7], s[1] - s[7], s[3] + s[5], s[5] - s[3]
    o4, s2 = x1 + x3, R2 * (x1 - x3)
    s1, s3 = C3 * y1 + C1 * y3, C1 * y1 - C3 * y3
    o = [o0, d1 + s1, d2 + s2, d3 + s3, o4, s3 - d3, s2 - d2, s1 - d1]
    d, a = R2 * (c[2] - c[6]), R2 * (s[2] + s[6])
    eo = [c[2] + c[6], d + a, s[2] - s[6], a - d]
    p0, p1 = c[0] + c[8], c[0] - c[8]
    ee = [p0 + c[4], p1 + s[4], p0 - c[4], p1 - s[4]]
    e = [ee[u] + eo[u] for u in range(4)] + [ee[u] - eo[u] for u in range(4)]
    return [e[u] + o[u] for u in range(8)] + [e[u] - o[u] for u in range(8)]


def convolve_x(f, table):
    keys, _, _ = x_basis()
    row = {key: k for k, key in enumerate(keys)}
    place = {(x % 3, x % 16): x for x in range(NG)}
    part = {"A": [], "c": [], "s": []}
    for u in range(16):
        f0, f1, f2 = (f[place[t, u]] for t in range(3))
        a = f1 + f2
        part["A"].append(f0 + a)
        part["c"].append(f0 - 0.5 * a)
        part["s"].append(S3 * (f1 - f2))
    c, s = t16(part["A"])
    c = {b: v * table(row["A", "C", b]) for b, v in c.items()}
    s = {b: v * table(row["A", "S", b]) for b, v in s.items()}
    back_a = t16_back(c, s)
    cc, cs = t16(part["c"])
    sc, ss = t16(part["s"])
    for b in (0, 8):
        cc[b] = cc[b] * table(row["c", "C", b])
        sc[b] = sc[b] * table(row["s", "C", b])
    for b in range(1, 8):
        p = (cc[b] - ss[b]) * table(row["cos", 1, b])
        m = (cc[b] + ss[b]) * table(row["cos", -1, b])
        cc[b], ss[b] = p + m, m - p
        p = (sc[b] + cs[b]) * table(row["sin", 1, b])
        m = (sc[b] - cs[b]) * table(row["sin", -1, b])
        sc[b], cs[b] = p + m, p - m
    back_c, back_s = t16_back(cc, cs), t16_back(sc, ss)
    out = [None] * NG
    for u in range(16):
        a, c_, s_ = back_a[u], back_c[u], S3 * back_s[u]
        h = a - 0.5 * c_
        out[place[0, u]] = a + c_
        out[place[1, u]] = h + s_
        out[place[2, u]] = h - s_
    return out


def group(k, j):
    return slice(k * SLAB + j * 256, k * SLAB + j * 256 + 256)


def split(hi, lo, rows, span, value):
    top = value.astype(BF16)
    hi[rows, span] = top
    lo[rows, span] = (value - top.astype(F32)).astype(BF16)


def product(hi, lo, whi, wlo, k, j):
    span = group(k, j)
    a, b = hi[:, span], lo[:, span]
    w = (k // 2) * 2 + j // 2
    lhs = jnp.concatenate([a, b, a], axis=1)
    rhs = jnp.concatenate([whi[w], whi[w], wlo[w]], axis=0)
    return jnp.dot(lhs, rhs, preferred_element_type=F32)


def turn(value, lanes):
    return pltpu.roll(value, lanes % 128, 1) if lanes % 128 else value


def to_thirds(f, third, first):
    c, s = third[first : first + 3], third[first + 3 : first + 6]
    return (
        f[0] + f[1] + f[2],
        f[0] * c[0] + f[1] * c[1] + f[2] * c[2],
        f[0] * s[0] + f[1] * s[1] + f[2] * s[2],
    )


def third_rows(third, h, rows):
    lanes = slice(128 * h, 128 * h + 128)
    return [jnp.broadcast_to(third[k : k + 1, lanes], (rows, 128)) for k in range(12)]


def from_thirds(a, c, s, third, first):
    return [a + c * third[first + m] + s * third[first + 3 + m] for m in range(3)]


def densities_of(q, sources, third, right, left, hi, lo):
    sub = lax.broadcasted_iota(jnp.int32, (8, 128), 0)
    to_right = sub % 4
    to_left = jnp.where(sub < 4, q, 4 + q % 2)
    place = lax.broadcasted_iota(jnp.int32, (8, 128), 1) // 16 % 3
    for delta, bands_ref, low_ref in sources:
        base = (q ^ delta) * QX

        def densities(i, carry):
            rows = pl.ds(pl.multiple_of(8 * base + 16 * i, 16), 16)
            for h in range(2):
                pairs = []
                for half in range(2):
                    x = base + 2 * i + half
                    f = [[None] * 3 for _ in range(3)]
                    for m in range(3):
                        v = []
                        for n in range(3):
                            at = pl.ds(pl.multiple_of((2 * i + half) * PLANE + (m * SLAB + h * 384 + n * 128), 128), 128)
                            low = low_ref[:, at]
                            v.append(jnp.concatenate([bands_ref[:, at], low, low], axis=0))
                        for j in range(3):
                            got = jnp.where(place == j, v[0], jnp.where(place == (j + 1) % 3, v[1], v[2]))
                            got = turn(got, -16 * j)
                            r = jnp.take_along_axis(got, to_right, axis=0)
                            l = jnp.take_along_axis(got, to_left, axis=0)
                            span = slice(m * SLAB + j * 256 + h * 128, m * SLAB + j * 256 + h * 128 + 128)
                            right[x, :, span] = r
                            left[x, :, span] = l
                            f[m][j] = r * l
                    pairs.append(f)
                thirds_h = third_rows(third, h, 8)
                spec = []
                for f in pairs:
                    f = [to_thirds([f[m][j] for m in range(3)], thirds_h, 0) for j in range(3)]
                    spec.append([to_thirds([f[n][k] for n in range(3)], thirds_h, 6) for k in range(3)])
                for k in range(3):
                    for j in range(3):
                        span = slice(k * SLAB + j * 256 + h * 128, k * SLAB + j * 256 + h * 128 + 128)
                        split(hi, lo, rows, span, jnp.concatenate([spec[0][k][j], spec[1][k][j]], axis=0))
            return carry

        lax.fori_loop(0, QX // 2, densities, 0)


def first_kernel(q_ref, own, one, low_a, core_a, third, right, left, hi, lo):
    densities_of(q_ref[0], ((0, own, low_a), (1, one, core_a)), third, right, left, hi, lo)


def spectrum_kernel(q_ref, two, three, low_b, core_b, kern, third, whi, wlo, right_in, left_in, hi_in, lo_in,
                    right, left, hi, lo, field):
    densities_of(q_ref[0], ((2, two, low_b), (3, three, core_b)), third, right, left, hi, lo)
    for k in (0, 1):
        if k == 0:
            rows_of = [[product(hi, lo, whi, wlo, 0, j)] for j in range(3)]
        else:
            both = [(product(hi, lo, whi, wlo, 1, j), product(hi, lo, whi, wlo, 2, j)) for j in range(3)]
            rows_of = [[c - s, c + s] for c, s in both]
        for n in range(len(rows_of[0])):
            a, c, s = (rows_of[j][n] for j in range(3))
            field[:, group(k + n, 0)] = a
            field[:, group(k + n, 1)] = c - s
            field[:, group(k + n, 2)] = c + s

    def along_x(i, carry):
        span = pl.ds(pl.multiple_of(128 * i, 128), 128)
        f = [field[8 * x : 8 * x + 8, span] for x in range(NG)]
        out = convolve_x(f, lambda k: kern[k : k + 1, span])
        for x in range(NG):
            field[8 * x : 8 * x + 8, span] = out[x]
        return carry

    lax.fori_loop(0, PLANE // 128, along_x, 0)


def terms_kernel(q_ref, right, left, field, third, whi, wlo, near0, near2, cross, low0, low2, hi, lo, back):
    q = q_ref[0]

    def unmix(i, carry):
        rows = pl.ds(pl.multiple_of(16 * i, 16), 16)
        mixed = [[field[rows, group(k, j)] for j in range(3)] for k in range(3)]
        mixed = [[a, u + v, v - u] for a, u, v in mixed]
        for j in range(3):
            a, u, v = (mixed[k][j] for k in range(3))
            for k, value in enumerate((a, u + v, v - u)):
                split(hi, lo, rows, group(k, j), value)
        return carry

    lax.fori_loop(0, NG // 2, unmix, 0)
    for k in range(3):
        for j in range(3):
            back[:, group(k, j)] = product(hi, lo, whi, wlo, k, j)

    sub = lax.broadcasted_iota(jnp.int32, (8, 128), 0)
    mine = (sub == q).astype(F32)
    place = lax.broadcasted_iota(jnp.int32, (8, 128), 1) // 16 % 3

    for delta in range(4):
        base = (q ^ delta) * QX

        def finish(i, carry):
            for half in range(X_STEP):
                x = base + X_STEP * i + half
                rows = pl.ds(pl.multiple_of(x * 8, 8), 8)
                for h in range(2):
                    thirds_h = third_rows(third, h, 8)

                    def spot(k, j):
                        return slice(k * SLAB + j * 256 + h * 128, k * SLAB + j * 256 + h * 128 + 128)

                    v = [from_thirds(*(back[rows, spot(k, j)] for j in range(3)), thirds_h, 6) for k in range(3)]
                    v = [from_thirds(*(v[k][j] for k in range(3)), thirds_h, 0) for j in range(3)]
                    for m in range(3):
                        parts = []
                        for j in range(3):
                            pr = v[j][m] * right[x, :, spot(m, j)]
                            pr = pr + swapped(pr, sub, 1)
                            pr = pr + swapped(pr, sub, 2)
                            po = swapped(v[j][m] * left[x, :, spot(m, j)], sub, 4) + mine * pr
                            parts.append(turn(jnp.where(sub < 4, po, pr), 16 * j))
                        for n in range(3):
                            out = jnp.where(place == n, parts[0], jnp.where(place == (n + 1) % 3, parts[1], parts[2]))
                            start = (X_STEP * i + half) * PLANE + (m * SLAB + h * 384 + n * 128)
                            at = pl.ds(pl.multiple_of(start, 128), 128)
                            if delta % 2:
                                cross[delta // 2 * 4 : delta // 2 * 4 + 4, at] = out[0:4, :]
                                cross[8 + delta // 2 : 9 + delta // 2, at] = out[4:5, :]
                            else:
                                (near0, near2)[delta // 2][:, at] = out[0:4, :]
                                (low0, low2)[delta // 2][:, at] = out[4:5, :]
            return carry

        lax.fori_loop(0, QX // X_STEP, finish, 0)


def swapped(value, sub, flip):
    return jnp.take_along_axis(value, sub ^ flip, axis=0)


X_STEP = 6
VMEM_SPEC = pl.BlockSpec(memory_space=pltpu.VMEM)
SMEM_SPEC = pl.BlockSpec(memory_space=pltpu.SMEM)
SPLIT = [pltpu.VMEM((NG * 8, PLANE), BF16)] * 2


STATE = [jax.ShapeDtypeStruct((NG, 8, PLANE), F32)] * 2 + [jax.ShapeDtypeStruct((NG * 8, PLANE), BF16)] * 2


def first_densities(q, bands, third):
    return pl.pallas_call(
        first_kernel,
        out_shape=STATE,
        in_specs=[SMEM_SPEC] + [VMEM_SPEC] * 5,
        out_specs=[VMEM_SPEC] * 4,
        name="first_densities",
        compiler_params=pltpu.CompilerParams(vmem_limit_bytes=16 << 20),
    )(q.reshape(1), *bands, third)


def spectrum(q, bands, kern, third, tables, state):
    return pl.pallas_call(
        spectrum_kernel,
        out_shape=STATE + [jax.ShapeDtypeStruct((NG * 8, PLANE), F32)],
        in_specs=[SMEM_SPEC] + [VMEM_SPEC] * 12,
        out_specs=[VMEM_SPEC] * 5,
        input_output_aliases={9: 0, 10: 1, 11: 2, 12: 3},
        name="spectrum",
        compiler_params=pltpu.CompilerParams(vmem_limit_bytes=28 << 20),
    )(q.reshape(1), *bands, kern, third, *tables, *state)


def terms(q, right, left, field, third, tables):
    return pl.pallas_call(
        terms_kernel,
        out_shape=[jax.ShapeDtypeStruct(shape, F32) for shape in [(4, QCELL)] * 2 + [(10, QCELL)] + [(1, QCELL)] * 2],
        in_specs=[SMEM_SPEC] + [VMEM_SPEC] * 6,
        out_specs=[VMEM_SPEC] * 5,
        scratch_shapes=SPLIT + [pltpu.VMEM((NG * 8, PLANE), F32)],
        name="terms",
        compiler_params=pltpu.CompilerParams(vmem_limit_bytes=28 << 20),
    )(q.reshape(1), right, left, field, third, *tables)


BOTH = ("band", "grid")
CHUNK = QCELL // 4


def small_call(body, outs, scratch=(), limit=8):
    vmem = pl.BlockSpec(memory_space=pltpu.VMEM)

    def call(where, *arrays):
        return pl.pallas_call(
            body,
            out_shape=[jax.ShapeDtypeStruct(shape, F32) for shape in outs],
            in_specs=[pl.BlockSpec(memory_space=pltpu.SMEM)] + [vmem] * len(arrays),
            out_specs=[vmem] * len(outs),
            scratch_shapes=list(scratch),
            compiler_params=pltpu.CompilerParams(vmem_limit_bytes=limit << 20),
        )(where, *arrays)

    return call


def chunk_of(where, k):
    return pl.ds(pl.multiple_of((where[2] ^ k) * CHUNK, 128), CHUNK)


def rows_kernel(where, orbitals, sel_a, sel_b):
    lower = where[0] < 2
    a, b = orbitals[0:2, :], orbitals[2:4, :]
    sel_a[...] = jnp.where(lower, a, b)
    sel_b[...] = jnp.where(lower, b, a)


def chunks_kernel(where, orbitals, copy, *chunks):
    copy[...] = orbitals[...]
    for k in range(4):
        chunks[k][...] = orbitals[:, chunk_of(where, k)]


def merge_kernel(where, near0, near2, low0, low2, across, near, far, owed_a, owed_b):
    first = where[0] % 2 == 0
    near[...] = near0[...] + across[0:4, :]
    far[...] = near2[...] + across[4:8, :]
    for out, low, row in ((owed_a, low0, 8), (owed_b, low2, 9)):
        a, b = low[...], across[row : row + 1, :]
        out[0:1, :] = jnp.where(first, a, b)
        out[1:2, :] = jnp.where(first, b, a)


def total_of(where, near, far, owed_a, owed_b, span):
    lower = where[0] < 2
    a, b = owed_a[:, span], owed_b[:, span]
    owed = jnp.concatenate([jnp.where(lower, a, b), jnp.where(lower, b, a)], axis=0)
    return -(near[:, span] + far[:, span] + owed)


def finalize_kernel(where, near, far, owed_a, owed_b, *chunks):
    for k in (1, 2, 3, 0):
        chunks[k][...] = total_of(where, near, far, owed_a, owed_b, chunk_of(where, k))


def vectors_kernel(where, near, far, owed_a, owed_b, vectors):
    for c in range(4):
        span = pl.ds(c * CHUNK, CHUNK)
        vectors[:, span] = total_of(where, near, far, owed_a, owed_b, span)


def margin_kernel(where, own0, oth0, own1, oth1, own2, oth2a, oth2b, own3, oth3, v0, v1, v2, v3, pieces, block):
    z, y, h = where[1], where[2], where[3]

    def halves(a):
        top = a.astype(BF16)
        return top, (a - top.astype(F32)).astype(BF16)

    v = jnp.concatenate(halves(jnp.concatenate([v0[...], v1[...], v2[...], v3[...]], axis=0)), axis=0)
    parts = jnp.concatenate([r[...] for r in (own0, oth0, own1, oth1, own2, oth2a, oth2b, own3, oth3)], axis=0)
    f = jnp.concatenate(halves(parts), axis=0)
    both = lax.dot_general(f, v, (((1,), (1,)), ((), ())), preferred_element_type=F32)
    both = both[0:128, :] + both[128:256, :]
    got = both[:, 0:16] + both[:, 16:32]
    for dz in range(4):
        for dy in range(4):
            row = 32 * dz + 4 * dy
            pair = got[row : row + 4, :], got[row + 16 : row + 20, :]
            at = (z + 4 - dz) % 4 * 4 + (y ^ dy)
            block[at, 0:4, :] = jnp.where(h == 0, pair[0], pair[1])
            block[at, 4:8, :] = jnp.where(h == 0, pair[1], pair[0])
    out = block[...].reshape(128, 16).T * (1.0 / NCELL)
    turned = [out] + [pltpu.roll(out, 32 * r, 1) for r in (1, 2, 3)]
    third_of = lax.broadcasted_iota(jnp.int32, (16, 128), 1) // 32
    keep = third_of == lax.broadcasted_iota(jnp.int32, (16, 128), 0) % 4
    for q_to in range(4):
        picked = turned[(3 - q_to) % 4]
        for j in range(3):
            picked = jnp.where(third_of == j, turned[(j - q_to) % 4], picked)
        picked = jnp.where(keep, picked, 0.0)
        for dy in range(4):
            row = jnp.sum(picked[4 * dy : 4 * dy + 4, :], axis=0, keepdims=True)
            pieces[pl.ds((y ^ dy) * 4 + q_to, 1), :] = row


def move(value, target):
    nb, nq = lax.axis_size("band"), lax.axis_size("grid")
    pairs = []
    for b in range(nb):
        for q in range(nq):
            z, y, h, q_to = target(b // 8, b // 2 % 4, b % 2, q)
            pairs.append((b * nq + q, ((z % 4) * 8 + (y % 4) * 2 + h) * nq + q_to))
    return lax.ppermute(value, BOTH, pairs)


def along_y(value, flip):
    return move(value, lambda z, y, h, q: (z, y ^ flip, h, q))


def along_z(value, k):
    return move(value, lambda z, y, h, q: (z + k, y, h, q))


def within(value, flip):
    return move(value, lambda z, y, h, q: (z, y, h, q ^ flip))


def around(value, blocks, flip):
    def target(z, y, h, q):
        b = (z * 8 + y * 2 + h + blocks) % 32
        return b // 8, b // 2 % 4, b % 2, q ^ flip

    return move(value, target)


def step(orbitals):
    b = lax.axis_index("band").astype(jnp.int32)
    q = lax.axis_index("grid").astype(jnp.int32)
    where = jnp.stack([q, b // 8, b // 2 % 4, b % 2])
    rows = small_call(rows_kernel, [(2, QCELL)] * 2)
    sel_a, sel_b = rows(where, orbitals)
    low_a = around(sel_a, 1, 0)
    low_b = around(sel_b, 1, 2)
    two = within(orbitals, 2)
    one = within(orbitals, 1)
    chunks = small_call(chunks_kernel, [(4, QCELL)] + [(4, CHUNK)] * 4)
    own, *pc = chunks(where, orbitals)
    pieces = [pc[0]] + [along_y(pc[k], k) for k in (1, 2, 3)]
    *tables, kern, third = plane_tables()
    together = jnp.concatenate(pieces, axis=0)
    core_a = within(low_a, 1)
    core_b = within(low_b, 1)
    three = within(two, 1)
    other = move(together, lambda z, y, h, q: (z, y, 1 - h, q))
    own1 = along_z(together, 1)
    own3 = along_z(together, 3)
    state = first_densities(q, (own, one, low_a, core_a), third)
    right, left, _, _, field = spectrum(q, (two, three, low_b, core_b), kern, third, tables[:2], state)
    near0, near2, cross, low0, low2 = terms(q, right, left, field, third, tables[2:4])
    across = within(cross, 1)
    other, _ = lax.optimization_barrier((other, near0))
    oth1 = along_z(other, 1)
    oth3 = along_z(other, 3)
    merge = small_call(merge_kernel, [(4, QCELL)] * 2 + [(2, QCELL)] * 2)
    near, both, owe_a, owe_b = merge(where, near0, near2, low0, low2, across)
    far = within(both, 2)
    owed_a = around(owe_a, -1, 0)
    owed_b = around(owe_b, -1, 2)
    own2 = along_z(own1, 1)
    oth2 = [along_z(oth1[:8], 1), along_z(oth3[8:], 3)]
    finalize = small_call(finalize_kernel, [(4, CHUNK)] * 4)
    vc = finalize(where, near, far, owed_a, owed_b)
    (vectors,) = small_call(vectors_kernel, [(4, QCELL)])(where, near, far, owed_a, owed_b)
    given = [vc[0]] + [along_y(vc[k], k) for k in (1, 2, 3)]
    margin_part = small_call(margin_kernel, [(16, 128)], [pltpu.VMEM((16, 8, 16), F32)], 20)
    (sums,) = margin_part(where, together, other, own1, oth1, own2, *oth2, own3, oth3, *given)
    groups = [[(z * 8 + y * 2 + h) * 4 + p for y in range(4) for p in range(4)] for z in range(4) for h in range(2)]
    sums = lax.all_to_all(sums, BOTH, 0, 0, tiled=True, axis_index_groups=groups)
    margin = jnp.sum(sums, axis=0).reshape(4, 32).T
    return vectors, margin


def solution(mesh):
    return jax.shard_map(
        step,
        mesh=mesh,
        in_specs=(P("band", "grid"),),
        out_specs=(P("band", "grid"), P("grid", "band")),
        check_vma=False,
    )
```
